32 devices in a mesh: seq: 4 (over z), fsdp: 8 (over y, x, core).
Axes of the slice: x: 2, y: 2, z: 4, core: 2. Of those that a mesh axis runs over, the one named last changes fastest.
Arguments:
- tokens: bfloat16 [8, 1024, 1536], P('fsdp', 'seq'), may hold values from -6 to 6
- teacher: bfloat16 [8, 1024, 1536], P('fsdp', 'seq'), may hold values from -6 to 6
- valid_mask: int32 [8, 1024], P('fsdp', 'seq'), may hold values 0 or 1
- segment_ids: int32 [8, 1024], P('fsdp'), may hold values from 0 to 11, never falling along the last dimension, each value on 1 to 512 neighbouring positions
- routes: int32 [8, 1024, 6], P('fsdp', 'seq'), may hold values from 0 to 31, all different within a row; in each aligned block of 256 rows (0 to 255, 256 to 511, ..., all dimensions but the last counted through in order) at most 64 rows name the same one
- gate_weights: float32 [8, 1024, 6], P('fsdp', 'seq'), may hold values from 0.1 to 0.4
- norm1_gain: bfloat16 [1536], P(('seq', 'fsdp')), may hold values from 0.5 to 1.5
- query_weight: bfloat16 [1536, 1536], P(('seq', 'fsdp')), may hold values from -0.15625 to 0.15625
- key_weight: bfloat16 [1536, 512], P(('seq', 'fsdp')), may hold values from -0.15625 to 0.15625
- value_weight: bfloat16 [1536, 512], P(('seq', 'fsdp')), may hold values from -0.15625 to 0.15625
- output_weight: bfloat16 [1536, 1536], P(('seq', 'fsdp')), may hold values from -0.625 to 0.625
- norm2_gain: bfloat16 [1536], P(('seq', 'fsdp')), may hold values from 0.5 to 1.5
- shared_gate_weight: bfloat16 [1536, 1024], P(('seq', 'fsdp')), may hold values from -0.15625 to 0.15625
- shared_up_weight: bfloat16 [1536, 1024], P(('seq', 'fsdp')), may hold values from -0.15625 to 0.15625
- shared_down_weight: bfloat16 [1024, 1536], P(('seq', 'fsdp')), may hold values from -0.1875 to 0.1875
- expert_gate_weight: bfloat16 [32, 1536, 512], P('fsdp', 'seq'), may hold values from -0.15625 to 0.15625
- expert_up_weight: bfloat16 [32, 1536, 512], P('fsdp', 'seq'), may hold values from -0.15625 to 0.15625
- expert_down_weight: bfloat16 [32, 512, 1536], P('fsdp', 'seq'), may hold values from -0.25 to 0.25
Outputs:
- block_output: bfloat16 [8, 1024, 1536], P('fsdp', 'seq')
- grad_tokens: float32 [8, 1024, 1536], P('fsdp', 'seq')
- grad_norm1_gain: float32 [1536], P(('seq', 'fsdp'))
- grad_query_weight: float32 [1536, 1536], P(('seq', 'fsdp'))
- grad_key_weight: float32 [1536, 512], P(('seq', 'fsdp'))
- grad_value_weight: float32 [1536, 512], P(('seq', 'fsdp'))
- grad_output_weight: float32 [1536, 1536], P(('seq', 'fsdp'))
- grad_norm2_gain: float32 [1536], P(('seq', 'fsdp'))
- grad_shared_gate_weight: float32 [1536, 1024], P(('seq', 'fsdp'))
- grad_shared_up_weight: float32 [1536, 1024], P(('seq', 'fsdp'))
- grad_shared_down_weight: float32 [1024, 1536], P(('seq', 'fsdp'))
- grad_expert_gate_weight: float32 [32, 1536, 512], P('fsdp', 'seq')
- grad_expert_up_weight: float32 [32, 1536, 512], P('fsdp', 'seq')
- grad_expert_down_weight: float32 [32, 512, 1536], P('fsdp', 'seq')
The draws below stay inside these ranges and needn't reach their ends.
Inputs may be any that keep to these rules, and one draw needn't show every extreme that they name: `segment_ids`: document numbers never fall along a sequence; a document has 1 to 512 tokens, and some document has exactly 512. `routes`: the 6 experts of a token differ; among the 256 tokens of one device no expert is named by more than 64 choices, and in some device's tokens one expert is named by exactly 64.
All inputs are finite; a program needn't handle non-finite values. No bound on the sum of `valid_mask` on one device may be relied on, other than what follows from the above.
Results may differ from the reference program's by a relative error of at most 0.015.
Values may be sent and summed in bfloat16 or wider, within the bound.
A program may use at most 256 MiB of HBM per device.

```python
import math
import jax
import jax.numpy as jnp
import numpy as np
from jax import lax

D = 1536
HEADS = 12
KV_HEADS = 4
HEAD = 128
FFE = 512
SHARED = 1024
TOP = 6
TOK_DEV = 256
DOCS = 12
EXPERTS = 32
SEQS = 8
LEN = 1024
CAP = 64


def with_ends(drawn, rng, smallest, largest):
    place = [jax.random.randint(jax.random.fold_in(rng, axis), (), 0, length) for axis, length in enumerate(drawn.shape)]
    longest = drawn.shape.index(max(drawn.shape))
    neighbour = place[:longest] + [(place[longest] + 1) % drawn.shape[longest]] + place[longest + 1:]
    return drawn.at[tuple(place)].set(smallest).at[tuple(neighbour)].set(largest)


def steps_of(key, shape, pieces, smallest, top_value):
    loudness, own = 1.0, jax.random.fold_in(key, 6)
    for dim, parts in pieces:
        steps = jnp.exp(jax.random.uniform(jax.random.fold_in(own, dim), (parts,), jnp.float32, smallest / len(pieces), top_value / len(pieces)))
        loudness = loudness * jnp.repeat(steps, shape[dim] // parts).reshape([-1 if axis == dim else 1 for axis in range(len(shape))])
    return loudness


def split_up(amount, total, bound, skew):
    portions = [(1 << 20) // math.isqrt(rank ** skew) + 1 for rank in range(2, amount + 1)]
    surplus, given = total - bound - (amount - 1), [1] * (amount - 1)
    while surplus > 0:
        candidates = [i for i in range(amount - 1) if given[i] < bound]
        mass, remaining = sum([portions[i] for i in candidates]), surplus
        for i in candidates:
            extra = min(bound - given[i], max(1, remaining * portions[i] // mass), surplus)
            given[i] = given[i] + extra
            surplus = surplus - extra
    return np.array([bound] + given)


def ragged_sizes(rng, amount, total, most, slope):
    if amount == 2:
        one = jax.random.randint(rng, (), max(1, total - most), min(most, total - 1) + 1)
        return jnp.stack([one, total - one])
    lengths = jnp.asarray(split_up(amount, total, most, slope), jnp.int32)
    couples = (amount - 1) // 2
    giver, sink = lengths[1:1 + 2 * couples:2], lengths[2:2 + 2 * couples:2]
    margin = jnp.minimum(giver - 1, most - sink)
    moved = jax.random.randint(jax.random.fold_in(rng, 1), (couples,), 0, 1 << 20) % (margin + 1)
    lengths = lengths.at[1:1 + 2 * couples:2].set(giver - moved).at[2:2 + 2 * couples:2].set(sink + moved)
    return lengths[jax.random.permutation(jax.random.fold_in(rng, 2), amount)]


def assign_block(key, own, number, rows, count, top, most, slope):
    sequence = jax.random.permutation(key, count)
    crowded, common = portions_of(count, rows * top, most, slope, True), portions_of(count, rows * top, most, slope, False)
    places = jnp.arange(count)

    def named(lengths, rotation):
        used = int((lengths > 0).sum())
        fixed = max(1, used // 4)
        moved = fixed + (places - fixed + rotation * (used - fixed)) % max(1, count - fixed)
        return jnp.zeros((count,), jnp.int32).at[sequence[jnp.where(places < fixed, places, moved)]].set(jnp.asarray(lengths, jnp.int32))

    lengths = jnp.where(number % 4 == 0, named(crowded, number // 4), named(common, number - number // 4 - 1))
    mixed = jax.random.permutation(jax.random.fold_in(own, 3), count)
    donor, receiver = mixed[0:count // 2 * 2:2], mixed[1:count // 2 * 2:2]
    margin = jnp.minimum(lengths[donor] - 1, most - lengths[receiver]) // 2
    margin = jnp.where((donor == sequence[0]) | (receiver == sequence[0]) | (lengths[receiver] == 0), 0, jnp.maximum(margin, 0))
    moved = jax.random.randint(jax.random.fold_in(own, 4), (count // 2,), 0, 1 << 20) % (margin + 1)
    lengths = lengths.at[donor].add(-moved).at[receiver].add(moved)
    labels = jnp.searchsorted(jnp.cumsum(lengths), jnp.arange(rows * top), side="right").astype(jnp.int32)
    table = labels.reshape(top, rows).T
    table = table[jax.random.permutation(jax.random.fold_in(own, 1), rows)]
    rotation = jax.random.randint(jax.random.fold_in(own, 2), (rows, 1), 0, top)
    return jnp.take_along_axis(table, (jnp.arange(top)[None, :] + rotation) % top, axis=1)


def portions_of(amount, total, most, lean, full):
    portions = [(1 << 20) // math.isqrt(standing ** lean) + 1 for standing in range(1, amount + 1)]
    largest = most if full else min(most, max(-(-total // amount), total * portions[0] // sum(portions)))
    least = 1 if total - largest >= amount - 1 else 0
    counts, spare = [largest] + [least] * (amount - 1), total - largest - least * (amount - 1)
    while spare > 0:
        free = [i for i in range(1, amount) if counts[i] < largest] or [i for i in range(1, amount) if counts[i] < most]
        mass, remaining = sum([portions[i] for i in free]), spare
        for i in free:
            more = min(most - counts[i], max(1, remaining * portions[i] // mass), spare)
            counts[i] = counts[i] + more
            spare = spare - more
    return np.array(counts)


def centred(rng, dims, width, bound, cuts=(), kind=jnp.bfloat16):
    entries = jax.random.normal(rng, dims, jnp.float32) * width
    if len(cuts) > 0:
        entries = steps_of(rng, dims, cuts, -0.22, 0.18) * entries
    return jnp.clip(entries, min=-bound, max=bound).astype(kind)


def setup_inputs(seed: int = 0) -> dict:
    key_of = jax.random.split(jax.random.key(seed), 19)
    tokens = centred(key_of[0], (SEQS, LEN, D), 1.0, 6.0, ((0, 8), (1, 4)))
    teacher = centred(key_of[1], (SEQS, LEN, D), 1.0, 6.0, ((0, 8), (1, 4)))
    valid_mask = with_ends((jax.random.randint(key_of[2], (SEQS, LEN), 0, 8) < 7).astype(jnp.int32), jax.random.fold_in(key_of[2], 1), 0, 1)
    segment_ids = jax.vmap(lambda own: jnp.searchsorted(jnp.cumsum(ragged_sizes(own, DOCS, LEN, LEN // 2, 2)), jnp.arange(LEN), side="right"))(jax.random.split(key_of[3], SEQS)).reshape((SEQS, LEN)).astype(jnp.int32)
    routes_keys = jax.random.split(jax.random.fold_in(key_of[4], 1), SEQS * LEN // TOK_DEV)
    routes_turns = jax.random.permutation(jax.random.fold_in(key_of[4], 3), SEQS * LEN // TOK_DEV)
    routes = jax.vmap(lambda own, number: assign_block(jax.random.fold_in(key_of[4], 2), own, number, TOK_DEV, EXPERTS, TOP, CAP, 1))(routes_keys, routes_turns).reshape((SEQS, LEN, TOP))
    gate_weights = jnp.clip(0.1 + 0.3 * jax.random.uniform(key_of[5], (SEQS, LEN, TOP), jnp.float32) ** steps_of(key_of[5], (SEQS, LEN, TOP), ((0, 8), (1, 4)), -0.2, 0.2), 0.1, 0.4)
    norm1_gain = jnp.clip(1.0 + 0.1 * jax.random.normal(key_of[6], (D,), jnp.float32), 0.5, 1.5).astype(jnp.bfloat16)
    query_weight = centred(key_of[7], (D, HEADS * HEAD), D ** -0.5, 0.15625, ((0, 32),))
    key_weight = centred(key_of[8], (D, KV_HEADS * HEAD), D ** -0.5, 0.15625, ((0, 32),))
    value_weight = centred(key_of[9], (D, KV_HEADS * HEAD), D ** -0.5, 0.15625, ((0, 32),))
    output_weight = centred(key_of[10], (HEADS * HEAD, D), (D // 16) ** -0.5, 0.625, ((0, 32),))
    norm2_gain = jnp.clip(1.0 + 0.1 * jax.random.normal(key_of[11], (D,), jnp.float32), 0.5, 1.5).astype(jnp.bfloat16)
    shared_gate_weight = centred(key_of[12], (D, SHARED), D ** -0.5, 0.15625, ((0, 32),))
    shared_up_weight = centred(key_of[13], (D, SHARED), D ** -0.5, 0.15625, ((0, 32),))
    shared_down_weight = centred(key_of[14], (SHARED, D), SHARED ** -0.5, 0.1875, ((0, 32),))
    expert_gate_weight = centred(key_of[15], (EXPERTS, D, FFE), D ** -0.5, 0.15625, ((0, 8), (1, 4)))
    expert_up_weight = centred(key_of[16], (EXPERTS, D, FFE), D ** -0.5, 0.15625, ((0, 8), (1, 4)))
    expert_down_weight = centred(key_of[17], (EXPERTS, FFE, D), FFE ** -0.5, 0.25, ((0, 8), (1, 4)))
    return {"tokens": tokens, "teacher": teacher, "valid_mask": valid_mask, "segment_ids": segment_ids, "routes": routes, "gate_weights": gate_weights, "norm1_gain": norm1_gain, "query_weight": query_weight, "key_weight": key_weight, "value_weight": value_weight, "output_weight": output_weight, "norm2_gain": norm2_gain, "shared_gate_weight": shared_gate_weight, "shared_up_weight": shared_up_weight, "shared_down_weight": shared_down_weight, "expert_gate_weight": expert_gate_weight, "expert_up_weight": expert_up_weight, "expert_down_weight": expert_down_weight}


EPSILON = 1e-05
MASKED = -1e+30
HIGHEST = lax.Precision.HIGHEST

@jax.custom_vjp
def low(v):
    return lax.optimization_barrier(v.astype(jnp.bfloat16)).astype(jnp.float32)

@jax.custom_vjp
def low_back(v):
    return v

def low_keep(v):
    return (low(v), None)

def low_pass(kept, grad):
    return (grad,)

def back_keep(v):
    return (v, None)

def back_low(kept, grad):
    return (low(grad),)
low.defvjp(low_keep, low_pass)
low_back.defvjp(back_keep, back_low)

def rms_norm(values, gain):
    factor = lax.rsqrt(lax.optimization_barrier(jnp.mean(values * values, axis=-1, keepdims=True)) + EPSILON)
    return values * factor * gain

def matmul(left, right):
    return jnp.dot(left, right, precision=HIGHEST, preferred_element_type=jnp.float32)

def attend_one(query_rows, key_rows, value_rows, segment):
    length = query_rows.shape[0]
    head_group = HEADS // KV_HEADS
    queries = query_rows.reshape(length, KV_HEADS, head_group, HEAD)
    key_heads = key_rows.reshape(length, KV_HEADS, HEAD)
    value_heads = value_rows.reshape(length, KV_HEADS, HEAD)
    raw_scores = jnp.einsum('ihgd,jhd->hgij', queries, key_heads, precision=HIGHEST)
    scores = low_back(raw_scores * (1.0 / math.sqrt(HEAD)))
    position = jnp.arange(length, dtype=jnp.int32)
    allowed = (position[None, :] <= position[:, None]) & (segment[None, :] == segment[:, None])
    scores = jnp.where(allowed, scores, MASKED)
    log_total = jax.nn.logsumexp(scores, axis=-1, keepdims=True)
    prob_low = low(jnp.exp(scores - log_total))
    attended = jnp.einsum('hgij,jhd->ihgd', prob_low, value_heads, precision=HIGHEST)
    return attended.reshape(length, HEADS * HEAD)

def expert_one(expert_rows, gate_weight, up_weight, down_weight):
    gate_rows = low_back(matmul(expert_rows, gate_weight))
    up_rows = low_back(matmul(expert_rows, up_weight))
    hidden = low(jax.nn.silu(gate_rows) * up_rows)
    return matmul(hidden, down_weight)

def reference(tokens, teacher, valid_mask, segment_ids, routes, gate_weights, norm1_gain, query_weight, key_weight, value_weight, output_weight, norm2_gain, shared_gate_weight, shared_up_weight, shared_down_weight, expert_gate_weight, expert_up_weight, expert_down_weight):
    seq_count, length, feat_width = tokens.shape
    token_count = seq_count * length
    blocks = token_count // TOK_DEV
    block_routes = routes.reshape(blocks, TOK_DEV * TOP)
    onehot = (block_routes[:, :, None] == jnp.arange(EXPERTS, dtype=jnp.int32)[None, None, :]).astype(jnp.int32)
    slot_index = lax.optimization_barrier(jnp.sum(jnp.cumsum(onehot, axis=1) * onehot, axis=2)) - 1
    block_index = jnp.arange(blocks, dtype=jnp.int32)[:, None]
    place_index = ((block_routes * blocks + block_index) * CAP + slot_index).reshape(token_count * TOP)
    slot_table = jnp.full((EXPERTS * blocks * CAP,), token_count * TOP, jnp.int32)
    slot_table = slot_table.at[place_index].set(jnp.arange(token_count * TOP, dtype=jnp.int32))
    source_row = slot_table // TOP
    gate_values = gate_weights.reshape(token_count, TOP).astype(jnp.float32)
    attend = jax.checkpoint(attend_one)
    expert_apply = jax.checkpoint(expert_one)

    def forward_pass(input_tokens, first_norm_gain, query_matrix, key_matrix, value_matrix, output_matrix, second_norm_gain, shared_gate_matrix, shared_up_matrix, shared_down_matrix, expert_gate_matrix, expert_up_matrix, expert_down_matrix):
        x_float = input_tokens.reshape(token_count, feat_width)
        normed_one = low(rms_norm(x_float, first_norm_gain))
        query_rows = low_back(low(matmul(normed_one, query_matrix)))
        key_rows = low_back(low(matmul(normed_one, key_matrix)))
        value_rows = low_back(low(matmul(normed_one, value_matrix)))
        attended = lax.map(lambda group_members: attend(*group_members), (query_rows.reshape(seq_count, length, -1), key_rows.reshape(seq_count, length, -1), value_rows.reshape(seq_count, length, -1), segment_ids))
        attended = low_back(low(attended.reshape(token_count, HEADS * HEAD)))
        mixed_rows = x_float + low_back(matmul(attended, output_matrix))
        normed_two = low(rms_norm(mixed_rows, second_norm_gain))
        shared_gate = low_back(matmul(normed_two, shared_gate_matrix))
        shared_up = low_back(matmul(normed_two, shared_up_matrix))
        shared_hidden = low(jax.nn.silu(shared_gate) * shared_up)
        shared_out = low_back(matmul(shared_hidden, shared_down_matrix))
        padded = jnp.concatenate([normed_two, jnp.zeros((1, feat_width), jnp.float32)], axis=0)
        dispatched_rows = low_back(padded[source_row]).reshape(EXPERTS, blocks * CAP, feat_width)
        expert_output = lax.map(lambda group_members: expert_apply(*group_members), (dispatched_rows, expert_gate_matrix, expert_up_matrix, expert_down_matrix))
        expert_output = low_back(low(expert_output)).reshape(EXPERTS * blocks * CAP, feat_width)
        per_choice = expert_output[place_index].reshape(token_count, TOP, feat_width)
        routed = lax.optimization_barrier(jnp.sum(gate_values[:, :, None] * per_choice, axis=1))
        return mixed_rows + shared_out + routed
    inputs_float = (tokens.astype(jnp.float32), norm1_gain.astype(jnp.float32), query_weight.astype(jnp.float32), key_weight.astype(jnp.float32), value_weight.astype(jnp.float32), output_weight.astype(jnp.float32), norm2_gain.astype(jnp.float32), shared_gate_weight.astype(jnp.float32), shared_up_weight.astype(jnp.float32), shared_down_weight.astype(jnp.float32), expert_gate_weight.astype(jnp.float32), expert_up_weight.astype(jnp.float32), expert_down_weight.astype(jnp.float32))
    output, pull_back = jax.vjp(forward_pass, *inputs_float)
    valid_rows = valid_mask.reshape(token_count, 1).astype(jnp.float32)
    cotangent = valid_rows * (output - teacher.reshape(token_count, feat_width).astype(jnp.float32))
    gradients = pull_back(cotangent)
    return (output.reshape(seq_count, length, feat_width).astype(jnp.bfloat16), gradients[0], gradients[1], gradients[2], gradients[3], gradients[4], gradients[5], gradients[6], gradients[7], gradients[8], gradients[9], gradients[10], gradients[11], gradients[12])
```

```python
import math

import jax
import jax.numpy as jnp
from jax import lax
from jax.sharding import PartitionSpec as P

HEADS = 12
KV_HEADS = 4
HEAD = 128
TOP = 6
EPSILON = 1e-05
MASKED = -1e30
PAIR = 2


BF16 = jnp.bfloat16
F32 = jnp.float32


def exchange(values, axis, bit):
    count = lax.axis_size(axis)
    return lax.ppermute(values, axis, [(i, i ^ bit) for i in range(count)])


def shift(values, axis, step):
    count = lax.axis_size(axis)
    pairs = [(i, i + step) for i in range(count) if 0 <= i + step < count]
    return lax.ppermute(values, axis, pairs)


def after(values, *others):
    return lax.optimization_barrier((values, *others))[0]


def pick(values, index):
    return values.at[index].get(mode="promise_in_bounds")


def dot(left, right, left_dim, right_dim):
    return lax.dot_general(
        left, right, (((left_dim,), (right_dim,)), ((), ())), preferred_element_type=F32
    )


def batch_dot(left, right, left_dim, right_dim):
    return lax.dot_general(
        left, right, (((left_dim,), (right_dim,)), ((0,), (0,))), preferred_element_type=F32
    )


def rms_norm(values, gain):
    factor = lax.rsqrt(jnp.mean(values * values, axis=-1, keepdims=True) + EPSILON)
    return values * factor * gain


def swiglu(gate_rows, up_rows):
    return jax.nn.silu(gate_rows) * up_rows


def swiglu_backward(gate_rows, up_rows, grad_rows):
    _, pull_back = jax.vjp(swiglu, gate_rows, up_rows)
    grad_gate, grad_up = pull_back(grad_rows)
    return (grad_gate.astype(BF16), grad_up.astype(BF16))


def far_bits():
    groups = lax.axis_size("fsdp")
    bits, bit = [], 2
    while bit < groups:
        bits.append(bit)
        bit *= 2
    return bits


def dense_codes():
    length, groups = lax.axis_size("seq"), lax.axis_size("fsdp")
    parts = []
    for half in (0, 1):
        codes = [groups * k for k in range(half * length // 2, (half + 1) * length // 2)]
        for bit in far_bits() if half == 0 else far_bits()[::-1]:
            codes = codes + [c ^ bit for c in codes]
        parts += [codes, [c ^ 1 for c in codes]]
    return parts


def gather_blocks(block, tokens):
    length = lax.axis_size("seq")
    first = after(block, *tokens.get("seq", ()))
    ring = [first] + [exchange(first, "seq", k) for k in range(1, length)]
    tokens["seq"] = ring[1:]
    parts = []
    for half in (0, 1):
        held = jnp.stack(ring[half * length // 2 : (half + 1) * length // 2])
        for stage, bit in enumerate(far_bits() if half == 0 else far_bits()[::-1]):
            sent = after(held, *tokens.get((half, stage), ()))
            came = exchange(sent, "fsdp", bit)
            tokens[(half, stage)] = (came,)
            held = jnp.concatenate([held, came], axis=0)
        parts += [held, exchange(held, "fsdp", 1)]
    return parts


def scatter_blocks(parts):
    length = lax.axis_size("seq")
    pieces = []
    for half in (0, 1):
        mine, other = parts[2 * half], parts[2 * half + 1]
        held = mine.astype(F32) + exchange(other, "fsdp", 1).astype(F32)
        for bit in (far_bits() if half == 0 else far_bits()[::-1])[::-1]:
            held = held.astype(mine.dtype)
            middle = held.shape[0] // 2
            came = exchange(held[middle:], "fsdp", bit)
            held = held[:middle].astype(F32) + came.astype(F32)
        pieces += [held[k] for k in range(length // 2)]
    total = pieces[0]
    for k in range(1, length):
        total = total + exchange(pieces[k].astype(parts[0].dtype), "seq", k).astype(F32)
    return total


def row_stages():
    return [("seq", 1)] + [("fsdp", bit) for bit in far_bits()]


def row_orders():
    groups = lax.axis_size("fsdp")
    stages = row_stages()
    orders = []
    for i in range(len(stages)):
        order = stages[i:] + stages[:i]
        codes = [0]
        for axis, bit in order:
            codes = codes + [c ^ (bit if axis == "fsdp" else groups * bit) for c in codes]
        orders.append((order, codes))
    return orders


def gather_rows(rows):
    orders = row_orders()
    width = rows.shape[1] // len(orders)
    gathered = []
    for i, (order, _) in enumerate(orders):
        held = rows[None, :, i * width : (i + 1) * width]
        for axis, bit in order:
            held = jnp.concatenate([held, exchange(held, axis, bit)], axis=0)
        gathered.append((held, exchange(held, "fsdp", 1)))
    return gathered


def scatter_rows(addends):
    outputs = []
    for (order, _), (mine, other) in zip(row_orders(), addends):
        held = mine.astype(F32) + exchange(other, "fsdp", 1).astype(F32)
        for axis, bit in order[::-1]:
            held = held.astype(BF16)
            middle = held.shape[0] // 2
            came = exchange(held[middle:], axis, bit)
            held = held[:middle].astype(F32) + came.astype(F32)
        outputs.append(held[0])
    return jnp.concatenate(outputs, axis=1)


def local(
    tokens,
    teacher,
    valid_mask,
    segment_ids,
    routes,
    gate_weights,
    norm1_gain,
    query_weight,
    key_weight,
    value_weight,
    output_weight,
    norm2_gain,
    shared_gate_weight,
    shared_up_weight,
    shared_down_weight,
    expert_gate_weight,
    expert_up_weight,
    expert_down_weight,
):
    length, groups = lax.axis_size("seq"), lax.axis_size("fsdp")
    seq_index, group_index = lax.axis_index("seq"), lax.axis_index("fsdp")
    devices = length * groups
    me = seq_index * groups + group_index
    tok_rows, feat_width = tokens.shape[1], tokens.shape[2]
    seq_len = segment_ids.shape[1]
    head_group = HEADS // KV_HEADS
    score_scale = 1.0 / math.sqrt(HEAD)
    key_width = KV_HEADS * HEAD
    query_width = HEADS * HEAD
    shared_width = shared_gate_weight.shape[1]

    meta = jnp.concatenate([routes[0].T.astype(F32), gate_weights[0].T], axis=0)[None]
    for axis, bit in [("fsdp", 1)] + row_stages():
        meta = jnp.concatenate([meta, exchange(meta, axis, bit)], axis=0)
    meta_codes = [0]
    for axis, bit in [("fsdp", 1)] + row_stages():
        meta_codes = meta_codes + [c ^ (bit if axis == "fsdp" else groups * bit) for c in meta_codes]

    waits = {}
    lanes = 128
    gains = jnp.pad(jnp.stack([norm1_gain, norm2_gain], axis=1), ((0, 0), (0, lanes - 2)))
    qkv_parts = gather_blocks(
        jnp.concatenate([query_weight, key_weight, value_weight, gains], axis=1), waits
    )
    output_parts = gather_blocks(output_weight, waits)
    gate_up_parts = gather_blocks(
        jnp.concatenate([shared_gate_weight, shared_up_weight], axis=1), waits
    )
    down_parts = gather_blocks(shared_down_weight, waits)
    codes = jnp.asarray(sum(dense_codes(), []), jnp.int32)
    to_code = me ^ codes
    place = [0] * devices
    for position, code in enumerate(sum(dense_codes(), [])):
        place[code] = position
    to_plain = pick(jnp.asarray(place, jnp.int32), me ^ jnp.arange(devices, dtype=jnp.int32))

    def coded(rows):
        turned = pick(rows.T.reshape(devices, -1, rows.shape[0]), to_code)
        return list(turned.reshape(4, -1, rows.shape[0]))

    def plain(parts):
        turned = jnp.concatenate(parts, axis=0)
        blocks = turned.reshape(devices, -1, turned.shape[-1])
        return pick(blocks, to_plain).reshape(turned.shape).T

    def flat(parts):
        return [part.reshape(-1, part.shape[-1]) for part in parts]

    def forward(coded_rows, weight_parts):
        return sum(dot(rows, part, 0, 0) for rows, part in zip(coded_rows, weight_parts))

    def backward_parts(grad_rows, weight_parts):
        return [dot(part, grad_rows, 1, 1) for part in weight_parts]

    def weight_grad(coded_rows, grad_rows):
        out = []
        for rows in coded_rows:
            grad = dot(rows, grad_rows, 1, 0).astype(BF16)
            out.append(grad.reshape(devices // 4, -1, grad.shape[-1]))
        return out

    qkv_flat = flat(qkv_parts)
    output_flat, gate_up_flat, down_flat = flat(output_parts), flat(gate_up_parts), flat(down_parts)
    qkv_width = query_width + 2 * key_width
    gain_codes = jnp.concatenate([part[:, :, qkv_width : qkv_width + 2] for part in qkv_parts], axis=0)
    gain_plain = pick(gain_codes, to_plain).reshape(feat_width, 2).T.astype(F32)
    gain_one, gain_two = gain_plain[0], gain_plain[1]

    num_local = expert_gate_weight.shape[0]
    num_held = num_local // PAIR
    side = seq_index % PAIR

    def share(weight, k):
        return lax.dynamic_slice_in_dim(weight, (side ^ (k % PAIR)) * num_held, num_held, axis=0)

    def collect(weight):
        blocks = [share(weight, 0)]
        sent = after(weight, *waits["seq"])
        came = [exchange(share(sent, k), "seq", k) for k in range(1, length)]
        waits["seq"] = came
        stacked = pick(jnp.stack(blocks + came), seq_index ^ jnp.arange(length, dtype=jnp.int32))
        return jnp.moveaxis(stacked, 0, 1).reshape(num_held, -1, weight.shape[2])

    expert_gate_full = collect(expert_gate_weight)
    expert_up_full = collect(expert_up_weight)
    expert_down_full = collect(expert_down_weight)

    x_float = tokens[0].astype(F32)
    normed_one = rms_norm(x_float, gain_one).astype(BF16)
    normed_one_codes = coded(normed_one)
    qkv_rows = forward(normed_one_codes, [part[:, :qkv_width] for part in qkv_flat]).astype(BF16)
    query_rows = qkv_rows[:, :query_width]
    key_value = [qkv_rows[:, query_width:]]
    longest = seq_len // 2
    back = min(length - 1, -(-(longest - 1) // tok_rows))
    for _ in range(back):
        key_value.insert(0, shift(key_value[0], "seq", 1))
    key_value_all = jnp.concatenate(key_value, axis=0)
    window = (back + 1) * tok_rows
    seg_padded = jnp.concatenate([jnp.full((back * tok_rows,), -1, jnp.int32), segment_ids[0]])
    seg_keys = lax.dynamic_slice_in_dim(seg_padded, seq_index * tok_rows, window)
    seg_here = seg_keys[back * tok_rows :]
    positions = back * tok_rows + jnp.arange(tok_rows, dtype=jnp.int32)
    key_positions = jnp.arange(window, dtype=jnp.int32)
    allowed = (key_positions[None, :] <= positions[:, None]) & (seg_keys[None, :] == seg_here[:, None])
    query_heads = query_rows.reshape(tok_rows, KV_HEADS, head_group, HEAD)
    key_heads = key_value_all[:, :key_width].reshape(window, KV_HEADS, HEAD)
    value_heads = key_value_all[:, key_width:].reshape(window, KV_HEADS, HEAD)

    def all_scores():
        raw_scores = jnp.einsum(
            "thgd,jhd->hgtj", query_heads, key_heads, preferred_element_type=F32
        )
        return jnp.where(allowed[None, None], raw_scores * score_scale, MASKED)

    scores = all_scores()
    log_total = jax.nn.logsumexp(scores, axis=-1, keepdims=True)
    prob_low = jnp.exp(scores - log_total).astype(BF16)
    attended = (
        jnp.einsum("hgtj,jhd->thgd", prob_low, value_heads, preferred_element_type=F32)
        .reshape(tok_rows, query_width)
        .astype(BF16)
    )
    attended_codes = coded(attended)
    mixed_rows = x_float + forward(attended_codes, output_flat)
    normed_two = rms_norm(mixed_rows, gain_two).astype(BF16)

    orders = row_orders()
    gathered = gather_rows(normed_two)
    experts_all = num_local * groups
    capacity = tok_rows * TOP * 4 // (3 * experts_all)
    route_all, gate_all = meta[:, :TOP], meta[:, TOP:]
    held_ids = group_index * num_local + side * num_held + jnp.arange(num_held, dtype=jnp.int32)
    named = route_all[:, None] == held_ids.astype(F32)[None, :, None, None]
    has = jnp.any(named, axis=2)
    gate_of = jnp.sum(jnp.where(named, gate_all[:, None], 0.0), axis=2)
    token_order = jnp.arange(tok_rows, dtype=jnp.int32)
    earlier = (token_order[:, None] < token_order[None, :]).astype(BF16)
    before = lax.dot_general(
        has.astype(BF16), earlier, (((2,), (0,)), ((), ())), preferred_element_type=F32
    )
    slot_number = jnp.arange(capacity, dtype=F32)
    chosen = has[:, :, None] & (before[:, :, None] == slot_number[None, None, :, None])
    gate_slots = jnp.sum(jnp.where(chosen, gate_of[:, :, None], 0.0), axis=3)
    sources = len(meta_codes)
    chosen_low = chosen.astype(BF16).reshape(sources, num_held * capacity, tok_rows)
    meta_place = {code: position for position, code in enumerate(meta_codes)}

    def in_order(array, piece_codes):
        return jnp.stack([array[meta_place[c]] for c in piece_codes])

    selectors = [
        (in_order(chosen_low, piece), in_order(chosen_low, [c ^ 1 for c in piece])) for _, piece in orders
    ]
    gate_canonical = jnp.moveaxis(
        in_order(gate_slots, orders[0][1] + [c ^ 1 for c in orders[0][1]]), 0, 1
    ).reshape(num_held, sources * capacity, 1)
    canonical = orders[0][1]

    def to_slots(pieces):
        columns = []
        for (_, piece), select, rows in zip(orders, selectors, pieces):
            where = {code: position for position, code in enumerate(piece)}
            turn = [where[c] for c in canonical]
            halves = []
            for selector, half in zip(select, rows):
                taken = batch_dot(selector, half, 2, 1).astype(BF16)
                halves.append(jnp.stack([taken[p] for p in turn]) if turn != sorted(turn) else taken)
            columns.append(jnp.concatenate(halves, axis=0))
        slots = jnp.concatenate(columns, axis=2).reshape(sources, num_held, capacity, feat_width)
        return jnp.moveaxis(slots, 0, 1).reshape(num_held, sources * capacity, feat_width)

    def from_slots(slots):
        by_source = jnp.moveaxis(
            slots.reshape(num_held, sources, capacity, feat_width), 0, 1
        ).reshape(sources, num_held * capacity, feat_width)
        width = feat_width // len(orders)
        half_count = sources // 2
        addends = []
        for i, ((_, piece), select) in enumerate(zip(orders, selectors)):
            where = {code: position for position, code in enumerate(canonical)}
            turn = [where[c] for c in piece]
            halves = []
            for h, selector in enumerate(select):
                part = by_source[h * half_count : (h + 1) * half_count, :, i * width : (i + 1) * width]
                if turn != sorted(turn):
                    part = jnp.stack([part[p] for p in turn])
                halves.append(batch_dot(selector, part, 1, 1).astype(BF16))
            addends.append(halves)
        return addends

    slot_rows = to_slots(gathered)
    expert_gate_rows = batch_dot(slot_rows, expert_gate_full, 2, 1)
    expert_up_rows = batch_dot(slot_rows, expert_up_full, 2, 1)
    expert_hidden = swiglu(expert_gate_rows, expert_up_rows).astype(BF16)
    expert_output = (gate_canonical * batch_dot(expert_hidden, expert_down_full, 2, 1)).astype(BF16)
    routed = scatter_rows(from_slots(expert_output))

    normed_two_codes = coded(normed_two)
    gate_up = forward(normed_two_codes, gate_up_flat)
    shared_gate, shared_up = gate_up[:, :shared_width], gate_up[:, shared_width:]
    shared_hidden = swiglu(shared_gate, shared_up).astype(BF16)
    shared_hidden_codes = coded(shared_hidden)
    shared_out = forward(shared_hidden_codes, down_flat)

    output = mixed_rows + shared_out + routed
    block_output = output.astype(BF16)
    valid_rows = valid_mask[0].astype(F32)[:, None]
    grad_out = valid_rows * (output - teacher[0].astype(F32))
    grad_low = grad_out.astype(BF16)

    grad_slots = (gate_canonical * to_slots(gather_rows(grad_low)).astype(F32)).astype(BF16)
    grad_hidden = batch_dot(grad_slots, expert_down_full, 2, 2)
    grad_gate_rows, grad_up_rows = swiglu_backward(expert_gate_rows, expert_up_rows, grad_hidden)
    grad_input = (
        batch_dot(grad_gate_rows, expert_gate_full, 2, 2) + batch_dot(grad_up_rows, expert_up_full, 2, 2)
    ).astype(BF16)
    grad_routed = scatter_rows(from_slots(grad_input))

    def expert_grad(left, right):
        grad = batch_dot(left, right, 1, 1).astype(BF16)
        rows = grad.shape[1] // length
        own = [None] * length
        for k in range(length):
            slab = lax.dynamic_slice_in_dim(grad, (seq_index ^ k) * rows, rows, axis=1)
            own[k] = (exchange(slab, "seq", k) if k else slab).astype(F32)
        same = sum(own[k] for k in range(0, length, PAIR))
        crossed = sum(own[k] for k in range(1, length, PAIR))
        return jnp.concatenate(
            [jnp.where(side == 0, same, crossed), jnp.where(side == 0, crossed, same)], axis=0
        )

    grad_expert_down = expert_grad(expert_hidden, grad_slots)
    grad_expert_gate = expert_grad(slot_rows, grad_gate_rows)
    grad_expert_up = expert_grad(slot_rows, grad_up_rows)

    grad_down_block = scatter_blocks(weight_grad(shared_hidden_codes, grad_low))
    grad_shidden = plain(backward_parts(grad_low, down_flat))
    grad_sgate_rows, grad_sup_rows = swiglu_backward(shared_gate, shared_up, grad_shidden)
    grad_gate_up = jnp.concatenate([grad_sgate_rows, grad_sup_rows], axis=1)
    grad_gate_up_block = scatter_blocks(weight_grad(normed_two_codes, grad_gate_up))
    grad_normed_two = plain(backward_parts(grad_gate_up, gate_up_flat)) + grad_routed
    _, pull_two = jax.vjp(rms_norm, mixed_rows, gain_two)
    grad_mixed_norm, grad_gain_two = pull_two(grad_normed_two)
    grad_mixed = grad_out + grad_mixed_norm
    grad_mixed_low = grad_mixed.astype(BF16)

    grad_output_block = scatter_blocks(weight_grad(attended_codes, grad_mixed_low))
    grad_attended = plain(backward_parts(grad_mixed_low, output_flat)).astype(BF16)
    grad_att_heads = grad_attended.reshape(tok_rows, KV_HEADS, head_group, HEAD)
    prob_full = jnp.exp(all_scores() - log_total)
    prob_back = prob_full.astype(BF16)
    grad_prob = jnp.einsum(
        "thgd,jhd->hgtj", grad_att_heads, value_heads, preferred_element_type=F32
    )
    grad_values = jnp.einsum(
        "hgtj,thgd->jhd", prob_back, grad_att_heads, preferred_element_type=F32
    ).reshape(window, key_width)
    row_delta = jnp.sum(prob_full * grad_prob, axis=-1, keepdims=True)
    grad_scores = (prob_full * (grad_prob - row_delta)).astype(BF16)
    grad_query = (
        (
            jnp.einsum("hgtj,jhd->thgd", grad_scores, key_heads, preferred_element_type=F32)
            * score_scale
        )
        .reshape(tok_rows, query_width)
        .astype(BF16)
    )
    grad_keys = (
        jnp.einsum("hgtj,thgd->jhd", grad_scores, query_heads, preferred_element_type=F32)
        * score_scale
    ).reshape(window, key_width)
    grad_key_value = jnp.concatenate([grad_keys, grad_values], axis=1)
    total = grad_key_value[:tok_rows]
    for step in range(1, back + 1):
        came = shift(total.astype(BF16), "seq", -1)
        total = came.astype(F32) + grad_key_value[step * tok_rows : (step + 1) * tok_rows]
    grad_qkv = jnp.concatenate([grad_query, total.astype(BF16)], axis=1)
    grad_qkv_block = scatter_blocks(weight_grad(normed_one_codes, grad_qkv))
    grad_normed_one = plain(backward_parts(grad_qkv, [part[:, :qkv_width] for part in qkv_flat]))
    _, pull_one = jax.vjp(rms_norm, x_float, gain_one)
    grad_x_norm, grad_gain_one = pull_one(grad_normed_one)
    grad_tokens = grad_mixed + grad_x_norm

    gain_grads = jnp.stack([grad_gain_one, grad_gain_two]).reshape(2, devices, -1)
    gain_coded = pick(jnp.moveaxis(gain_grads, 1, 0), to_code)
    grad_gain_block = scatter_blocks(list(gain_coded.reshape(4, devices // 4, 2, -1)))
    return (
        block_output[None],
        grad_tokens[None],
        grad_gain_block[0],
        grad_qkv_block[:, :query_width],
        grad_qkv_block[:, query_width : query_width + key_width],
        grad_qkv_block[:, query_width + key_width :],
        grad_output_block,
        grad_gain_block[1],
        grad_gate_up_block[:, :shared_width],
        grad_gate_up_block[:, shared_width:],
        grad_down_block,
        grad_expert_gate,
        grad_expert_up,
        grad_expert_down,
    )


def solution(mesh):
    rows = P("fsdp", "seq", None)
    dense = P(("seq", "fsdp"), None)
    gain = P(("seq", "fsdp"))
    return jax.shard_map(
        local,
        mesh=mesh,
        in_specs=(
            rows, rows, P("fsdp", "seq"), P("fsdp", None), rows, rows,
            gain, dense, dense, dense, dense, gain, dense, dense, dense, rows, rows, rows,
        ),
        out_specs=(
            rows, rows, gain, dense, dense, dense, dense, gain, dense, dense, dense, rows, rows, rows,
        ),
        check_vma=False,
    )
```

```python
import functools
import math

import jax
import jax.numpy as jnp
from jax import lax
from jax.experimental import pallas as pl
from jax.experimental.pallas import tpu as pltpu
from jax.sharding import PartitionSpec as P


HEADS = 12
KV_HEADS = 4
HEAD = 128
TOP = 6
EPSILON = 1e-05
MASKED = -1e30
PAIR = 2


BF16 = jnp.bfloat16
F32 = jnp.float32


def exchange(values, axis, bit):
    count = lax.axis_size(axis)
    return lax.ppermute(values, axis, [(i, i ^ bit) for i in range(count)])


def shift(values, axis, step):
    count = lax.axis_size(axis)
    pairs = [(i, i + step) for i in range(count) if 0 <= i + step < count]
    return lax.ppermute(values, axis, pairs)


def after(values, *others):
    return lax.optimization_barrier((values, *others))[0]


def dot(left, right, left_dim, right_dim):
    return lax.dot_general(
        left, right, (((left_dim,), (right_dim,)), ((), ())), preferred_element_type=F32
    )


def batch_dot(left, right, left_dim, right_dim):
    return lax.dot_general(
        left, right, (((left_dim,), (right_dim,)), ((0,), (0,))), preferred_element_type=F32
    )


def rms_norm(values, gain):
    factor = lax.rsqrt(jnp.mean(values * values, axis=-1, keepdims=True) + EPSILON)
    return values * factor * gain


def swiglu(gate_rows, up_rows):
    return jax.nn.silu(gate_rows) * up_rows


def swiglu_backward(gate_rows, up_rows, grad_rows):
    _, pull_back = jax.vjp(swiglu, gate_rows, up_rows)
    grad_gate, grad_up = pull_back(grad_rows)
    return (grad_gate.astype(BF16), grad_up.astype(BF16))


MESH = pl.DeviceIdType.MESH


def grant(scratch, extra):
    size = extra
    for ref in scratch:
        shape = list(ref.shape)
        shape[-2] = -(-shape[-2] // 16) * 16
        size += math.prod(shape) * jnp.dtype(ref.dtype).itemsize
    return min(size + 6 * 2**20, 66 * 10**6)


class Copies:
    def __init__(self, send_sems, recv_sems):
        self.send_sems, self.recv_sems, self.made = send_sems, recv_sems, []

    def start(self, source, target, axis, partner):
        number = len(self.made)
        copy = pltpu.make_async_remote_copy(
            src_ref=source,
            dst_ref=target,
            send_sem=self.send_sems.at[number],
            recv_sem=self.recv_sems.at[number],
            device_id={axis: partner},
            device_id_type=MESH,
        )
        copy.start()
        self.made.append(copy)
        return copy

    def finish(self):
        for copy in self.made:
            copy.wait_send()


def greet(partners):
    barrier = pltpu.get_barrier_semaphore()
    for axis, partner in partners:
        pl.semaphore_signal(barrier, inc=1, device_id={axis: partner}, device_id_type=MESH)
    pl.semaphore_wait(barrier, len(partners))


def bit_of(index, bit):
    return lax.rem(lax.div(index, bit), 2)


def flip(index, bit):
    return index + bit - 2 * bit * bit_of(index, bit)


def flip_all(index, mask):
    bit = 1
    while bit <= mask:
        if mask & bit:
            index = flip(index, bit)
        bit *= 2
    return index


def gather_dense_kernel(length, bits, count, *refs):
    shards, expert, outs, expert_full = refs[:count], refs[count], refs[count + 1 : 2 * count + 1], refs[2 * count + 1]
    send_sems, recv_sems, local_sems = refs[2 * count + 2 :]
    seq, group = lax.axis_index("seq"), lax.axis_index("fsdp")
    own = [bit_of(group, bit) for bit in bits]
    partners = [("seq", flip_all(seq, k)) for k in range(1, length)]
    partners += [("fsdp", flip(group, bit)) for bit in bits]
    greet(partners)
    copies = Copies(send_sems, recv_sems)
    far = len(bits) - 1
    half = length // 2
    side = lax.div(seq, half)
    low = [side * half, (1 - side) * half]
    orders = [list(range(far)), list(range(far))[::-1]]
    stages = far + 2
    waiting = [None] * count

    def launch(t, stage):
        if stage == 0:
            local = pltpu.make_async_copy(shards[t], outs[t].at[(seq, *own)], local_sems.at[t])
            local.start()
            made = [
                copies.start(shards[t], outs[t].at[(seq, *own)], "seq", flip_all(seq, k))
                for k in range(1, length)
            ]
            return made, local
        made = []
        for part in (0, 1):
            where = [pl.ds(low[part], half)] + list(own)
            for done in orders[part][: stage - 1]:
                where[1 + done] = slice(None)
            dim = orders[part][stage - 1] if stage <= far else far
            view = outs[t].at[tuple(where)]
            made.append(copies.start(view, view, "fsdp", flip(group, bits[dim])))
        return made, None

    def ship_expert():
        held, depth = expert.shape[0] // PAIR, expert.shape[1]
        rows = pl.ds(pl.multiple_of(seq * depth, depth), depth)
        parity = lax.rem(seq, PAIR)
        local = pltpu.make_async_copy(
            expert.at[pl.ds(parity * held, held)], expert_full.at[:, rows], local_sems.at[count]
        )
        local.start()
        made = []
        for k in range(1, length):
            other = lax.rem(parity + k, PAIR)
            made.append(
                copies.start(
                    expert.at[pl.ds(other * held, held)], expert_full.at[:, rows], "seq", flip_all(seq, k)
                )
            )
        return made, local

    for step in range(count + stages):
        if step == count:
            expert_waiting = ship_expert()
        for t in range(count):
            stage = step - t
            if 0 < stage <= stages and waiting[t]:
                made, local = waiting[t]
                for copy in made:
                    copy.wait_recv()
                if local is not None:
                    local.wait()
                waiting[t] = None
            if 0 <= stage < stages:
                waiting[t] = launch(t, stage)
    made, local = expert_waiting
    for copy in made:
        copy.wait_recv()
    local.wait()
    copies.finish()


def gather_dense(shards, expert):
    length, groups = lax.axis_size("seq"), lax.axis_size("fsdp")
    bits, bit = [], groups // 2
    while bit >= 1:
        bits.append(bit)
        bit //= 2
    count = len(shards)
    number = count * (length - 1 + 2 * len(bits)) + length - 1
    size = sum(s.size * s.dtype.itemsize for s in shards) * length * groups
    experts, depth, wide = expert.shape
    *outs, expert_full = pl.pallas_call(
        functools.partial(gather_dense_kernel, length, bits, count),
        out_shape=[
            jax.ShapeDtypeStruct((length,) + (2,) * len(bits) + s.shape, s.dtype) for s in shards
        ]
        + [jax.ShapeDtypeStruct((experts // PAIR, length * depth, wide), expert.dtype)],
        in_specs=[pl.BlockSpec(memory_space=pltpu.VMEM)] * count + [pl.BlockSpec(memory_space=pl.ANY)],
        out_specs=[pl.BlockSpec(memory_space=pl.ANY)] * (count + 1),
        scratch_shapes=[
            pltpu.SemaphoreType.DMA((number,)),
            pltpu.SemaphoreType.DMA((number,)),
            pltpu.SemaphoreType.DMA((count + 1,)),
        ],
        compiler_params=pltpu.CompilerParams(
            collective_id=0, has_side_effects=True, vmem_limit_bytes=16 * 2**20
        ),
        cost_estimate=pl.CostEstimate(flops=0, bytes_accessed=3 * size, transcendentals=0),
        name="gather_dense",
    )(*shards, expert)
    return [out.reshape(-1, out.shape[-1]) for out in outs] + [expert_full]


def scatter_dense_kernel(length, bits, count, *refs):
    grads, outs = refs[:count], refs[count : 2 * count]
    far = len(bits) - 1
    per = 3 + far
    scratch = refs[2 * count : 2 * count + per * count]
    send_sems, recv_sems, local_sems = refs[2 * count + per * count :]
    seq, group = lax.axis_index("seq"), lax.axis_index("fsdp")
    own = [bit_of(group, bit) for bit in bits]
    partners = [("seq", flip_all(seq, k)) for k in range(1, length)]
    partners += [("fsdp", flip(group, bit)) for bit in bits]
    greet(partners)
    copies = Copies(send_sems, recv_sems)
    half = length // 2
    side = lax.div(seq, half)
    low = [side * half, (1 - side) * half]
    orders = [list(range(far))[::-1], list(range(far))]
    stages = far + 2
    everything = (slice(None),) * (1 + far)

    def buffers(t):
        held = scratch[per * t : per * (t + 1)]
        return held[0], held[1], held[2 : 2 + far], held[2 + far]

    waiting = [None] * count

    def add(mine, came, lead, fixed, inner_of):
        start, size = lead
        left = [d for d in range(far) if d not in fixed]

        def body(i, carry):
            z = lax.div(i, 2 ** len(left))
            where, inner = [own[d] for d in range(far)], []
            for k, d in enumerate(left):
                where[d] = lax.rem(lax.div(i, 2 ** (len(left) - 1 - k)), 2)
                inner.append(where[d])
            place = (start + z, *where)
            total = mine[place].astype(jnp.float32) + came[inner_of(start + z, z, inner)].astype(jnp.float32)
            mine[place] = total.astype(mine.dtype)
            return carry

        lax.fori_loop(0, size * 2 ** len(left), body, 0)

    def launch(t, stage):
        mine, came_core, came_far, came_seq = buffers(t)
        if stage == 0:
            local = pltpu.make_async_copy(grads[t].at[(*everything, own[far])], mine, local_sems.at[t])
            local.start()
            sent = grads[t].at[(*everything, 1 - own[far])]
            return [copies.start(sent, came_core, "fsdp", flip(group, bits[far]))], local
        if stage <= far:
            made = []
            for part in (0, 1):
                order = orders[part]
                if stage == 1:
                    add(mine, came_core, (low[part], half), [], lambda z, at, inner: (z, *inner))
                else:
                    came = came_far[stage - 2].at[part]
                    add(mine, came, (low[part], half), order[: stage - 1], lambda z, at, inner: (at, *inner))
                dim = order[stage - 1]
                where = [slice(None)] * far
                for d in order[: stage - 1]:
                    where[d] = own[d]
                where[dim] = 1 - own[dim]
                made.append(
                    copies.start(
                        mine.at[(pl.ds(low[part], half), *where)],
                        came_far[stage - 1].at[part],
                        "fsdp",
                        flip(group, bits[dim]),
                    )
                )
            return made, None
        for part in (0, 1):
            came = came_far[far - 1].at[part]
            add(mine, came, (low[part], half), orders[part], lambda z, at, inner: (at,))
        made = []
        for k in range(1, length):
            other = flip_all(seq, k)
            made.append(copies.start(mine.at[(other, *own[:far])], came_seq.at[k - 1], "seq", other))
        return made, None

    def close(t):
        mine, _, _, came_seq = buffers(t)
        total = mine[(seq, *own[:far])].astype(jnp.float32)
        for k in range(1, length):
            total = total + came_seq[k - 1].astype(jnp.float32)
        outs[t][...] = total

    for step in range(count + stages):
        for t in range(count):
            stage = step - t
            if 0 < stage <= stages:
                made, local = waiting[t]
                for copy in made:
                    copy.wait_recv()
                if local is not None:
                    local.wait()
            if 0 <= stage < stages:
                waiting[t] = launch(t, stage)
            elif stage == stages:
                close(t)
    copies.finish()


def scatter_dense(grads, collective_id):
    length, groups = lax.axis_size("seq"), lax.axis_size("fsdp")
    bits, bit = [], groups // 2
    while bit >= 1:
        bits.append(bit)
        bit //= 2
    far = len(bits) - 1
    count = len(grads)
    number = count * (1 + 2 * far + length - 1)
    size = sum(g.size * g.dtype.itemsize for g in grads)
    scratch = []
    for g in grads:
        block = g.shape[1:]
        scratch += [pltpu.VMEM((length,) + (2,) * far + block, g.dtype)] * 2
        scratch += [
            pltpu.VMEM((2, length // 2) + (2,) * (far - 1 - s) + block, g.dtype) for s in range(far)
        ]
        scratch.append(pltpu.VMEM((length - 1,) + block, g.dtype))
    return pl.pallas_call(
        functools.partial(scatter_dense_kernel, length, bits, count),
        out_shape=[jax.ShapeDtypeStruct(g.shape[1:], jnp.float32) for g in grads],
        in_specs=[pl.BlockSpec(memory_space=pl.ANY)] * count,
        out_specs=[pl.BlockSpec(memory_space=pltpu.VMEM)] * count,
        scratch_shapes=scratch
        + [
            pltpu.SemaphoreType.DMA((number,)),
            pltpu.SemaphoreType.DMA((number,)),
            pltpu.SemaphoreType.DMA((count,)),
        ],
        compiler_params=pltpu.CompilerParams(
            collective_id=collective_id, has_side_effects=True, vmem_limit_bytes=grant(scratch, 0)
        ),
        cost_estimate=pl.CostEstimate(flops=0, bytes_accessed=3 * size, transcendentals=0),
        name="scatter_dense",
    )(*[g.reshape((length,) + (2,) * len(bits) + g.shape[1:]) for g in grads])


def row_dims():
    groups = lax.axis_size("fsdp")
    dims, bit = [("seq", 1)], groups // 2
    while bit >= 1:
        dims.append(("fsdp", bit))
        bit //= 2
    return dims


def row_places(dims):
    seq, group = lax.axis_index("seq"), lax.axis_index("fsdp")
    index = {"seq": seq, "fsdp": group}
    own = [bit_of(index[axis], bit) for axis, bit in dims]
    partner = [(axis, flip(index[axis], bit)) for axis, bit in dims]
    return own, partner


def gather_rows_kernel(dims, held, rows_ref, pick_ref, slots_ref, buffer, send_sems, recv_sems, local_sem):
    own, partner = row_places(dims)
    greet(partner)
    copies = Copies(send_sems, recv_sems)
    far = len(dims) - 1
    pieces = far
    width = rows_ref.shape[2]
    capacity = slots_ref.shape[-2]

    def view(piece, done):
        where = list(own)
        for d in done:
            where[d] = slice(None)
        return buffer.at[(piece, *where)]

    local = pltpu.make_async_copy(rows_ref, buffer.at[(slice(None), *own)], local_sem)
    local.start()
    flying = []
    for piece in range(pieces):
        first = piece
        flying.append(copies.start(rows_ref.at[piece], view(piece, []), *partner[first]))
    local.wait()

    def pick_block(piece, where):
        taken = jnp.dot(
            pick_ref[tuple(where)], buffer[(piece, *where)], preferred_element_type=jnp.float32
        ).astype(slots_ref.dtype)
        for e in range(held):
            slots_ref[(e, *where, slice(None), pl.ds(piece * width, width))] = taken[
                e * capacity : (e + 1) * capacity
            ]

    def pick_all(piece, core):
        def body(i, carry):
            where, rest = [], i
            for d in range(far):
                where.append(lax.rem(lax.div(rest, 2 ** (far - 1 - d)), 2))
            pick_block(piece, where + [core])
            return carry

        lax.fori_loop(0, 2**far, body, 0)

    for stage in range(1, far + 1):
        for piece in range(pieces):
            flying[piece].wait_recv()
            order = [(piece + k) % far for k in range(far)]
            done = order[:stage]
            ref = view(piece, done)
            flying[piece] = copies.start(ref, ref, *(partner[order[stage]] if stage < far else partner[far]))
    for piece in range(pieces):
        pick_all(piece, own[far])
    for piece in range(pieces):
        flying[piece].wait_recv()
        pick_all(piece, 1 - own[far])
    copies.finish()


def gather_rows(rows, pick_low, held, collective_id):
    dims = row_dims()
    far = len(dims) - 1
    count, feat = rows.shape
    width = feat // far
    sources = 2 ** len(dims)
    capacity = pick_low.shape[1] // held
    lead = (2,) * len(dims)
    cut = rows.reshape(count, far, width).swapaxes(0, 1)
    number = far * (far + 1)
    scratch = [pltpu.VMEM((far,) + lead + (count, width), rows.dtype)]
    slots = pl.pallas_call(
        functools.partial(gather_rows_kernel, dims, held),
        out_shape=jax.ShapeDtypeStruct((held,) + lead + (capacity, feat), rows.dtype),
        in_specs=[pl.BlockSpec(memory_space=pltpu.VMEM)] * 2,
        out_specs=pl.BlockSpec(memory_space=pltpu.VMEM),
        scratch_shapes=scratch
        + [pltpu.SemaphoreType.DMA((number,)), pltpu.SemaphoreType.DMA((number,)), pltpu.SemaphoreType.DMA],
        compiler_params=pltpu.CompilerParams(
            collective_id=collective_id,
            has_side_effects=True,
            vmem_limit_bytes=grant(scratch, 12 * 2**20),
        ),
        cost_estimate=pl.CostEstimate(
            flops=2 * sources * pick_low.shape[1] * count * feat,
            bytes_accessed=6 * sources * count * feat,
            transcendentals=0,
        ),
        name="gather_rows",
    )(cut, pick_low.reshape(lead + pick_low.shape[1:]))
    return slots.reshape(held, sources * capacity, feat)


def scatter_rows_kernel(
    dims, held, slots_ref, pick_ref, out_ref, mine, other, came_core, came_far, send_sems, recv_sems
):
    own, partner = row_places(dims)
    greet(partner)
    copies = Copies(send_sems, recv_sems)
    far = len(dims) - 1
    pieces = far
    width = out_ref.shape[2]
    capacity = slots_ref.shape[-2]
    count = out_ref.shape[1]

    def spread(piece, core, target):
        def body(i, carry):
            where = [lax.rem(lax.div(i, 2 ** (far - 1 - d)), 2) for d in range(far)]
            total = jnp.zeros((count, width), jnp.float32)
            for e in range(held):
                rows = slots_ref[(e, *where, core, slice(None), pl.ds(piece * width, width))]
                chosen = pick_ref[(*where, core, pl.ds(e * capacity, capacity))]
                total = total + lax.dot_general(
                    chosen, rows, (((0,), (0,)), ((), ())), preferred_element_type=jnp.float32
                )
            target[(piece, *where)] = total.astype(target.dtype)
            return carry

        lax.fori_loop(0, 2**far, body, 0)

    flying = []
    for piece in range(pieces):
        spread(piece, 1 - own[far], other)
        flying.append(copies.start(other.at[piece], came_core.at[piece], *partner[far]))
    for piece in range(pieces):
        spread(piece, own[far], mine)

    def add_into(piece, fixed, came_view):
        left = [d for d in range(far) if d not in fixed]

        def body(i, carry):
            where, inner = [None] * far, []
            for k, d in enumerate(left):
                where[d] = lax.rem(lax.div(i, 2 ** (len(left) - 1 - k)), 2)
                inner.append(where[d])
            for d in fixed:
                where[d] = own[d]
            total = mine[(piece, *where)].astype(jnp.float32) + came_view[tuple(inner)].astype(jnp.float32)
            mine[(piece, *where)] = total.astype(mine.dtype)
            return carry

        lax.fori_loop(0, 2 ** len(left), body, 0)

    for stage in range(far):
        for piece in range(pieces):
            order = [(piece + k) % far for k in range(far)][::-1]
            fixed = order[:stage]
            flying[piece].wait_recv()
            add_into(piece, fixed, came_core.at[piece] if stage == 0 else came_far[stage - 1].at[piece])
            dim = order[stage]
            where = [slice(None)] * far
            for d in fixed:
                where[d] = own[d]
            where[dim] = 1 - own[dim]
            flying[piece] = copies.start(
                mine.at[(piece, *where)], came_far[stage].at[piece], *partner[dim]
            )
    for piece in range(pieces):
        flying[piece].wait_recv()
        out_ref[piece] = mine[(piece, *own[:far])].astype(jnp.float32) + came_far[far - 1][piece].astype(
            jnp.float32
        )
    copies.finish()


def scatter_rows(slots, pick_low, held, collective_id):
    dims = row_dims()
    far = len(dims) - 1
    count, feat = pick_low.shape[2], slots.shape[2]
    width = feat // far
    sources = 2 ** len(dims)
    capacity = pick_low.shape[1] // held
    lead = (2,) * len(dims)
    number = far * (far + 1)

    scratch = [pltpu.VMEM((far,) + (2,) * far + (count, width), slots.dtype)] * 3
    scratch += [pltpu.VMEM((far,) + (2,) * (far - 1 - s) + (count, width), slots.dtype) for s in range(far)]

    def kernel(slots_ref, pick_ref, out_ref, mine, other, came_core, *rest):
        came_far, sems = rest[:far], rest[far:]
        scatter_rows_kernel(
            dims, held, slots_ref, pick_ref, out_ref, mine, other, came_core, came_far, *sems
        )

    out = pl.pallas_call(
        kernel,
        out_shape=jax.ShapeDtypeStruct((far, count, width), jnp.float32),
        in_specs=[pl.BlockSpec(memory_space=pltpu.VMEM)] * 2,
        out_specs=pl.BlockSpec(memory_space=pltpu.VMEM),
        scratch_shapes=scratch + [pltpu.SemaphoreType.DMA((number,)), pltpu.SemaphoreType.DMA((number,))],
        compiler_params=pltpu.CompilerParams(
            collective_id=collective_id,
            has_side_effects=True,
            vmem_limit_bytes=grant(scratch, 4 * 2**20),
        ),
        cost_estimate=pl.CostEstimate(
            flops=2 * sources * pick_low.shape[1] * count * feat,
            bytes_accessed=6 * sources * count * feat,
            transcendentals=0,
        ),
        name="scatter_rows",
    )(slots.reshape((held,) + lead + (capacity, feat)), pick_low.reshape(lead + pick_low.shape[1:]))
    return out.swapaxes(0, 1).reshape(count, feat)


def block(
    tokens,
    teacher,
    valid_mask,
    segment_ids,
    routes,
    gate_weights,
    norm1_gain,
    query_weight,
    key_weight,
    value_weight,
    output_weight,
    norm2_gain,
    shared_gate_weight,
    shared_up_weight,
    shared_down_weight,
    expert_gate_weight,
    expert_up_weight,
    expert_down_weight,
):
    length, groups = lax.axis_size("seq"), lax.axis_size("fsdp")
    seq_index, group_index = lax.axis_index("seq"), lax.axis_index("fsdp")
    devices = length * groups
    tok_rows = tokens.shape[1]
    seq_len = segment_ids.shape[1]
    head_group = HEADS // KV_HEADS
    score_scale = 1.0 / math.sqrt(HEAD)
    key_width = KV_HEADS * HEAD
    query_width = HEADS * HEAD
    shared_width = shared_gate_weight.shape[1]

    lanes = 128
    gains = jnp.pad(jnp.stack([norm1_gain, norm2_gain], axis=1), ((0, 0), (0, lanes - 2)))
    qkv_full, output_full, gate_up_full, down_full, expert_gate_full = gather_dense(
        [
            jnp.concatenate([query_weight, key_weight, value_weight, gains], axis=1),
            output_weight,
            jnp.concatenate([shared_gate_weight, shared_up_weight], axis=1),
            shared_down_weight,
        ],
        expert_gate_weight,
    )

    def weight_grad(rows, grad_rows):
        grad = dot(rows, grad_rows, 0, 0).astype(BF16)
        return grad.reshape(devices, -1, grad.shape[1])

    qkv_width = query_width + 2 * key_width
    gain_plain = qkv_full[:, qkv_width : qkv_width + 2].T.astype(F32)
    qkv_full = qkv_full[:, :qkv_width]
    gain_one, gain_two = gain_plain[0], gain_plain[1]

    meta = jnp.concatenate([routes[0].T.astype(F32), gate_weights[0].T], axis=0)
    meta = after(meta, qkv_full)[None]
    for axis, bit in row_dims()[::-1]:
        came = exchange(meta, axis, bit)
        high = lax.rem(lax.div(lax.axis_index(axis), bit), 2) == 1
        meta = jnp.where(high, jnp.concatenate([came, meta]), jnp.concatenate([meta, came]))

    num_local = expert_gate_weight.shape[0]
    num_held = num_local // PAIR
    side = seq_index % PAIR

    def share(weight, k):
        return lax.dynamic_slice_in_dim(weight, (side ^ (k % PAIR)) * num_held, num_held, axis=0)

    def collect_start(weight, wait):
        sent = after(weight, *wait)
        return [exchange(share(sent, k), "seq", k) for k in range(1, length)]

    def collect_done(weight, came):
        part = weight.shape[1]
        full = jnp.zeros((num_held, length * part, weight.shape[2]), weight.dtype)
        for k, block in enumerate([share(weight, 0)] + came):
            full = lax.dynamic_update_slice(full, block, (0, (seq_index ^ k) * part, 0))
        return full

    x_float = tokens[0].astype(F32)
    normed_one = rms_norm(x_float, gain_one).astype(BF16)
    qkv_rows = dot(normed_one, qkv_full, 1, 0).astype(BF16)
    query_rows = qkv_rows[:, :query_width]
    key_value = [qkv_rows[:, query_width:]]
    longest = seq_len // 2
    back = min(length - 1, -(-(longest - 1) // tok_rows))
    for _ in range(back):
        key_value.insert(0, shift(key_value[0], "seq", 1))
    key_value_all = jnp.concatenate(key_value, axis=0)
    up_came = collect_start(expert_up_weight, [key_value_all])
    window = (back + 1) * tok_rows
    seg_padded = jnp.concatenate([jnp.full((back * tok_rows,), -1, jnp.int32), segment_ids[0]])
    seg_keys = lax.dynamic_slice_in_dim(seg_padded, seq_index * tok_rows, window)
    seg_here = seg_keys[back * tok_rows :]
    positions = back * tok_rows + jnp.arange(tok_rows, dtype=jnp.int32)
    key_positions = jnp.arange(window, dtype=jnp.int32)
    allowed = (key_positions[None, :] <= positions[:, None]) & (seg_keys[None, :] == seg_here[:, None])
    query_heads = query_rows.reshape(tok_rows, KV_HEADS, head_group, HEAD)
    key_heads = key_value_all[:, :key_width].reshape(window, KV_HEADS, HEAD)
    value_heads = key_value_all[:, key_width:].reshape(window, KV_HEADS, HEAD)

    def all_scores():
        raw_scores = jnp.einsum(
            "thgd,jhd->hgtj", query_heads, key_heads, preferred_element_type=F32
        )
        return jnp.where(allowed[None, None], raw_scores * score_scale, MASKED)

    scores = all_scores()
    log_total = jax.nn.logsumexp(scores, axis=-1, keepdims=True)
    prob_low = jnp.exp(scores - log_total).astype(BF16)
    attended = (
        jnp.einsum("hgtj,jhd->thgd", prob_low, value_heads, preferred_element_type=F32)
        .reshape(tok_rows, query_width)
        .astype(BF16)
    )
    mixed_rows = x_float + dot(attended, output_full, 1, 0)
    normed_two = rms_norm(mixed_rows, gain_two).astype(BF16)

    experts_all = num_local * groups
    capacity = tok_rows * TOP * 4 // (3 * experts_all)
    route_all, gate_all = meta[:, :TOP], meta[:, TOP:]
    held_ids = group_index * num_local + side * num_held + jnp.arange(num_held, dtype=jnp.int32)
    named = route_all[:, None] == held_ids.astype(F32)[None, :, None, None]
    has = jnp.any(named, axis=2)
    gate_of = jnp.sum(jnp.where(named, gate_all[:, None], 0.0), axis=2)
    token_order = jnp.arange(tok_rows, dtype=jnp.int32)
    earlier = (token_order[:, None] < token_order[None, :]).astype(BF16)
    before = lax.dot_general(
        has.astype(BF16), earlier, (((2,), (0,)), ((), ())), preferred_element_type=F32
    )
    slot_number = jnp.arange(capacity, dtype=F32)
    chosen = has[:, :, None] & (before[:, :, None] == slot_number[None, None, :, None])
    gate_slots = jnp.sum(jnp.where(chosen, gate_of[:, :, None], 0.0), axis=3)
    sources = PAIR * groups
    chosen_low = chosen.astype(BF16).reshape(sources, num_held * capacity, tok_rows)
    gate_canonical = jnp.moveaxis(gate_slots, 0, 1).reshape(num_held, sources * capacity, 1)
    down_came = collect_start(expert_down_weight, [normed_two])
    slot_rows = gather_rows(normed_two, chosen_low, num_held, 1)

    gate_up = dot(normed_two, gate_up_full, 1, 0)
    shared_gate, shared_up = gate_up[:, :shared_width], gate_up[:, shared_width:]
    shared_hidden = swiglu(shared_gate, shared_up).astype(BF16)
    shared_out = dot(shared_hidden, down_full, 1, 0)
    expert_gate_rows = batch_dot(slot_rows, expert_gate_full, 2, 1)
    up_came = [after(came, shared_out) for came in up_came]
    expert_up_full = collect_done(expert_up_weight, up_came)
    expert_up_rows = batch_dot(slot_rows, expert_up_full, 2, 1)
    expert_hidden = swiglu(expert_gate_rows, expert_up_rows).astype(BF16)
    expert_down_full = collect_done(
        expert_down_weight, [after(came, expert_hidden) for came in down_came]
    )
    expert_output = (gate_canonical * batch_dot(expert_hidden, expert_down_full, 2, 1)).astype(BF16)
    routed = scatter_rows(expert_output, chosen_low, num_held, 2)

    output = mixed_rows + shared_out + routed
    block_output = output.astype(BF16)
    valid_rows = valid_mask[0].astype(F32)[:, None]
    grad_out = valid_rows * (output - teacher[0].astype(F32))
    grad_low = grad_out.astype(BF16)

    grad_slots = gather_rows(grad_low, chosen_low, num_held, 3)
    grad_slots = (gate_canonical * grad_slots.astype(F32)).astype(BF16)

    def expert_grad(left, right, wait):
        grad = after(batch_dot(left, right, 1, 1).astype(BF16), *wait)
        rows = grad.shape[1] // length
        own = [None] * length
        for k in range(length):
            slab = lax.dynamic_slice_in_dim(grad, (seq_index ^ k) * rows, rows, axis=1)
            own[k] = exchange(slab, "seq", k) if k else slab
        return own

    def expert_sum(own, wait):
        own = [after(part, *wait).astype(F32) for part in own]
        same = sum(own[k] for k in range(0, length, PAIR))
        crossed = sum(own[k] for k in range(1, length, PAIR))
        return jnp.concatenate(
            [jnp.where(side == 0, same, crossed), jnp.where(side == 0, crossed, same)], axis=0
        )

    expert_down_own = expert_grad(expert_hidden, grad_slots, [])
    grad_hidden = batch_dot(grad_slots, expert_down_full, 2, 2)
    grad_gate_rows, grad_up_rows = swiglu_backward(expert_gate_rows, expert_up_rows, grad_hidden)
    grad_input = (
        batch_dot(grad_gate_rows, expert_gate_full, 2, 2) + batch_dot(grad_up_rows, expert_up_full, 2, 2)
    ).astype(BF16)
    grad_routed = scatter_rows(grad_input, chosen_low, num_held, 4)
    expert_gate_own = expert_grad(slot_rows, grad_gate_rows, [grad_routed])
    expert_up_own = expert_grad(slot_rows, grad_up_rows, [grad_routed])

    grad_shidden = dot(grad_low, down_full, 1, 1)
    grad_sgate_rows, grad_sup_rows = swiglu_backward(shared_gate, shared_up, grad_shidden)
    grad_gate_up = jnp.concatenate([grad_sgate_rows, grad_sup_rows], axis=1)
    grad_normed_two = dot(grad_gate_up, gate_up_full, 1, 1) + grad_routed
    _, pull_two = jax.vjp(rms_norm, mixed_rows, gain_two)
    grad_mixed_norm, grad_gain_two = pull_two(grad_normed_two)
    grad_mixed = grad_out + grad_mixed_norm
    grad_mixed_low = grad_mixed.astype(BF16)

    grad_attended = dot(grad_mixed_low, output_full, 1, 1).astype(BF16)
    grad_att_heads = grad_attended.reshape(tok_rows, KV_HEADS, head_group, HEAD)
    prob_full = jnp.exp(all_scores() - log_total)
    prob_back = prob_full.astype(BF16)
    grad_prob = jnp.einsum(
        "thgd,jhd->hgtj", grad_att_heads, value_heads, preferred_element_type=F32
    )
    grad_values = jnp.einsum(
        "hgtj,thgd->jhd", prob_back, grad_att_heads, preferred_element_type=F32
    ).reshape(window, key_width)
    row_delta = jnp.sum(prob_full * grad_prob, axis=-1, keepdims=True)
    grad_scores = (prob_full * (grad_prob - row_delta)).astype(BF16)
    grad_query = (
        (
            jnp.einsum("hgtj,jhd->thgd", grad_scores, key_heads, preferred_element_type=F32)
            * score_scale
        )
        .reshape(tok_rows, query_width)
        .astype(BF16)
    )
    grad_keys = (
        jnp.einsum("hgtj,thgd->jhd", grad_scores, query_heads, preferred_element_type=F32)
        * score_scale
    ).reshape(window, key_width)
    grad_key_value = jnp.concatenate([grad_keys, grad_values], axis=1)
    total = grad_key_value[:tok_rows]
    for step in range(1, back + 1):
        came = shift(total.astype(BF16), "seq", -1)
        total = came.astype(F32) + grad_key_value[step * tok_rows : (step + 1) * tok_rows]
    grad_qkv = jnp.concatenate([grad_query, total.astype(BF16)], axis=1)
    grad_normed_one = dot(grad_qkv, qkv_full, 1, 1)
    _, pull_one = jax.vjp(rms_norm, x_float, gain_one)
    grad_x_norm, grad_gain_one = pull_one(grad_normed_one)
    grad_tokens = grad_mixed + grad_x_norm

    gain_grads = jnp.stack([grad_gain_one, grad_gain_two]).reshape(2, devices, -1).swapaxes(0, 1)
    gain_rows = gain_grads.shape[2]
    gain_grads = jnp.pad(gain_grads, ((0, 0), (0, 6), (0, lanes - gain_rows)))
    grad_gate_up_block, grad_qkv_block, grad_output_block, grad_down_block, grad_gain_block = scatter_dense(
        [
            weight_grad(normed_two, grad_gate_up),
            weight_grad(normed_one, grad_qkv),
            weight_grad(attended, grad_mixed_low),
            weight_grad(shared_hidden, grad_low),
            gain_grads,
        ],
        5,
    )
    last = [grad_gain_block]
    grad_expert_down = expert_sum(expert_down_own, last)
    grad_expert_gate = expert_sum(expert_gate_own, last)
    grad_expert_up = expert_sum(expert_up_own, last)
    return (
        block_output[None],
        grad_tokens[None],
        grad_gain_block[0, :gain_rows],
        grad_qkv_block[:, :query_width],
        grad_qkv_block[:, query_width : query_width + key_width],
        grad_qkv_block[:, query_width + key_width :],
        grad_output_block,
        grad_gain_block[1, :gain_rows],
        grad_gate_up_block[:, :shared_width],
        grad_gate_up_block[:, shared_width:],
        grad_down_block,
        grad_expert_gate,
        grad_expert_up,
        grad_expert_down,
    )


def solution(mesh):
    rows = P("fsdp", "seq", None)
    dense = P(("seq", "fsdp"), None)
    gain = P(("seq", "fsdp"))
    return jax.shard_map(
        block,
        mesh=mesh,
        in_specs=(
            rows, rows, P("fsdp", "seq"), P("fsdp", None), rows, rows,
            gain, dense, dense, dense, dense, gain, dense, dense, dense, rows, rows, rows,
        ),
        out_specs=(
            rows, rows, gain, dense, dense, dense, dense, gain, dense, dense, dense, rows, rows, rows,
        ),
        check_vma=False,
    )
```

```python
import functools
import math

import jax
import jax.numpy as jnp
from jax import lax
from jax.experimental import pallas as pl
from jax.experimental.pallas import tpu as pltpu
from jax.sharding import PartitionSpec as P


HEADS = 12
KV_HEADS = 4
HEAD = 128
TOP = 6
EPSILON = 1e-05
MASKED = -1e30
PAIR = 2


BF16 = jnp.bfloat16
F32 = jnp.float32


def exchange(values, axis, bit):
    count = lax.axis_size(axis)
    return lax.ppermute(values, axis, [(i, i ^ bit) for i in range(count)])


def shift(values, axis, step):
    count = lax.axis_size(axis)
    pairs = [(i, i + step) for i in range(count) if 0 <= i + step < count]
    return lax.ppermute(values, axis, pairs)


def after(values, *others):
    return lax.optimization_barrier((values, *others))[0]


def dot(left, right, left_dim, right_dim):
    return lax.dot_general(
        left, right, (((left_dim,), (right_dim,)), ((), ())), preferred_element_type=F32
    )


def batch_dot(left, right, left_dim, right_dim):
    return lax.dot_general(
        left, right, (((left_dim,), (right_dim,)), ((0,), (0,))), preferred_element_type=F32
    )


def rms_norm(values, gain):
    factor = lax.rsqrt(jnp.mean(values * values, axis=-1, keepdims=True) + EPSILON)
    return values * factor * gain


def swiglu(gate_rows, up_rows):
    return jax.nn.silu(gate_rows) * up_rows


def swiglu_backward(gate_rows, up_rows, grad_rows):
    _, pull_back = jax.vjp(swiglu, gate_rows, up_rows)
    grad_gate, grad_up = pull_back(grad_rows)
    return (grad_gate.astype(BF16), grad_up.astype(BF16))


MESH = pl.DeviceIdType.MESH


def grant(scratch, extra):
    size = extra
    for ref in scratch:
        shape = list(ref.shape)
        shape[-2] = -(-shape[-2] // 16) * 16
        size += math.prod(shape) * jnp.dtype(ref.dtype).itemsize
    return min(size + 6 * 2**20, 66 * 10**6)


class Copies:
    def __init__(self, send_sems, recv_sems):
        self.send_sems, self.recv_sems, self.made = send_sems, recv_sems, []

    def start(self, source, target, axis, partner):
        number = len(self.made)
        copy = pltpu.make_async_remote_copy(
            src_ref=source,
            dst_ref=target,
            send_sem=self.send_sems.at[number],
            recv_sem=self.recv_sems.at[number],
            device_id={axis: partner},
            device_id_type=MESH,
        )
        copy.start()
        self.made.append(copy)
        return copy

    def finish(self):
        for copy in self.made:
            copy.wait_send()


def greet(partners):
    barrier = pltpu.get_barrier_semaphore()
    for axis, partner in partners:
        pl.semaphore_signal(barrier, inc=1, device_id={axis: partner}, device_id_type=MESH)
    pl.semaphore_wait(barrier, len(partners))


def bit_of(index, bit):
    return lax.rem(lax.div(index, bit), 2)


def flip(index, bit):
    return index + bit - 2 * bit * bit_of(index, bit)


def flip_all(index, mask):
    bit = 1
    while bit <= mask:
        if mask & bit:
            index = flip(index, bit)
        bit *= 2
    return index


def gather_dense_kernel(length, bits, count, *refs):
    shards, expert, outs, expert_full = refs[:count], refs[count], refs[count + 1 : 2 * count + 1], refs[2 * count + 1]
    send_sems, recv_sems, local_sems = refs[2 * count + 2 :]
    seq, group = lax.axis_index("seq"), lax.axis_index("fsdp")
    own = [bit_of(group, bit) for bit in bits]
    partners = [("seq", flip_all(seq, k)) for k in range(1, length)]
    partners += [("fsdp", flip(group, bit)) for bit in bits]
    greet(partners)
    copies = Copies(send_sems, recv_sems)
    far = len(bits) - 1
    half = length // 2
    side = lax.div(seq, half)
    low = [side * half, (1 - side) * half]
    orders = [list(range(far)), list(range(far))[::-1]]
    stages = far + 2
    waiting = [None] * count

    def launch(t, stage):
        if stage == 0:
            local = pltpu.make_async_copy(shards[t], outs[t].at[(seq, *own)], local_sems.at[t])
            local.start()
            made = [
                copies.start(shards[t], outs[t].at[(seq, *own)], "seq", flip_all(seq, k))
                for k in range(1, length)
            ]
            return made, local
        made = []
        for part in (0, 1):
            where = [pl.ds(low[part], half)] + list(own)
            for done in orders[part][: stage - 1]:
                where[1 + done] = slice(None)
            dim = orders[part][stage - 1] if stage <= far else far
            view = outs[t].at[tuple(where)]
            made.append(copies.start(view, view, "fsdp", flip(group, bits[dim])))
        return made, None

    def ship_expert():
        held, depth = expert.shape[0] // PAIR, expert.shape[1]
        rows = pl.ds(pl.multiple_of(seq * depth, depth), depth)
        parity = lax.rem(seq, PAIR)
        local = pltpu.make_async_copy(
            expert.at[pl.ds(parity * held, held)], expert_full.at[:, rows], local_sems.at[count]
        )
        local.start()
        made = []
        for k in range(1, length):
            other = lax.rem(parity + k, PAIR)
            made.append(
                copies.start(
                    expert.at[pl.ds(other * held, held)], expert_full.at[:, rows], "seq", flip_all(seq, k)
                )
            )
        return made, local

    for step in range(count + stages):
        if step == count:
            expert_waiting = ship_expert()
        for t in range(count):
            stage = step - t
            if 0 < stage <= stages and waiting[t]:
                made, local = waiting[t]
                for copy in made:
                    copy.wait_recv()
                if local is not None:
                    local.wait()
                waiting[t] = None
            if 0 <= stage < stages:
                waiting[t] = launch(t, stage)
    made, local = expert_waiting
    for copy in made:
        copy.wait_recv()
    local.wait()
    copies.finish()


def gather_dense(shards, expert):
    length, groups = lax.axis_size("seq"), lax.axis_size("fsdp")
    bits, bit = [], groups // 2
    while bit >= 1:
        bits.append(bit)
        bit //= 2
    count = len(shards)
    number = count * (length - 1 + 2 * len(bits)) + length - 1
    size = sum(s.size * s.dtype.itemsize for s in shards) * length * groups
    experts, depth, wide = expert.shape
    *outs, expert_full = pl.pallas_call(
        functools.partial(gather_dense_kernel, length, bits, count),
        out_shape=[
            jax.ShapeDtypeStruct((length,) + (2,) * len(bits) + s.shape, s.dtype) for s in shards
        ]
        + [jax.ShapeDtypeStruct((experts // PAIR, length * depth, wide), expert.dtype)],
        in_specs=[pl.BlockSpec(memory_space=pltpu.VMEM)] * count + [pl.BlockSpec(memory_space=pl.ANY)],
        out_specs=[pl.BlockSpec(memory_space=pl.ANY)] * (count + 1),
        scratch_shapes=[
            pltpu.SemaphoreType.DMA((number,)),
            pltpu.SemaphoreType.DMA((number,)),
            pltpu.SemaphoreType.DMA((count + 1,)),
        ],
        compiler_params=pltpu.CompilerParams(
            collective_id=0, has_side_effects=True, vmem_limit_bytes=60 * 2**20
        ),
        cost_estimate=pl.CostEstimate(flops=0, bytes_accessed=3 * size, transcendentals=0),
        name="gather_dense",
    )(*shards, expert)
    return [out.reshape(-1, out.shape[-1]) for out in outs] + [expert_full]


def scatter_dense_kernel(length, bits, count, *refs):
    grads, outs = refs[:count], refs[count : 2 * count]
    far = len(bits) - 1
    per = 3 + far
    scratch = refs[2 * count : 2 * count + per * count]
    send_sems, recv_sems, local_sems = refs[2 * count + per * count :]
    seq, group = lax.axis_index("seq"), lax.axis_index("fsdp")
    own = [bit_of(group, bit) for bit in bits]
    partners = [("seq", flip_all(seq, k)) for k in range(1, length)]
    partners += [("fsdp", flip(group, bit)) for bit in bits]
    greet(partners)
    copies = Copies(send_sems, recv_sems)
    half = length // 2
    side = lax.div(seq, half)
    low = [side * half, (1 - side) * half]
    orders = [list(range(far))[::-1], list(range(far))]
    stages = far + 2
    everything = (slice(None),) * (1 + far)

    def buffers(t):
        held = scratch[per * t : per * (t + 1)]
        return held[0], held[1], held[2 : 2 + far], held[2 + far]

    waiting = [None] * count

    def add(mine, came, lead, fixed, inner_of):
        start, size = lead
        left = [d for d in range(far) if d not in fixed]

        def body(i, carry):
            z = lax.div(i, 2 ** len(left))
            where, inner = [own[d] for d in range(far)], []
            for k, d in enumerate(left):
                where[d] = lax.rem(lax.div(i, 2 ** (len(left) - 1 - k)), 2)
                inner.append(where[d])
            place = (start + z, *where)
            total = mine[place].astype(jnp.float32) + came[inner_of(start + z, z, inner)].astype(jnp.float32)
            mine[place] = total.astype(mine.dtype)
            return carry

        lax.fori_loop(0, size * 2 ** len(left), body, 0)

    def launch(t, stage):
        mine, came_core, came_far, came_seq = buffers(t)
        if stage == 0:
            local = pltpu.make_async_copy(grads[t].at[(*everything, own[far])], mine, local_sems.at[t])
            local.start()
            sent = grads[t].at[(*everything, 1 - own[far])]
            return [copies.start(sent, came_core, "fsdp", flip(group, bits[far]))], local
        if stage <= far:
            made = []
            for part in (0, 1):
                order = orders[part]
                if stage == 1:
                    add(mine, came_core, (low[part], half), [], lambda z, at, inner: (z, *inner))
                else:
                    came = came_far[stage - 2].at[part]
                    add(mine, came, (low[part], half), order[: stage - 1], lambda z, at, inner: (at, *inner))
                dim = order[stage - 1]
                where = [slice(None)] * far
                for d in order[: stage - 1]:
                    where[d] = own[d]
                where[dim] = 1 - own[dim]
                made.append(
                    copies.start(
                        mine.at[(pl.ds(low[part], half), *where)],
                        came_far[stage - 1].at[part],
                        "fsdp",
                        flip(group, bits[dim]),
                    )
                )
            return made, None
        for part in (0, 1):
            came = came_far[far - 1].at[part]
            add(mine, came, (low[part], half), orders[part], lambda z, at, inner: (at,))
        made = []
        for k in range(1, length):
            other = flip_all(seq, k)
            made.append(copies.start(mine.at[(other, *own[:far])], came_seq.at[k - 1], "seq", other))
        return made, None

    def close(t):
        mine, _, _, came_seq = buffers(t)
        total = mine[(seq, *own[:far])].astype(jnp.float32)
        for k in range(1, length):
            total = total + came_seq[k - 1].astype(jnp.float32)
        outs[t][...] = total

    for step in range(count + stages):
        for t in range(count):
            stage = step - t
            if 0 < stage <= stages:
                made, local = waiting[t]
                for copy in made:
                    copy.wait_recv()
                if local is not None:
                    local.wait()
            if 0 <= stage < stages:
                waiting[t] = launch(t, stage)
            elif stage == stages:
                close(t)
    copies.finish()


def scatter_dense(grads, collective_id):
    length, groups = lax.axis_size("seq"), lax.axis_size("fsdp")
    bits, bit = [], groups // 2
    while bit >= 1:
        bits.append(bit)
        bit //= 2
    far = len(bits) - 1
    count = len(grads)
    number = count * (1 + 2 * far + length - 1)
    size = sum(g.size * g.dtype.itemsize for g in grads)
    scratch = []
    for g in grads:
        block = g.shape[1:]
        scratch += [pltpu.VMEM((length,) + (2,) * far + block, g.dtype)] * 2
        scratch += [
            pltpu.VMEM((2, length // 2) + (2,) * (far - 1 - s) + block, g.dtype) for s in range(far)
        ]
        scratch.append(pltpu.VMEM((length - 1,) + block, g.dtype))
    return pl.pallas_call(
        functools.partial(scatter_dense_kernel, length, bits, count),
        out_shape=[jax.ShapeDtypeStruct(g.shape[1:], jnp.float32) for g in grads],
        in_specs=[pl.BlockSpec(memory_space=pl.ANY)] * count,
        out_specs=[pl.BlockSpec(memory_space=pltpu.VMEM)] * count,
        scratch_shapes=scratch
        + [
            pltpu.SemaphoreType.DMA((number,)),
            pltpu.SemaphoreType.DMA((number,)),
            pltpu.SemaphoreType.DMA((count,)),
        ],
        compiler_params=pltpu.CompilerParams(
            collective_id=collective_id, has_side_effects=True, vmem_limit_bytes=grant(scratch, 0)
        ),
        cost_estimate=pl.CostEstimate(flops=0, bytes_accessed=3 * size, transcendentals=0),
        name="scatter_dense",
    )(*[g.reshape((length,) + (2,) * len(bits) + g.shape[1:]) for g in grads])


def row_dims():
    groups = lax.axis_size("fsdp")
    dims, bit = [("seq", 1)], groups // 2
    while bit >= 1:
        dims.append(("fsdp", bit))
        bit //= 2
    return dims


def row_places(dims):
    seq, group = lax.axis_index("seq"), lax.axis_index("fsdp")
    index = {"seq": seq, "fsdp": group}
    own = [bit_of(index[axis], bit) for axis, bit in dims]
    partner = [(axis, flip(index[axis], bit)) for axis, bit in dims]
    return own, partner


def gather_rows_kernel(dims, held, rows_ref, pick_ref, slots_ref, buffer, send_sems, recv_sems, local_sem):
    own, partner = row_places(dims)
    greet(partner)
    copies = Copies(send_sems, recv_sems)
    far = len(dims) - 1
    pieces = far
    width = rows_ref.shape[2]
    capacity = slots_ref.shape[-2]

    def view(piece, done):
        where = list(own)
        for d in done:
            where[d] = slice(None)
        return buffer.at[(piece, *where)]

    local = pltpu.make_async_copy(rows_ref, buffer.at[(slice(None), *own)], local_sem)
    local.start()
    flying = []
    for piece in range(pieces):
        first = piece
        flying.append(copies.start(rows_ref.at[piece], view(piece, []), *partner[first]))
    local.wait()

    def pick_block(piece, where):
        taken = jnp.dot(
            pick_ref[tuple(where)], buffer[(piece, *where)], preferred_element_type=jnp.float32
        ).astype(slots_ref.dtype)
        for e in range(held):
            slots_ref[(e, *where, slice(None), pl.ds(piece * width, width))] = taken[
                e * capacity : (e + 1) * capacity
            ]

    def pick_all(piece, core):
        def body(i, carry):
            where, rest = [], i
            for d in range(far):
                where.append(lax.rem(lax.div(rest, 2 ** (far - 1 - d)), 2))
            pick_block(piece, where + [core])
            return carry

        lax.fori_loop(0, 2**far, body, 0)

    for stage in range(1, far + 1):
        for piece in range(pieces):
            flying[piece].wait_recv()
            order = [(piece + k) % far for k in range(far)]
            done = order[:stage]
            ref = view(piece, done)
            flying[piece] = copies.start(ref, ref, *(partner[order[stage]] if stage < far else partner[far]))
    for piece in range(pieces):
        pick_all(piece, own[far])
    for piece in range(pieces):
        flying[piece].wait_recv()
        pick_all(piece, 1 - own[far])
    copies.finish()


def gather_rows(rows, pick_low, held, collective_id):
    dims = row_dims()
    far = len(dims) - 1
    count, feat = rows.shape
    width = feat // far
    sources = 2 ** len(dims)
    capacity = pick_low.shape[1] // held
    lead = (2,) * len(dims)
    cut = rows.reshape(count, far, width).swapaxes(0, 1)
    number = far * (far + 1)
    scratch = [pltpu.VMEM((far,) + lead + (count, width), rows.dtype)]
    slots = pl.pallas_call(
        functools.partial(gather_rows_kernel, dims, held),
        out_shape=jax.ShapeDtypeStruct((held,) + lead + (capacity, feat), rows.dtype),
        in_specs=[pl.BlockSpec(memory_space=pltpu.VMEM)] * 2,
        out_specs=pl.BlockSpec(memory_space=pltpu.VMEM),
        scratch_shapes=scratch
        + [pltpu.SemaphoreType.DMA((number,)), pltpu.SemaphoreType.DMA((number,)), pltpu.SemaphoreType.DMA],
        compiler_params=pltpu.CompilerParams(
            collective_id=collective_id,
            has_side_effects=True,
            vmem_limit_bytes=grant(scratch, 12 * 2**20),
        ),
        cost_estimate=pl.CostEstimate(
            flops=2 * sources * pick_low.shape[1] * count * feat,
            bytes_accessed=6 * sources * count * feat,
            transcendentals=0,
        ),
        name="gather_rows",
    )(cut, pick_low.reshape(lead + pick_low.shape[1:]))
    return slots.reshape(held, sources * capacity, feat)


def scatter_rows_kernel(
    dims, held, slots_ref, pick_ref, out_ref, mine, other, came_core, came_far, send_sems, recv_sems
):
    own, partner = row_places(dims)
    greet(partner)
    copies = Copies(send_sems, recv_sems)
    far = len(dims) - 1
    pieces = far
    width = out_ref.shape[2]
    capacity = slots_ref.shape[-2]
    count = out_ref.shape[1]

    def spread(piece, core, target):
        def body(i, carry):
            where = [lax.rem(lax.div(i, 2 ** (far - 1 - d)), 2) for d in range(far)]
            total = jnp.zeros((count, width), jnp.float32)
            for e in range(held):
                rows = slots_ref[(e, *where, core, slice(None), pl.ds(piece * width, width))]
                chosen = pick_ref[(*where, core, pl.ds(e * capacity, capacity))]
                total = total + lax.dot_general(
                    chosen, rows, (((0,), (0,)), ((), ())), preferred_element_type=jnp.float32
                )
            target[(piece, *where)] = total.astype(target.dtype)
            return carry

        lax.fori_loop(0, 2**far, body, 0)

    flying = []
    for piece in range(pieces):
        spread(piece, 1 - own[far], other)
        flying.append(copies.start(other.at[piece], came_core.at[piece], *partner[far]))
    for piece in range(pieces):
        spread(piece, own[far], mine)

    def add_into(piece, fixed, came_view):
        left = [d for d in range(far) if d not in fixed]

        def body(i, carry):
            where, inner = [None] * far, []
            for k, d in enumerate(left):
                where[d] = lax.rem(lax.div(i, 2 ** (len(left) - 1 - k)), 2)
                inner.append(where[d])
            for d in fixed:
                where[d] = own[d]
            total = mine[(piece, *where)].astype(jnp.float32) + came_view[tuple(inner)].astype(jnp.float32)
            mine[(piece, *where)] = total.astype(mine.dtype)
            return carry

        lax.fori_loop(0, 2 ** len(left), body, 0)

    for stage in range(far):
        for piece in range(pieces):
            order = [(piece + k) % far for k in range(far)][::-1]
            fixed = order[:stage]
            flying[piece].wait_recv()
            add_into(piece, fixed, came_core.at[piece] if stage == 0 else came_far[stage - 1].at[piece])
            dim = order[stage]
            where = [slice(None)] * far
            for d in fixed:
                where[d] = own[d]
            where[dim] = 1 - own[dim]
            flying[piece] = copies.start(
                mine.at[(piece, *where)], came_far[stage].at[piece], *partner[dim]
            )
    for piece in range(pieces):
        flying[piece].wait_recv()
        out_ref[piece] = mine[(piece, *own[:far])].astype(jnp.float32) + came_far[far - 1][piece].astype(
            jnp.float32
        )
    copies.finish()


def scatter_rows(slots, pick_low, held, collective_id):
    dims = row_dims()
    far = len(dims) - 1
    count, feat = pick_low.shape[2], slots.shape[2]
    width = feat // far
    sources = 2 ** len(dims)
    capacity = pick_low.shape[1] // held
    lead = (2,) * len(dims)
    number = far * (far + 1)

    scratch = [pltpu.VMEM((far,) + (2,) * far + (count, width), slots.dtype)] * 3
    scratch += [pltpu.VMEM((far,) + (2,) * (far - 1 - s) + (count, width), slots.dtype) for s in range(far)]

    def kernel(slots_ref, pick_ref, out_ref, mine, other, came_core, *rest):
        came_far, sems = rest[:far], rest[far:]
        scatter_rows_kernel(
            dims, held, slots_ref, pick_ref, out_ref, mine, other, came_core, came_far, *sems
        )

    out = pl.pallas_call(
        kernel,
        out_shape=jax.ShapeDtypeStruct((far, count, width), jnp.float32),
        in_specs=[pl.BlockSpec(memory_space=pltpu.VMEM)] * 2,
        out_specs=pl.BlockSpec(memory_space=pltpu.VMEM),
        scratch_shapes=scratch + [pltpu.SemaphoreType.DMA((number,)), pltpu.SemaphoreType.DMA((number,))],
        compiler_params=pltpu.CompilerParams(
            collective_id=collective_id,
            has_side_effects=True,
            vmem_limit_bytes=grant(scratch, 4 * 2**20),
        ),
        cost_estimate=pl.CostEstimate(
            flops=2 * sources * pick_low.shape[1] * count * feat,
            bytes_accessed=6 * sources * count * feat,
            transcendentals=0,
        ),
        name="scatter_rows",
    )(slots.reshape((held,) + lead + (capacity, feat)), pick_low.reshape(lead + pick_low.shape[1:]))
    return out.swapaxes(0, 1).reshape(count, feat)


def block(
    tokens,
    teacher,
    valid_mask,
    segment_ids,
    routes,
    gate_weights,
    norm1_gain,
    query_weight,
    key_weight,
    value_weight,
    output_weight,
    norm2_gain,
    shared_gate_weight,
    shared_up_weight,
    shared_down_weight,
    expert_gate_weight,
    expert_up_weight,
    expert_down_weight,
):
    length, groups = lax.axis_size("seq"), lax.axis_size("fsdp")
    seq_index, group_index = lax.axis_index("seq"), lax.axis_index("fsdp")
    devices = length * groups
    tok_rows = tokens.shape[1]
    seq_len = segment_ids.shape[1]
    head_group = HEADS // KV_HEADS
    score_scale = 1.0 / math.sqrt(HEAD)
    key_width = KV_HEADS * HEAD
    query_width = HEADS * HEAD
    shared_width = shared_gate_weight.shape[1]

    lanes = 128
    gains = jnp.pad(jnp.stack([norm1_gain, norm2_gain], axis=1), ((0, 0), (0, lanes - 2)))
    meta = jnp.concatenate([routes[0].T.astype(F32), gate_weights[0].T], axis=0)
    meta = jnp.pad(meta, ((0, 16 - 2 * TOP), (0, 0)))
    qkv_full, meta, output_full, gate_up_full, down_full, expert_gate_full = gather_dense(
        [
            jnp.concatenate([query_weight, key_weight, value_weight, gains], axis=1),
            meta,
            output_weight,
            jnp.concatenate([shared_gate_weight, shared_up_weight], axis=1),
            shared_down_weight,
        ],
        expert_gate_weight,
    )

    def weight_grad(rows, grad_rows):
        grad = dot(rows, grad_rows, 0, 0).astype(BF16)
        return grad.reshape(devices, -1, grad.shape[1])

    qkv_width = query_width + 2 * key_width
    gain_plain = qkv_full[:, qkv_width : qkv_width + 2].T.astype(F32)
    qkv_full = qkv_full[:, :qkv_width]
    gain_one, gain_two = gain_plain[0], gain_plain[1]

    num_local = expert_gate_weight.shape[0]
    num_held = num_local // PAIR
    side = seq_index % PAIR

    def share(weight, k):
        return lax.dynamic_slice_in_dim(weight, (side ^ (k % PAIR)) * num_held, num_held, axis=0)

    def collect_start(weight, wait):
        sent = after(weight, *wait)
        return [exchange(share(sent, k), "seq", k) for k in range(1, length)]

    def collect_done(weight, came):
        part = weight.shape[1]
        full = jnp.zeros((num_held, length * part, weight.shape[2]), weight.dtype)
        for k, block in enumerate([share(weight, 0)] + came):
            full = lax.dynamic_update_slice(full, block, (0, (seq_index ^ k) * part, 0))
        return full

    x_float = tokens[0].astype(F32)
    normed_one = rms_norm(x_float, gain_one).astype(BF16)
    qkv_rows = dot(normed_one, qkv_full, 1, 0).astype(BF16)
    query_rows = qkv_rows[:, :query_width]
    key_value = [qkv_rows[:, query_width:]]
    longest = seq_len // 2
    back = min(length - 1, -(-(longest - 1) // tok_rows))
    for _ in range(back):
        key_value.insert(0, shift(key_value[0], "seq", 1))
    key_value_all = jnp.concatenate(key_value, axis=0)
    up_came = collect_start(expert_up_weight, [key_value_all])
    window = (back + 1) * tok_rows
    seg_padded = jnp.concatenate([jnp.full((back * tok_rows,), -1, jnp.int32), segment_ids[0]])
    seg_keys = lax.dynamic_slice_in_dim(seg_padded, seq_index * tok_rows, window)
    seg_here = seg_keys[back * tok_rows :]
    positions = back * tok_rows + jnp.arange(tok_rows, dtype=jnp.int32)
    key_positions = jnp.arange(window, dtype=jnp.int32)
    allowed = (key_positions[None, :] <= positions[:, None]) & (seg_keys[None, :] == seg_here[:, None])
    query_heads = query_rows.reshape(tok_rows, KV_HEADS, head_group, HEAD)
    key_heads = key_value_all[:, :key_width].reshape(window, KV_HEADS, HEAD)
    value_heads = key_value_all[:, key_width:].reshape(window, KV_HEADS, HEAD)

    def all_scores():
        raw_scores = jnp.einsum(
            "thgd,jhd->hgtj", query_heads, key_heads, preferred_element_type=F32
        )
        return jnp.where(allowed[None, None], raw_scores * score_scale, MASKED)

    scores = all_scores()
    log_total = jax.nn.logsumexp(scores, axis=-1, keepdims=True)
    prob_low = jnp.exp(scores - log_total).astype(BF16)
    attended = (
        jnp.einsum("hgtj,jhd->thgd", prob_low, value_heads, preferred_element_type=F32)
        .reshape(tok_rows, query_width)
        .astype(BF16)
    )
    mixed_rows = x_float + dot(attended, output_full, 1, 0)
    normed_two = rms_norm(mixed_rows, gain_two).astype(BF16)

    experts_all = num_local * groups
    capacity = tok_rows * TOP * 4 // (3 * experts_all)
    meta = lax.dynamic_slice_in_dim(
        meta.reshape(length, groups, 16, tok_rows), seq_index // PAIR * PAIR, PAIR, axis=0
    ).reshape(PAIR * groups, 16, tok_rows)
    route_all, gate_all = meta[:, :TOP], meta[:, TOP : 2 * TOP]
    held_ids = group_index * num_local + side * num_held + jnp.arange(num_held, dtype=jnp.int32)
    named = route_all[:, None] == held_ids.astype(F32)[None, :, None, None]
    has = jnp.any(named, axis=2)
    gate_of = jnp.sum(jnp.where(named, gate_all[:, None], 0.0), axis=2)
    token_order = jnp.arange(tok_rows, dtype=jnp.int32)
    earlier = (token_order[:, None] < token_order[None, :]).astype(BF16)
    before = lax.dot_general(
        has.astype(BF16), earlier, (((2,), (0,)), ((), ())), preferred_element_type=F32
    )
    slot_number = jnp.arange(capacity, dtype=F32)
    chosen = has[:, :, None] & (before[:, :, None] == slot_number[None, None, :, None])
    gate_slots = jnp.sum(jnp.where(chosen, gate_of[:, :, None], 0.0), axis=3)
    sources = PAIR * groups
    chosen_low = chosen.astype(BF16).reshape(sources, num_held * capacity, tok_rows)
    gate_canonical = jnp.moveaxis(gate_slots, 0, 1).reshape(num_held, sources * capacity, 1)
    down_came = collect_start(expert_down_weight, [normed_two])
    slot_rows = gather_rows(normed_two, chosen_low, num_held, 1)

    gate_up = dot(normed_two, gate_up_full, 1, 0)
    shared_gate, shared_up = gate_up[:, :shared_width], gate_up[:, shared_width:]
    shared_hidden = swiglu(shared_gate, shared_up).astype(BF16)
    shared_out = dot(shared_hidden, down_full, 1, 0)
    expert_gate_rows = batch_dot(slot_rows, expert_gate_full, 2, 1)
    up_came = [after(came, shared_out) for came in up_came]
    expert_up_full = collect_done(expert_up_weight, up_came)
    expert_up_rows = batch_dot(slot_rows, expert_up_full, 2, 1)
    expert_hidden = swiglu(expert_gate_rows, expert_up_rows).astype(BF16)
    expert_down_full = collect_done(
        expert_down_weight, [after(came, expert_hidden) for came in down_came]
    )
    expert_output = (gate_canonical * batch_dot(expert_hidden, expert_down_full, 2, 1)).astype(BF16)
    routed = scatter_rows(expert_output, chosen_low, num_held, 2)

    output = mixed_rows + shared_out + routed
    block_output = output.astype(BF16)
    valid_rows = valid_mask[0].astype(F32)[:, None]
    grad_out = valid_rows * (output - teacher[0].astype(F32))
    grad_low = grad_out.astype(BF16)

    grad_slots = gather_rows(grad_low, chosen_low, num_held, 3)
    grad_slots = (gate_canonical * grad_slots.astype(F32)).astype(BF16)

    def expert_grad(left, right, wait):
        grad = after(batch_dot(left, right, 1, 1).astype(BF16), *wait)
        rows = grad.shape[1] // length
        own = [None] * length
        for k in range(length):
            slab = lax.dynamic_slice_in_dim(grad, (seq_index ^ k) * rows, rows, axis=1)
            own[k] = exchange(slab, "seq", k) if k else slab
        return own

    def expert_sum(own, wait):
        own = [after(part, *wait).astype(F32) for part in own]
        same = sum(own[k] for k in range(0, length, PAIR))
        crossed = sum(own[k] for k in range(1, length, PAIR))
        return jnp.concatenate(
            [jnp.where(side == 0, same, crossed), jnp.where(side == 0, crossed, same)], axis=0
        )

    expert_down_own = expert_grad(expert_hidden, grad_slots, [])
    grad_hidden = batch_dot(grad_slots, expert_down_full, 2, 2)
    grad_gate_rows, grad_up_rows = swiglu_backward(expert_gate_rows, expert_up_rows, grad_hidden)
    grad_input = (
        batch_dot(grad_gate_rows, expert_gate_full, 2, 2) + batch_dot(grad_up_rows, expert_up_full, 2, 2)
    ).astype(BF16)
    grad_routed = scatter_rows(grad_input, chosen_low, num_held, 4)
    expert_gate_own = expert_grad(slot_rows, grad_gate_rows, [grad_routed])

    grad_shidden = dot(grad_low, down_full, 1, 1)
    grad_sgate_rows, grad_sup_rows = swiglu_backward(shared_gate, shared_up, grad_shidden)
    grad_gate_up = jnp.concatenate([grad_sgate_rows, grad_sup_rows], axis=1)
    grad_normed_two = dot(grad_gate_up, gate_up_full, 1, 1) + grad_routed
    _, pull_two = jax.vjp(rms_norm, mixed_rows, gain_two)
    grad_mixed_norm, grad_gain_two = pull_two(grad_normed_two)
    grad_mixed = grad_out + grad_mixed_norm
    grad_mixed_low = grad_mixed.astype(BF16)

    grad_attended = dot(grad_mixed_low, output_full, 1, 1).astype(BF16)
    grad_att_heads = grad_attended.reshape(tok_rows, KV_HEADS, head_group, HEAD)
    prob_full = jnp.exp(all_scores() - log_total)
    prob_back = prob_full.astype(BF16)
    grad_prob = jnp.einsum(
        "thgd,jhd->hgtj", grad_att_heads, value_heads, preferred_element_type=F32
    )
    grad_values = jnp.einsum(
        "hgtj,thgd->jhd", prob_back, grad_att_heads, preferred_element_type=F32
    ).reshape(window, key_width)
    row_delta = jnp.sum(prob_full * grad_prob, axis=-1, keepdims=True)
    grad_scores = (prob_full * (grad_prob - row_delta)).astype(BF16)
    grad_query = (
        (
            jnp.einsum("hgtj,jhd->thgd", grad_scores, key_heads, preferred_element_type=F32)
            * score_scale
        )
        .reshape(tok_rows, query_width)
        .astype(BF16)
    )
    grad_keys = (
        jnp.einsum("hgtj,thgd->jhd", grad_scores, query_heads, preferred_element_type=F32)
        * score_scale
    ).reshape(window, key_width)
    grad_key_value = jnp.concatenate([grad_keys, grad_values], axis=1)
    total = grad_key_value[:tok_rows]
    for step in range(1, back + 1):
        came = shift(total.astype(BF16), "seq", -1)
        total = came.astype(F32) + grad_key_value[step * tok_rows : (step + 1) * tok_rows]
    grad_qkv = jnp.concatenate([grad_query, total.astype(BF16)], axis=1)
    expert_up_own = expert_grad(slot_rows, grad_up_rows, [total])
    grad_normed_one = dot(grad_qkv, qkv_full, 1, 1)
    _, pull_one = jax.vjp(rms_norm, x_float, gain_one)
    grad_x_norm, grad_gain_one = pull_one(grad_normed_one)
    grad_tokens = grad_mixed + grad_x_norm

    gain_grads = jnp.stack([grad_gain_one, grad_gain_two]).reshape(2, devices, -1).swapaxes(0, 1)
    gain_rows = gain_grads.shape[2]
    gain_grads = jnp.pad(gain_grads, ((0, 0), (0, 6), (0, lanes - gain_rows)))
    dense_grads = [
        weight_grad(normed_two, grad_gate_up),
        weight_grad(normed_one, grad_qkv),
        weight_grad(attended, grad_mixed_low),
        weight_grad(shared_hidden, grad_low),
        gain_grads,
    ]
    sums = scatter_dense(dense_grads, 5)
    grad_gate_up_block, grad_qkv_block, grad_output_block, grad_down_block, grad_gain_block = sums
    last = [grad_gain_block]
    grad_expert_down = expert_sum(expert_down_own, last)
    grad_expert_gate = expert_sum(expert_gate_own, last)
    grad_expert_up = expert_sum(expert_up_own, last)
    return (
        block_output[None],
        grad_tokens[None],
        grad_gain_block[0, :gain_rows],
        grad_qkv_block[:, :query_width],
        grad_qkv_block[:, query_width : query_width + key_width],
        grad_qkv_block[:, query_width + key_width :],
        grad_output_block,
        grad_gain_block[1, :gain_rows],
        grad_gate_up_block[:, :shared_width],
        grad_gate_up_block[:, shared_width:],
        grad_down_block,
        grad_expert_gate,
        grad_expert_up,
        grad_expert_down,
    )


def solution(mesh):
    rows = P("fsdp", "seq", None)
    dense = P(("seq", "fsdp"), None)
    gain = P(("seq", "fsdp"))
    return jax.shard_map(
        block,
        mesh=mesh,
        in_specs=(
            rows, rows, P("fsdp", "seq"), P("fsdp", None), rows, rows,
            gain, dense, dense, dense, dense, gain, dense, dense, dense, rows, rows, rows,
        ),
        out_specs=(
            rows, rows, gain, dense, dense, dense, dense, gain, dense, dense, dense, rows, rows, rows,
        ),
        check_vma=False,
    )
```

```python
import functools
import math

import jax
import jax.numpy as jnp
from jax import lax
from jax.experimental import pallas as pl
from jax.experimental.pallas import tpu as pltpu
from jax.sharding import PartitionSpec as P


HEADS = 12
KV_HEADS = 4
HEAD = 128
TOP = 6
EPSILON = 1e-05
MASKED = -1e30
PAIR = 2


BF16 = jnp.bfloat16
F32 = jnp.float32


def exchange(values, axis, bit):
    count = lax.axis_size(axis)
    return lax.ppermute(values, axis, [(i, i ^ bit) for i in range(count)])


def shift(values, axis, step):
    count = lax.axis_size(axis)
    pairs = [(i, i + step) for i in range(count) if 0 <= i + step < count]
    return lax.ppermute(values, axis, pairs)


def after(values, *others):
    return lax.optimization_barrier((values, *others))[0]


def dot(left, right, left_dim, right_dim):
    return lax.dot_general(
        left, right, (((left_dim,), (right_dim,)), ((), ())), preferred_element_type=F32
    )


def batch_dot(left, right, left_dim, right_dim):
    return lax.dot_general(
        left, right, (((left_dim,), (right_dim,)), ((0,), (0,))), preferred_element_type=F32
    )


def rms_norm(values, gain):
    factor = lax.rsqrt(jnp.mean(values * values, axis=-1, keepdims=True) + EPSILON)
    return values * factor * gain


def swiglu(gate_rows, up_rows):
    return jax.nn.silu(gate_rows) * up_rows


def swiglu_backward(gate_rows, up_rows, grad_rows):
    _, pull_back = jax.vjp(swiglu, gate_rows, up_rows)
    grad_gate, grad_up = pull_back(grad_rows)
    return (grad_gate.astype(BF16), grad_up.astype(BF16))


MESH = pl.DeviceIdType.MESH


def grant(scratch, extra):
    size = extra
    for ref in scratch:
        shape = list(ref.shape)
        shape[-2] = -(-shape[-2] // 16) * 16
        size += math.prod(shape) * jnp.dtype(ref.dtype).itemsize
    return min(size + 6 * 2**20, 66 * 10**6)


class Copies:
    def __init__(self, send_sems, recv_sems):
        self.send_sems, self.recv_sems, self.made = send_sems, recv_sems, []

    def start(self, source, target, axis, partner):
        number = len(self.made)
        copy = pltpu.make_async_remote_copy(
            src_ref=source,
            dst_ref=target,
            send_sem=self.send_sems.at[number],
            recv_sem=self.recv_sems.at[number],
            device_id={axis: partner},
            device_id_type=MESH,
        )
        copy.start()
        self.made.append(copy)
        return copy

    def finish(self):
        for copy in self.made:
            copy.wait_send()


def greet(partners):
    barrier = pltpu.get_barrier_semaphore()
    for axis, partner in partners:
        pl.semaphore_signal(barrier, inc=1, device_id={axis: partner}, device_id_type=MESH)
    pl.semaphore_wait(barrier, len(partners))


def bit_of(index, bit):
    return lax.rem(lax.div(index, bit), 2)


def flip(index, bit):
    return index + bit - 2 * bit * bit_of(index, bit)


def flip_all(index, mask):
    bit = 1
    while bit <= mask:
        if mask & bit:
            index = flip(index, bit)
        bit *= 2
    return index


def gather_dense_kernel(length, bits, count, back, *refs):
    extra = 0 if back is None else 1
    shards, expert = refs[:count], refs[count]
    outs, expert_full = refs[count + 1 + extra : 2 * count + 1 + extra], refs[2 * count + 1 + extra]
    if back is None:
        send_sems, recv_sems, local_sems = refs[2 * count + 2 :]
        places = list(outs)
    else:
        tokens = refs[count + 1]
        normed_ref, query_ref, window_ref, held, send_sems, recv_sems, local_sems, key_sems = refs[2 * count + 3 :]
        places = [held] + list(outs[1:])
    seq, group = lax.axis_index("seq"), lax.axis_index("fsdp")
    own = [bit_of(group, bit) for bit in bits]
    partners = [("seq", flip_all(seq, k)) for k in range(1, length)]
    partners += [("fsdp", flip(group, bit)) for bit in bits]
    greet(partners)
    copies = Copies(send_sems, recv_sems)
    far = len(bits) - 1
    half = length // 2
    side = lax.div(seq, half)
    low = [side * half, (1 - side) * half]
    orders = [list(range(far)), list(range(far))[::-1]]
    stages = far + 2
    waiting = [None] * count

    def launch(t, stage):
        if stage == 0:
            local = pltpu.make_async_copy(shards[t], places[t].at[(seq, *own)], local_sems.at[t])
            local.start()
            made = [
                copies.start(shards[t], places[t].at[(seq, *own)], "seq", flip_all(seq, k))
                for k in range(1, length)
            ]
            return made, local
        made = []
        for part in (0, 1):
            where = [pl.ds(low[part], half)] + list(own)
            for done in orders[part][: stage - 1]:
                where[1 + done] = slice(None)
            dim = orders[part][stage - 1] if stage <= far else far
            view = places[t].at[tuple(where)]
            made.append(copies.start(view, view, "fsdp", flip(group, bits[dim])))
        return made, None

    def ship_expert():
        held, depth = expert.shape[0] // PAIR, expert.shape[1]
        rows = pl.ds(pl.multiple_of(seq * depth, depth), depth)
        parity = lax.rem(seq, PAIR)
        local = pltpu.make_async_copy(
            expert.at[pl.ds(parity * held, held)], expert_full.at[:, rows], local_sems.at[count]
        )
        local.start()
        made = []
        for k in range(1, length):
            other = lax.rem(parity + k, PAIR)
            made.append(
                copies.start(
                    expert.at[pl.ds(other * held, held)], expert_full.at[:, rows], "seq", flip_all(seq, k)
                )
            )
        return made, local

    def project():
        rows, width = normed_ref.shape
        query_width = query_ref.shape[1]
        key_width = window_ref.shape[1]

        def columns(start, size):
            return held[(slice(None),) * (2 + far) + (slice(None), pl.ds(start, size))].reshape(width, size)

        gain = columns(query_width + key_width, 128).astype(jnp.float32).T[0:1]
        values = tokens[...].astype(jnp.float32)
        factor = lax.rsqrt(jnp.mean(values * values, axis=-1, keepdims=True) + EPSILON)
        normed_ref[...] = (values * factor * gain).astype(normed_ref.dtype)
        here = pl.ds(back * rows, rows)
        for start in range(0, key_width, 512):
            tile = jnp.dot(
                normed_ref[...], columns(query_width + start, 512), preferred_element_type=jnp.float32
            )
            window_ref[here, pl.ds(start, 512)] = tile.astype(window_ref.dtype)
        sent = []
        for j in range(1, back + 1):
            copy = pltpu.make_async_remote_copy(
                src_ref=window_ref.at[here],
                dst_ref=window_ref.at[pl.ds((back - j) * rows, rows)],
                send_sem=key_sems.at[0, j - 1],
                recv_sem=key_sems.at[1, j - 1],
                device_id={"seq": lax.rem(seq + j, length)},
                device_id_type=MESH,
            )
            pl.when(seq + j < length)(copy.start)
            sent.append(copy)

            @pl.when(seq < j)
            def _(j=j):
                window_ref[pl.ds((back - j) * rows, rows)] = jnp.zeros((rows, key_width), window_ref.dtype)

        for start in range(0, query_width, 512):
            tile = jnp.dot(normed_ref[...], columns(start, 512), preferred_element_type=jnp.float32)
            query_ref[:, pl.ds(start, 512)] = tile.astype(query_ref.dtype)
        kept = pltpu.make_async_copy(held, outs[0], local_sems.at[0])
        kept.start()
        return sent, kept

    for step in range(count + stages):
        if step == count:
            expert_waiting = ship_expert()
        for t in range(count):
            stage = step - t
            if 0 < stage <= stages and waiting[t]:
                made, local = waiting[t]
                for copy in made:
                    copy.wait_recv()
                if local is not None:
                    local.wait()
                waiting[t] = None
            if 0 <= stage < stages:
                waiting[t] = launch(t, stage)
        if step == stages and back is not None:
            sent, kept = project()
    made, local = expert_waiting
    for copy in made:
        copy.wait_recv()
    local.wait()
    copies.finish()
    if back is not None:
        for j, copy in enumerate(sent, 1):
            pl.when(seq >= j)(copy.wait_recv)
            pl.when(seq + j < length)(copy.wait_send)
        kept.wait()


def gather_dense(shards, expert, tokens, back, key_width):
    length, groups = lax.axis_size("seq"), lax.axis_size("fsdp")
    bits, bit = [], groups // 2
    while bit >= 1:
        bits.append(bit)
        bit //= 2
    count = len(shards)
    number = count * (length - 1 + 2 * len(bits)) + length - 1
    size = sum(s.size * s.dtype.itemsize for s in shards) * length * groups
    experts, depth, wide = expert.shape
    lead = (length,) + (2,) * len(bits)
    rows, width = tokens.shape
    fused = shards[0].shape[0] % 16 == 0
    extra_in, extra_out, extra_scratch, key_scratch = [], [], [], []
    if fused:
        query_width = shards[0].shape[1] - key_width - 128
        extra_in = [tokens]
        extra_out = [
            jax.ShapeDtypeStruct((rows, width), tokens.dtype),
            jax.ShapeDtypeStruct((rows, query_width), tokens.dtype),
            jax.ShapeDtypeStruct(((back + 1) * rows, key_width), tokens.dtype),
        ]
        extra_scratch = [pltpu.VMEM(lead + shards[0].shape, shards[0].dtype)]
        key_scratch = [pltpu.SemaphoreType.DMA((2, back))]
    results = pl.pallas_call(
        functools.partial(gather_dense_kernel, length, bits, count, back if fused else None),
        out_shape=[
            jax.ShapeDtypeStruct((length,) + (2,) * len(bits) + s.shape, s.dtype) for s in shards
        ]
        + [jax.ShapeDtypeStruct((experts // PAIR, length * depth, wide), expert.dtype)]
        + extra_out,
        in_specs=[pl.BlockSpec(memory_space=pltpu.VMEM)] * count
        + [pl.BlockSpec(memory_space=pl.ANY)]
        + [pl.BlockSpec(memory_space=pltpu.VMEM)] * len(extra_in),
        out_specs=[pl.BlockSpec(memory_space=pl.ANY)] * (count + 1)
        + [pl.BlockSpec(memory_space=pltpu.VMEM)] * len(extra_out),
        scratch_shapes=extra_scratch
        + [
            pltpu.SemaphoreType.DMA((number,)),
            pltpu.SemaphoreType.DMA((number,)),
            pltpu.SemaphoreType.DMA((count + 1,)),
        ]
        + key_scratch,
        compiler_params=pltpu.CompilerParams(
            collective_id=0, has_side_effects=True, vmem_limit_bytes=60 * 2**20
        ),
        cost_estimate=pl.CostEstimate(flops=0, bytes_accessed=3 * size, transcendentals=0),
        name="gather_dense",
    )(*shards, expert, *extra_in)
    outs = [out.reshape(-1, out.shape[-1]) for out in results[:count]] + [results[count]]
    return outs + (list(results[count + 1 :]) if fused else [None] * 3)


def scatter_dense_kernel(length, bits, count, *refs):
    grads, outs = refs[:count], refs[count : 2 * count]
    far = len(bits) - 1
    per = 3 + far
    scratch = refs[2 * count : 2 * count + per * count]
    send_sems, recv_sems, local_sems = refs[2 * count + per * count :]
    seq, group = lax.axis_index("seq"), lax.axis_index("fsdp")
    own = [bit_of(group, bit) for bit in bits]
    partners = [("seq", flip_all(seq, k)) for k in range(1, length)]
    partners += [("fsdp", flip(group, bit)) for bit in bits]
    greet(partners)
    copies = Copies(send_sems, recv_sems)
    half = length // 2
    side = lax.div(seq, half)
    low = [side * half, (1 - side) * half]
    orders = [list(range(far))[::-1], list(range(far))]
    stages = far + 2
    everything = (slice(None),) * (1 + far)

    def buffers(t):
        held = scratch[per * t : per * (t + 1)]
        return held[0], held[1], held[2 : 2 + far], held[2 + far]

    waiting = [None] * count

    def add(mine, came, lead, fixed, inner_of):
        start, size = lead
        left = [d for d in range(far) if d not in fixed]

        def body(i, carry):
            z = lax.div(i, 2 ** len(left))
            where, inner = [own[d] for d in range(far)], []
            for k, d in enumerate(left):
                where[d] = lax.rem(lax.div(i, 2 ** (len(left) - 1 - k)), 2)
                inner.append(where[d])
            place = (start + z, *where)
            total = mine[place].astype(jnp.float32) + came[inner_of(start + z, z, inner)].astype(jnp.float32)
            mine[place] = total.astype(mine.dtype)
            return carry

        lax.fori_loop(0, size * 2 ** len(left), body, 0)

    def launch(t, stage):
        mine, came_core, came_far, came_seq = buffers(t)
        if stage == 0:
            local = pltpu.make_async_copy(grads[t].at[(*everything, own[far])], mine, local_sems.at[t])
            local.start()
            sent = grads[t].at[(*everything, 1 - own[far])]
            return [copies.start(sent, came_core, "fsdp", flip(group, bits[far]))], local
        if stage <= far:
            made = []
            for part in (0, 1):
                order = orders[part]
                if stage == 1:
                    add(mine, came_core, (low[part], half), [], lambda z, at, inner: (z, *inner))
                else:
                    came = came_far[stage - 2].at[part]
                    add(mine, came, (low[part], half), order[: stage - 1], lambda z, at, inner: (at, *inner))
                dim = order[stage - 1]
                where = [slice(None)] * far
                for d in order[: stage - 1]:
                    where[d] = own[d]
                where[dim] = 1 - own[dim]
                made.append(
                    copies.start(
                        mine.at[(pl.ds(low[part], half), *where)],
                        came_far[stage - 1].at[part],
                        "fsdp",
                        flip(group, bits[dim]),
                    )
                )
            return made, None
        for part in (0, 1):
            came = came_far[far - 1].at[part]
            add(mine, came, (low[part], half), orders[part], lambda z, at, inner: (at,))
        made = []
        for k in range(1, length):
            other = flip_all(seq, k)
            made.append(copies.start(mine.at[(other, *own[:far])], came_seq.at[k - 1], "seq", other))
        return made, None

    def close(t):
        mine, _, _, came_seq = buffers(t)
        total = mine[(seq, *own[:far])].astype(jnp.float32)
        for k in range(1, length):
            total = total + came_seq[k - 1].astype(jnp.float32)
        outs[t][...] = total

    for step in range(count + stages):
        for t in range(count):
            stage = step - t
            if 0 < stage <= stages:
                made, local = waiting[t]
                for copy in made:
                    copy.wait_recv()
                if local is not None:
                    local.wait()
            if 0 <= stage < stages:
                waiting[t] = launch(t, stage)
            elif stage == stages:
                close(t)
    copies.finish()


def scatter_dense(grads, collective_id):
    length, groups = lax.axis_size("seq"), lax.axis_size("fsdp")
    bits, bit = [], groups // 2
    while bit >= 1:
        bits.append(bit)
        bit //= 2
    far = len(bits) - 1
    count = len(grads)
    number = count * (1 + 2 * far + length - 1)
    size = sum(g.size * g.dtype.itemsize for g in grads)
    scratch = []
    for g in grads:
        block = g.shape[1:]
        scratch += [pltpu.VMEM((length,) + (2,) * far + block, g.dtype)] * 2
        scratch += [
            pltpu.VMEM((2, length // 2) + (2,) * (far - 1 - s) + block, g.dtype) for s in range(far)
        ]
        scratch.append(pltpu.VMEM((length - 1,) + block, g.dtype))
    return pl.pallas_call(
        functools.partial(scatter_dense_kernel, length, bits, count),
        out_shape=[jax.ShapeDtypeStruct(g.shape[1:], jnp.float32) for g in grads],
        in_specs=[pl.BlockSpec(memory_space=pl.ANY)] * count,
        out_specs=[pl.BlockSpec(memory_space=pltpu.VMEM)] * count,
        scratch_shapes=scratch
        + [
            pltpu.SemaphoreType.DMA((number,)),
            pltpu.SemaphoreType.DMA((number,)),
            pltpu.SemaphoreType.DMA((count,)),
        ],
        compiler_params=pltpu.CompilerParams(
            collective_id=collective_id, has_side_effects=True, vmem_limit_bytes=grant(scratch, 0)
        ),
        cost_estimate=pl.CostEstimate(flops=0, bytes_accessed=3 * size, transcendentals=0),
        name="scatter_dense",
    )(*[g.reshape((length,) + (2,) * len(bits) + g.shape[1:]) for g in grads])


def row_dims():
    groups = lax.axis_size("fsdp")
    dims, bit = [("seq", 1)], groups // 2
    while bit >= 1:
        dims.append(("fsdp", bit))
        bit //= 2
    return dims


def row_places(dims):
    seq, group = lax.axis_index("seq"), lax.axis_index("fsdp")
    index = {"seq": seq, "fsdp": group}
    own = [bit_of(index[axis], bit) for axis, bit in dims]
    partner = [(axis, flip(index[axis], bit)) for axis, bit in dims]
    return own, partner


def row_orders(far, light):
    if light:
        return [[0] + [1 + (i + k) % (far - 1) for k in range(far - 1)] for i in range(far - 1)]
    return [[(i + k) % far for k in range(far)] for i in range(far)]


def gather_rows_kernel(dims, orders, held, rows_ref, pick_ref, slots_ref, buffer, send_sems, recv_sems, local_sem):
    own, partner = row_places(dims)
    greet(partner)
    copies = Copies(send_sems, recv_sems)
    far = len(dims) - 1
    pieces = len(orders)
    width = rows_ref.shape[1] // pieces
    capacity = slots_ref.shape[-2]

    def view(piece, done):
        where = list(own)
        for d in done:
            where[d] = slice(None)
        return buffer.at[(piece, *where)]

    flying, local = [], []
    for piece in range(pieces):
        cut = rows_ref.at[:, pl.ds(piece * width, width)]
        flying.append(copies.start(cut, view(piece, []), *partner[orders[piece][0]]))
        local.append(pltpu.make_async_copy(cut, view(piece, []), local_sem.at[piece]))
        local[piece].start()
    for copy in local:
        copy.wait()

    def pick_block(piece, where):
        taken = jnp.dot(
            pick_ref[tuple(where)], buffer[(piece, *where)], preferred_element_type=jnp.float32
        ).astype(slots_ref.dtype)
        for e in range(held):
            slots_ref[(e, *where, slice(None), pl.ds(piece * width, width))] = taken[
                e * capacity : (e + 1) * capacity
            ]

    def pick_all(piece, core):
        def body(i, carry):
            where, rest = [], i
            for d in range(far):
                where.append(lax.rem(lax.div(rest, 2 ** (far - 1 - d)), 2))
            pick_block(piece, where + [core])
            return carry

        lax.fori_loop(0, 2**far, body, 0)

    for stage in range(1, far + 1):
        for piece in range(pieces):
            flying[piece].wait_recv()
            order = orders[piece]
            done = order[:stage]
            ref = view(piece, done)
            flying[piece] = copies.start(ref, ref, *(partner[order[stage]] if stage < far else partner[far]))
    for piece in range(pieces):
        pick_all(piece, own[far])
    for piece in range(pieces):
        flying[piece].wait_recv()
        pick_all(piece, 1 - own[far])
    copies.finish()


def gather_rows(rows, pick_low, held, collective_id, light):
    dims = row_dims()
    far = len(dims) - 1
    orders = row_orders(far, light)
    count, feat = rows.shape
    width = feat // len(orders)
    sources = 2 ** len(dims)
    capacity = pick_low.shape[1] // held
    lead = (2,) * len(dims)
    number = len(orders) * (far + 1)
    scratch = [pltpu.VMEM((len(orders),) + lead + (count, width), rows.dtype)]
    slots = pl.pallas_call(
        functools.partial(gather_rows_kernel, dims, orders, held),
        out_shape=jax.ShapeDtypeStruct((held,) + lead + (capacity, feat), rows.dtype),
        in_specs=[pl.BlockSpec(memory_space=pltpu.VMEM)] * 2,
        out_specs=pl.BlockSpec(memory_space=pltpu.VMEM),
        scratch_shapes=scratch
        + [pltpu.SemaphoreType.DMA((n,)) for n in (number, number, len(orders))],
        compiler_params=pltpu.CompilerParams(
            collective_id=collective_id,
            has_side_effects=True,
            vmem_limit_bytes=grant(scratch, 12 * 2**20),
        ),
        cost_estimate=pl.CostEstimate(
            flops=2 * sources * pick_low.shape[1] * count * feat,
            bytes_accessed=6 * sources * count * feat,
            transcendentals=0,
        ),
        name="gather_rows",
    )(rows, pick_low.reshape(lead + pick_low.shape[1:]))
    return slots.reshape(held, sources * capacity, feat)


def scatter_rows_kernel(
    dims, orders, held, slots_ref, pick_ref, out_ref, mine, other, came_core, came_far, send_sems, recv_sems
):
    own, partner = row_places(dims)
    greet(partner)
    copies = Copies(send_sems, recv_sems)
    far = len(dims) - 1
    pieces = len(orders)
    width = out_ref.shape[1] // pieces
    capacity = slots_ref.shape[-2]
    count = out_ref.shape[0]

    def spread(piece, core, target):
        def body(i, carry):
            where = [lax.rem(lax.div(i, 2 ** (far - 1 - d)), 2) for d in range(far)]
            total = jnp.zeros((count, width), jnp.float32)
            for e in range(held):
                rows = slots_ref[(e, *where, core, slice(None), pl.ds(piece * width, width))]
                chosen = pick_ref[(*where, core, pl.ds(e * capacity, capacity))]
                total = total + lax.dot_general(
                    chosen, rows, (((0,), (0,)), ((), ())), preferred_element_type=jnp.float32
                )
            target[(piece, *where)] = total.astype(target.dtype)
            return carry

        lax.fori_loop(0, 2**far, body, 0)

    flying = []
    for piece in range(pieces):
        spread(piece, 1 - own[far], other)
        flying.append(copies.start(other.at[piece], came_core.at[piece], *partner[far]))
    for piece in range(pieces):
        spread(piece, own[far], mine)

    def add_into(piece, fixed, came_view):
        left = [d for d in range(far) if d not in fixed]

        def body(i, carry):
            where, inner = [None] * far, []
            for k, d in enumerate(left):
                where[d] = lax.rem(lax.div(i, 2 ** (len(left) - 1 - k)), 2)
                inner.append(where[d])
            for d in fixed:
                where[d] = own[d]
            total = mine[(piece, *where)].astype(jnp.float32) + came_view[tuple(inner)].astype(jnp.float32)
            mine[(piece, *where)] = total.astype(mine.dtype)
            return carry

        lax.fori_loop(0, 2 ** len(left), body, 0)

    for stage in range(far):
        for piece in range(pieces):
            order = orders[piece][::-1]
            fixed = order[:stage]
            flying[piece].wait_recv()
            add_into(piece, fixed, came_core.at[piece] if stage == 0 else came_far[stage - 1].at[piece])
            dim = order[stage]
            where = [slice(None)] * far
            for d in fixed:
                where[d] = own[d]
            where[dim] = 1 - own[dim]
            flying[piece] = copies.start(
                mine.at[(piece, *where)], came_far[stage].at[piece], *partner[dim]
            )
    for piece in range(pieces):
        flying[piece].wait_recv()
        out_ref[:, pl.ds(piece * width, width)] = mine[(piece, *own[:far])].astype(jnp.float32) + came_far[far - 1][piece].astype(
            jnp.float32
        )
    copies.finish()


def scatter_rows(slots, pick_low, held, collective_id, light):
    dims = row_dims()
    far = len(dims) - 1
    orders = row_orders(far, light)
    count, feat = pick_low.shape[2], slots.shape[2]
    width = feat // len(orders)
    sources = 2 ** len(dims)
    capacity = pick_low.shape[1] // held
    lead = (2,) * len(dims)
    number = len(orders) * (far + 1)

    scratch = [pltpu.VMEM((len(orders),) + (2,) * far + (count, width), slots.dtype)] * 3
    scratch += [pltpu.VMEM((len(orders),) + (2,) * (far - 1 - s) + (count, width), slots.dtype) for s in range(far)]

    def kernel(slots_ref, pick_ref, out_ref, mine, other, came_core, *rest):
        came_far, sems = rest[:far], rest[far:]
        scatter_rows_kernel(
            dims, orders, held, slots_ref, pick_ref, out_ref, mine, other, came_core, came_far, *sems
        )

    return pl.pallas_call(
        kernel,
        out_shape=jax.ShapeDtypeStruct((count, feat), jnp.float32),
        in_specs=[pl.BlockSpec(memory_space=pltpu.VMEM)] * 2,
        out_specs=pl.BlockSpec(memory_space=pltpu.VMEM),
        scratch_shapes=scratch + [pltpu.SemaphoreType.DMA((number,)), pltpu.SemaphoreType.DMA((number,))],
        compiler_params=pltpu.CompilerParams(
            collective_id=collective_id,
            has_side_effects=True,
            vmem_limit_bytes=grant(scratch, 4 * 2**20),
        ),
        cost_estimate=pl.CostEstimate(
            flops=2 * sources * pick_low.shape[1] * count * feat,
            bytes_accessed=6 * sources * count * feat,
            transcendentals=0,
        ),
        name="scatter_rows",
    )(slots.reshape((held,) + lead + (capacity, feat)), pick_low.reshape(lead + pick_low.shape[1:]))


def allowed_keys(seg_rows_ref, seg_keys_ref, back_rows):
    shape = (seg_rows_ref.shape[0], seg_keys_ref.shape[1])
    row = lax.broadcasted_iota(jnp.int32, shape, 0) + back_rows
    key = lax.broadcasted_iota(jnp.int32, shape, 1)
    return (key <= row) & (seg_rows_ref[...] == seg_keys_ref[...])


def attend_kernel(scale, back_rows, query, key, value, seg_rows, seg_keys, out, log_total):
    allowed = allowed_keys(seg_rows, seg_keys, back_rows)
    keys, values = key[...], value[...]
    lane = lax.broadcasted_iota(jnp.int32, (query.shape[0], 128), 1)
    logs = jnp.zeros((query.shape[0], 128), jnp.float32)
    for j in range(query.shape[1] // HEAD):
        columns = slice(j * HEAD, (j + 1) * HEAD)
        scores = lax.dot_general(
            query[:, columns], keys, (((1,), (1,)), ((), ())), preferred_element_type=jnp.float32
        )
        scores = jnp.where(allowed, scores * scale, MASKED)
        top = jnp.max(scores, axis=1, keepdims=True)
        weights = jnp.exp(scores - top)
        total = jnp.sum(weights, axis=1, keepdims=True)
        prob = (weights * (1.0 / total)).astype(jnp.bfloat16)
        out[:, columns] = jnp.dot(prob, values, preferred_element_type=jnp.float32).astype(out.dtype)
        logs = jnp.where(lane == j, top + jnp.log(total), logs)
    log_total[...] = logs


def attend_back_kernel(
    scale, back_rows, query, key, value, seg_rows, seg_keys, log_total, grad, grad_query, grad_key_value
):
    allowed = allowed_keys(seg_rows, seg_keys, back_rows)
    keys, values = key[...], value[...]
    grad_keys = jnp.zeros(keys.shape, jnp.float32)
    grad_values = jnp.zeros(values.shape, jnp.float32)
    for j in range(query.shape[1] // HEAD):
        columns = slice(j * HEAD, (j + 1) * HEAD)
        rows, grad_rows = query[:, columns], grad[:, columns]
        scores = lax.dot_general(
            rows, keys, (((1,), (1,)), ((), ())), preferred_element_type=jnp.float32
        )
        scores = jnp.where(allowed, scores * scale, MASKED)
        prob = jnp.exp(scores - log_total[:, j : j + 1])
        grad_prob = lax.dot_general(
            grad_rows, values, (((1,), (1,)), ((), ())), preferred_element_type=jnp.float32
        )
        delta = jnp.sum(prob * grad_prob, axis=1, keepdims=True)
        grad_scores = (prob * (grad_prob - delta)).astype(jnp.bfloat16)
        grad_query[:, columns] = (
            jnp.dot(grad_scores, keys, preferred_element_type=jnp.float32) * scale
        ).astype(grad_query.dtype)
        grad_keys = grad_keys + lax.dot_general(
            grad_scores, rows, (((0,), (0,)), ((), ())), preferred_element_type=jnp.float32
        )
        grad_values = grad_values + lax.dot_general(
            prob.astype(jnp.bfloat16), grad_rows, (((0,), (0,)), ((), ())), preferred_element_type=jnp.float32
        )
    grad_key_value[0] = grad_keys * scale
    grad_key_value[1] = grad_values


def attend_specs(tok_rows, window, group_width):
    return [
        pl.BlockSpec((tok_rows, group_width), lambda g: (0, g)),
        pl.BlockSpec((window, HEAD), lambda g: (0, g)),
        pl.BlockSpec((window, HEAD), lambda g: (0, KV_HEADS + g)),
        pl.BlockSpec((tok_rows, 1), lambda g: (0, 0)),
        pl.BlockSpec((1, window), lambda g: (0, 0)),
    ]


def attend(query, key_value, seg_rows, seg_keys, scale):
    tok_rows, window = query.shape[0], key_value.shape[0]
    group_width = query.shape[1] // KV_HEADS
    return pl.pallas_call(
        functools.partial(attend_kernel, scale, window - tok_rows),
        grid=(KV_HEADS,),
        in_specs=attend_specs(tok_rows, window, group_width),
        out_specs=[
            pl.BlockSpec((tok_rows, group_width), lambda g: (0, g)),
            pl.BlockSpec((None, tok_rows, 128), lambda g: (g, 0, 0)),
        ],
        out_shape=[
            jax.ShapeDtypeStruct(query.shape, query.dtype),
            jax.ShapeDtypeStruct((KV_HEADS, tok_rows, 128), jnp.float32),
        ],
        compiler_params=pltpu.CompilerParams(vmem_limit_bytes=32 * 2**20),
        cost_estimate=pl.CostEstimate(
            flops=4 * HEADS * tok_rows * window * HEAD,
            bytes_accessed=8 * query.size,
            transcendentals=HEADS * tok_rows * window,
        ),
        name="attend",
    )(query, key_value, key_value, seg_rows, seg_keys)


def attend_back(query, key_value, seg_rows, seg_keys, log_total, grad, scale):
    tok_rows, window = query.shape[0], key_value.shape[0]
    group_width = query.shape[1] // KV_HEADS
    return pl.pallas_call(
        functools.partial(attend_back_kernel, scale, window - tok_rows),
        grid=(KV_HEADS,),
        in_specs=attend_specs(tok_rows, window, group_width)
        + [
            pl.BlockSpec((None, tok_rows, 128), lambda g: (g, 0, 0)),
            pl.BlockSpec((tok_rows, group_width), lambda g: (0, g)),
        ],
        out_specs=[
            pl.BlockSpec((tok_rows, group_width), lambda g: (0, g)),
            pl.BlockSpec((2, window, HEAD), lambda g: (0, 0, g)),
        ],
        out_shape=[
            jax.ShapeDtypeStruct(query.shape, query.dtype),
            jax.ShapeDtypeStruct((2, window, KV_HEADS * HEAD), jnp.float32),
        ],
        compiler_params=pltpu.CompilerParams(vmem_limit_bytes=32 * 2**20),
        cost_estimate=pl.CostEstimate(
            flops=10 * HEADS * tok_rows * window * HEAD,
            bytes_accessed=16 * query.size,
            transcendentals=HEADS * tok_rows * window,
        ),
        name="attend_back",
    )(query, key_value, key_value, seg_rows, seg_keys, log_total, grad)


def block(
    tokens,
    teacher,
    valid_mask,
    segment_ids,
    routes,
    gate_weights,
    norm1_gain,
    query_weight,
    key_weight,
    value_weight,
    output_weight,
    norm2_gain,
    shared_gate_weight,
    shared_up_weight,
    shared_down_weight,
    expert_gate_weight,
    expert_up_weight,
    expert_down_weight,
):
    length, groups = lax.axis_size("seq"), lax.axis_size("fsdp")
    seq_index, group_index = lax.axis_index("seq"), lax.axis_index("fsdp")
    devices = length * groups
    tok_rows = tokens.shape[1]
    seq_len = segment_ids.shape[1]
    score_scale = 1.0 / math.sqrt(HEAD)
    key_width = KV_HEADS * HEAD
    query_width = HEADS * HEAD
    shared_width = shared_gate_weight.shape[1]

    lanes = 128
    gains = jnp.pad(jnp.stack([norm1_gain, norm2_gain], axis=1), ((0, 0), (0, lanes - 2)))
    meta = jnp.concatenate([routes[0].T.astype(F32), gate_weights[0].T], axis=0)
    meta = jnp.pad(meta, ((0, 16 - 2 * TOP), (0, 0)))
    longest = seq_len // 2
    back = min(length - 1, -(-(longest - 1) // tok_rows))
    gathered = gather_dense(
        [
            jnp.concatenate([query_weight, key_weight, value_weight, gains], axis=1),
            meta,
            output_weight,
            jnp.concatenate([shared_gate_weight, shared_up_weight], axis=1),
            shared_down_weight,
        ],
        expert_gate_weight,
        tokens[0],
        back,
        2 * key_width,
    )
    qkv_full, meta, output_full, gate_up_full, down_full, expert_gate_full = gathered[:6]
    normed_one, query_rows, key_value_all = gathered[6:]

    def weight_grad(rows, grad_rows):
        grad = dot(rows, grad_rows, 0, 0).astype(BF16)
        return grad.reshape(devices, -1, grad.shape[1])

    qkv_width = query_width + 2 * key_width
    gain_plain = qkv_full[:, qkv_width : qkv_width + 2].T.astype(F32)
    qkv_full = qkv_full[:, :qkv_width]
    gain_one, gain_two = gain_plain[0], gain_plain[1]

    num_local = expert_gate_weight.shape[0]
    num_held = num_local // PAIR
    side = seq_index % PAIR

    def share(weight, k):
        return lax.dynamic_slice_in_dim(weight, (side ^ (k % PAIR)) * num_held, num_held, axis=0)

    def collect_start(weight, wait):
        sent = after(weight, *wait)
        return [exchange(share(sent, k), "seq", k) for k in range(1, length)]

    def collect_done(weight, came):
        part = weight.shape[1]
        full = jnp.zeros((num_held, length * part, weight.shape[2]), weight.dtype)
        for k, block in enumerate([share(weight, 0)] + came):
            full = lax.dynamic_update_slice(full, block, (0, (seq_index ^ k) * part, 0))
        return full

    x_float = tokens[0].astype(F32)
    if normed_one is None:
        normed_one = rms_norm(x_float, gain_one).astype(BF16)
        qkv_rows = dot(normed_one, qkv_full, 1, 0).astype(BF16)
        query_rows = qkv_rows[:, :query_width]
        key_value = [qkv_rows[:, query_width:]]
        for _ in range(back):
            key_value.insert(0, shift(key_value[0], "seq", 1))
        key_value_all = jnp.concatenate(key_value, axis=0)
    up_came = collect_start(expert_up_weight, [key_value_all])
    window = (back + 1) * tok_rows
    seg_padded = jnp.concatenate([jnp.full((back * tok_rows,), -1, jnp.int32), segment_ids[0]])
    seg_keys = lax.dynamic_slice_in_dim(seg_padded, seq_index * tok_rows, window)
    seg_here = seg_keys[back * tok_rows :]
    seg_rows, seg_line = seg_here[:, None], seg_keys[None, :]
    attended, log_total = attend(query_rows, key_value_all, seg_rows, seg_line, score_scale)
    mixed_rows = x_float + dot(attended, output_full, 1, 0)
    normed_two = rms_norm(mixed_rows, gain_two).astype(BF16)

    experts_all = num_local * groups
    capacity = tok_rows * TOP * 4 // (3 * experts_all)
    meta = lax.dynamic_slice_in_dim(
        meta.reshape(length, groups, 16, tok_rows), seq_index // PAIR * PAIR, PAIR, axis=0
    ).reshape(PAIR * groups, 16, tok_rows)
    route_all, gate_all = meta[:, :TOP], meta[:, TOP : 2 * TOP]
    held_ids = group_index * num_local + side * num_held + jnp.arange(num_held, dtype=jnp.int32)
    named = route_all[:, None] == held_ids.astype(F32)[None, :, None, None]
    has = jnp.any(named, axis=2)
    gate_of = jnp.sum(jnp.where(named, gate_all[:, None], 0.0), axis=2)
    token_order = jnp.arange(tok_rows, dtype=jnp.int32)
    earlier = (token_order[:, None] < token_order[None, :]).astype(BF16)
    before = lax.dot_general(
        has.astype(BF16), earlier, (((2,), (0,)), ((), ())), preferred_element_type=F32
    )
    slot_number = jnp.arange(capacity, dtype=F32)
    chosen = has[:, :, None] & (before[:, :, None] == slot_number[None, None, :, None])
    gate_slots = jnp.sum(jnp.where(chosen, gate_of[:, :, None], 0.0), axis=3)
    sources = PAIR * groups
    chosen_low = chosen.astype(BF16).reshape(sources, num_held * capacity, tok_rows)
    gate_canonical = jnp.moveaxis(gate_slots, 0, 1).reshape(num_held, sources * capacity, 1)
    down_came = collect_start(expert_down_weight, [normed_two])
    slot_rows = gather_rows(normed_two, chosen_low, num_held, 1, False)

    gate_up = dot(normed_two, gate_up_full, 1, 0)
    shared_gate, shared_up = gate_up[:, :shared_width], gate_up[:, shared_width:]
    shared_hidden = swiglu(shared_gate, shared_up).astype(BF16)
    shared_out = dot(shared_hidden, down_full, 1, 0)
    expert_gate_rows = batch_dot(slot_rows, expert_gate_full, 2, 1)
    up_came = [after(came, shared_out) for came in up_came]
    expert_up_full = collect_done(expert_up_weight, up_came)
    expert_up_rows = batch_dot(slot_rows, expert_up_full, 2, 1)
    expert_hidden = swiglu(expert_gate_rows, expert_up_rows).astype(BF16)
    expert_down_full = collect_done(
        expert_down_weight, [after(came, expert_hidden) for came in down_came]
    )
    expert_output = (gate_canonical * batch_dot(expert_hidden, expert_down_full, 2, 1)).astype(BF16)
    routed = scatter_rows(expert_output, chosen_low, num_held, 2, False)

    output = mixed_rows + shared_out + routed
    block_output = output.astype(BF16)
    valid_rows = valid_mask[0].astype(F32)[:, None]
    grad_out = valid_rows * (output - teacher[0].astype(F32))
    grad_low = grad_out.astype(BF16)

    grad_slots = gather_rows(grad_low, chosen_low, num_held, 3, False)
    grad_slots = (gate_canonical * grad_slots.astype(F32)).astype(BF16)

    def expert_grad(left, right, wait):
        grad = after(batch_dot(left, right, 1, 1).astype(BF16), *wait)
        rows = grad.shape[1] // length
        own = [None] * length
        for k in range(length):
            slab = lax.dynamic_slice_in_dim(grad, (seq_index ^ k) * rows, rows, axis=1)
            own[k] = exchange(slab, "seq", k) if k else slab
        return own

    def expert_sum(own, wait):
        own = [after(part, *wait) for part in own]
        same = sum(own[k].astype(F32) for k in range(0, length, PAIR))
        crossed = sum(own[k].astype(F32) for k in range(1, length, PAIR))
        first = (jnp.arange(PAIR) == side)[:, None, None, None]
        return jnp.where(first, same[None], crossed[None]).reshape(num_local, *same.shape[1:])

    expert_down_own = expert_grad(expert_hidden, grad_slots, [])
    grad_hidden = batch_dot(grad_slots, expert_down_full, 2, 2)
    grad_gate_rows, grad_up_rows = swiglu_backward(expert_gate_rows, expert_up_rows, grad_hidden)
    expert_gate_own = expert_grad(slot_rows, grad_gate_rows, [])
    grad_input = (
        batch_dot(grad_gate_rows, expert_gate_full, 2, 2) + batch_dot(grad_up_rows, expert_up_full, 2, 2)
    ).astype(BF16)
    grad_routed = scatter_rows(grad_input, chosen_low, num_held, 4, True)
    grad_shidden = dot(grad_low, down_full, 1, 1)
    grad_sgate_rows, grad_sup_rows = swiglu_backward(shared_gate, shared_up, grad_shidden)
    grad_gate_up = jnp.concatenate([grad_sgate_rows, grad_sup_rows], axis=1)
    grad_normed_two = dot(grad_gate_up, gate_up_full, 1, 1) + grad_routed
    _, pull_two = jax.vjp(rms_norm, mixed_rows, gain_two)
    grad_mixed_norm, grad_gain_two = pull_two(grad_normed_two)
    grad_mixed = grad_out + grad_mixed_norm
    grad_mixed_low = grad_mixed.astype(BF16)

    grad_attended = dot(grad_mixed_low, output_full, 1, 1).astype(BF16)
    grad_query, grad_key_value = attend_back(
        query_rows, key_value_all, seg_rows, seg_line, log_total, grad_attended, score_scale
    )
    grad_key_value = jnp.concatenate([grad_key_value[0], grad_key_value[1]], axis=1)
    total = grad_key_value[:tok_rows]
    for step in range(1, back + 1):
        came = shift(total.astype(BF16), "seq", -1)
        total = came.astype(F32) + grad_key_value[step * tok_rows : (step + 1) * tok_rows]
    grad_qkv = jnp.concatenate([grad_query, total.astype(BF16)], axis=1)
    expert_up_own = expert_grad(slot_rows, grad_up_rows, [total])
    grad_normed_one = dot(grad_qkv, qkv_full, 1, 1)
    _, pull_one = jax.vjp(rms_norm, x_float, gain_one)
    grad_x_norm, grad_gain_one = pull_one(grad_normed_one)
    grad_tokens = grad_mixed + grad_x_norm

    gain_grads = jnp.stack([grad_gain_one, grad_gain_two]).reshape(2, devices, -1).swapaxes(0, 1)
    gain_rows = gain_grads.shape[2]
    gain_grads = jnp.pad(gain_grads, ((0, 0), (0, 6), (0, lanes - gain_rows)))
    dense_grads = [
        weight_grad(normed_two, grad_gate_up),
        weight_grad(normed_one, grad_qkv),
        weight_grad(attended, grad_mixed_low),
        weight_grad(shared_hidden, grad_low),
        gain_grads,
    ]
    sums = scatter_dense(dense_grads, 5)
    grad_gate_up_block, grad_qkv_block, grad_output_block, grad_down_block, grad_gain_block = sums
    last = [grad_gain_block]
    grad_expert_down = expert_sum(expert_down_own, last)
    grad_expert_gate = expert_sum(expert_gate_own, last)
    grad_expert_up = expert_sum(expert_up_own, last)
    return (
        block_output[None],
        grad_tokens[None],
        grad_gain_block[0, :gain_rows],
        grad_qkv_block[:, :query_width],
        grad_qkv_block[:, query_width : query_width + key_width],
        grad_qkv_block[:, query_width + key_width :],
        grad_output_block,
        grad_gain_block[1, :gain_rows],
        grad_gate_up_block[:, :shared_width],
        grad_gate_up_block[:, shared_width:],
        grad_down_block,
        grad_expert_gate,
        grad_expert_up,
        grad_expert_down,
    )


def solution(mesh):
    rows = P("fsdp", "seq", None)
    dense = P(("seq", "fsdp"), None)
    gain = P(("seq", "fsdp"))
    return jax.shard_map(
        block,
        mesh=mesh,
        in_specs=(
            rows, rows, P("fsdp", "seq"), P("fsdp", None), rows, rows,
            gain, dense, dense, dense, dense, gain, dense, dense, dense, rows, rows, rows,
        ),
        out_specs=(
            rows, rows, gain, dense, dense, dense, dense, gain, dense, dense, dense, rows, rows, rows,
        ),
        check_vma=False,
    )
```

```python
import functools
import math

import jax
import jax.numpy as jnp
from jax import lax
from jax.experimental import pallas as pl
from jax.experimental.pallas import tpu as pltpu
from jax.sharding import PartitionSpec as P


HEADS = 12
KV_HEADS = 4
HEAD = 128
TOP = 6
EPSILON = 1e-05
MASKED = -1e30
PAIR = 2


BF16 = jnp.bfloat16
F32 = jnp.float32


def exchange(values, axis, bit):
    count = lax.axis_size(axis)
    return lax.ppermute(values, axis, [(i, i ^ bit) for i in range(count)])


def shift(values, axis, step):
    count = lax.axis_size(axis)
    pairs = [(i, i + step) for i in range(count) if 0 <= i + step < count]
    return lax.ppermute(values, axis, pairs)


def after(values, *others):
    return lax.optimization_barrier((values, *others))[0]


def dot(left, right, left_dim, right_dim):
    return lax.dot_general(
        left, right, (((left_dim,), (right_dim,)), ((), ())), preferred_element_type=F32
    )


def batch_dot(left, right, left_dim, right_dim):
    return lax.dot_general(
        left, right, (((left_dim,), (right_dim,)), ((0,), (0,))), preferred_element_type=F32
    )


def rms_norm(values, gain):
    factor = lax.rsqrt(jnp.mean(values * values, axis=-1, keepdims=True) + EPSILON)
    return values * factor * gain


def swiglu(gate_rows, up_rows):
    return jax.nn.silu(gate_rows) * up_rows


def swiglu_backward(gate_rows, up_rows, grad_rows):
    _, pull_back = jax.vjp(swiglu, gate_rows, up_rows)
    grad_gate, grad_up = pull_back(grad_rows)
    return (grad_gate.astype(BF16), grad_up.astype(BF16))


MESH = pl.DeviceIdType.MESH


def grant(scratch, extra):
    size = extra
    for ref in scratch:
        shape = list(ref.shape)
        shape[-2] = -(-shape[-2] // 16) * 16
        size += math.prod(shape) * jnp.dtype(ref.dtype).itemsize
    return min(size + 6 * 2**20, 66 * 10**6)


class Copies:
    def __init__(self, send_sems, recv_sems):
        self.send_sems, self.recv_sems, self.made = send_sems, recv_sems, []

    def start(self, source, target, axis, partner, when=None):
        number = len(self.made)
        copy = pltpu.make_async_remote_copy(
            src_ref=source,
            dst_ref=target,
            send_sem=self.send_sems.at[number],
            recv_sem=self.recv_sems.at[number],
            device_id={axis: partner},
            device_id_type=MESH,
        )
        if when is None:
            copy.start()
        else:
            pl.when(when)(copy.start)
        self.made.append((copy, when))
        return copy

    def finish(self):
        for copy, when in self.made:
            if when is None:
                copy.wait_send()
            else:
                pl.when(when)(copy.wait_send)


def greet(partners):
    barrier = pltpu.get_barrier_semaphore()
    for axis, partner in partners:
        pl.semaphore_signal(barrier, inc=1, device_id={axis: partner}, device_id_type=MESH)
    pl.semaphore_wait(barrier, len(partners))


def bit_of(index, bit):
    return lax.rem(lax.div(index, bit), 2)


def flip(index, bit):
    return index + bit - 2 * bit * bit_of(index, bit)


def flip_all(index, mask):
    bit = 1
    while bit <= mask:
        if mask & bit:
            index = flip(index, bit)
        bit *= 2
    return index


def gather_dense_kernel(length, bits, count, back, *refs):
    extra = 0 if back is None else 1
    shards, expert = refs[:count], refs[count]
    outs, expert_full = refs[count + 1 + extra : 2 * count + 1 + extra], refs[2 * count + 1 + extra]
    if back is None:
        send_sems, recv_sems, local_sems = refs[2 * count + 2 :]
        places = list(outs)
    else:
        tokens = refs[count + 1]
        normed_ref, query_ref, window_ref, held, send_sems, recv_sems, local_sems = refs[2 * count + 3 :]
        places = [held] + list(outs[1:])
    seq, group = lax.axis_index("seq"), lax.axis_index("fsdp")
    own = [bit_of(group, bit) for bit in bits]
    partners = [("seq", flip_all(seq, k)) for k in range(1, length)]
    partners += [("fsdp", flip(group, bit)) for bit in bits]
    greet(partners)
    copies = Copies(send_sems, recv_sems)
    far = len(bits) - 1
    half = length // 2
    side = lax.div(seq, half)
    low = [side * half, (1 - side) * half]
    orders = [list(range(far)), list(range(far))[::-1]]
    hops = length - 1
    stages = hops + far + 1
    waiting = [[] for _ in range(count)]
    right, left = lax.rem(seq + 1, length), lax.rem(seq + length - 1, length)

    def launch(t, stage):
        if stage < hops:
            back_block = lax.rem(seq - stage + length, length)
            next_block = lax.rem(seq + stage, length)
            if stage == 0:
                local = pltpu.make_async_copy(shards[t], places[t].at[(seq, *own)], local_sems.at[t])
                local.start()
            made = []
            for block, target, sends, comes in (
                (back_block, right, (seq >= stage) & (seq + 1 < length), seq > stage),
                (next_block, left, (seq + stage < length) & (seq >= 1), seq + 1 + stage < length),
            ):
                view = places[t].at[(block, *own)]
                source = shards[t] if stage == 0 else view
                made.append((copies.start(source, view, "seq", target, sends).wait_recv, comes))
            if stage == 0:
                made.append((local.wait, None))
            return made
        made = []
        for part in (0, 1):
            where = [pl.ds(low[part], half)] + list(own)
            for done in orders[part][: stage - hops]:
                where[1 + done] = slice(None)
            dim = orders[part][stage - hops] if stage < hops + far else far
            view = places[t].at[tuple(where)]
            made.append((copies.start(view, view, "fsdp", flip(group, bits[dim])).wait_recv, None))
        return made

    def settle(made):
        for wait, when in made:
            if when is None:
                wait()
            else:
                pl.when(when)(wait)

    def ship_expert():
        held_experts, depth = expert.shape[0] // PAIR, expert.shape[1]
        rows = pl.ds(pl.multiple_of(seq * depth, depth), depth)
        parity = lax.rem(seq, PAIR)
        local = pltpu.make_async_copy(
            expert.at[pl.ds(parity * held_experts, held_experts)], expert_full.at[:, rows], local_sems.at[count]
        )
        local.start()
        made = [(local.wait, None)]
        for k in range(1, length):
            mine = pl.ds(lax.rem(parity + k, PAIR) * held_experts, held_experts)
            copy = copies.start(expert.at[mine], expert_full.at[:, rows], "seq", flip_all(seq, k))
            made.append((copy.wait_recv, None))
        return made

    def project():
        rows, width = normed_ref.shape
        query_width = query_ref.shape[1]
        key_width = window_ref.shape[1]

        def columns(start, size):
            return held[(slice(None),) * (2 + far) + (slice(None), pl.ds(start, size))].reshape(width, size)

        gain = columns(query_width + key_width, 128).astype(jnp.float32).T[0:1]
        values = tokens[...].astype(jnp.float32)
        factor = lax.rsqrt(jnp.mean(values * values, axis=-1, keepdims=True) + EPSILON)
        normed_ref[...] = (values * factor * gain).astype(normed_ref.dtype)
        here = pl.ds(back * rows, rows)
        for start in range(0, key_width, 512):
            tile = jnp.dot(
                normed_ref[...], columns(query_width + start, 512), preferred_element_type=jnp.float32
            )
            window_ref[here, pl.ds(start, 512)] = tile.astype(window_ref.dtype)
        for j in range(1, back + 1):

            @pl.when(seq < j)
            def _(j=j):
                window_ref[pl.ds((back - j) * rows, rows)] = jnp.zeros((rows, key_width), window_ref.dtype)

        first = pass_keys(1)
        for start in range(0, query_width, 512):
            tile = jnp.dot(normed_ref[...], columns(start, 512), preferred_element_type=jnp.float32)
            query_ref[:, pl.ds(start, 512)] = tile.astype(query_ref.dtype)
        kept = pltpu.make_async_copy(held, outs[0], local_sems.at[0])
        kept.start()
        return first, kept

    def pass_keys(j):
        rows = normed_ref.shape[0]
        source = window_ref.at[pl.ds((back - j + 1) * rows, rows)]
        target = window_ref.at[pl.ds((back - j) * rows, rows)]
        sends = (seq >= j - 1) & (seq + 1 < length)
        return [(copies.start(source, target, "seq", right, sends).wait_recv, seq >= j)]

    passing, passed = [], 0
    for step in range(count + stages):
        if step == hops + 1:
            expert_waiting = ship_expert()
        if passing:
            settle(passing)
            passing = []
            if passed < back:
                passed += 1
                passing = pass_keys(passed)
        for t in range(count):
            stage = step - t
            if 0 < stage <= stages:
                settle(waiting[t])
            if 0 <= stage < stages:
                waiting[t] = launch(t, stage)
        if step == stages and back is not None:
            passing, kept = project()
            passed = 1
    while passing:
        settle(passing)
        passed += 1
        passing = pass_keys(passed) if passed <= back else []
    settle(expert_waiting)
    copies.finish()
    if back is not None:
        kept.wait()


def gather_dense(shards, expert, tokens, back, key_width):
    length, groups = lax.axis_size("seq"), lax.axis_size("fsdp")
    bits, bit = [], groups // 2
    while bit >= 1:
        bits.append(bit)
        bit //= 2
    count = len(shards)
    number = count * 2 * (length - 1 + len(bits)) + length - 1 + back
    size = sum(s.size * s.dtype.itemsize for s in shards) * length * groups
    experts, depth, wide = expert.shape
    lead = (length,) + (2,) * len(bits)
    rows, width = tokens.shape
    fused = shards[0].shape[0] % 16 == 0
    extra_in, extra_out, extra_scratch = [], [], []
    if fused:
        query_width = shards[0].shape[1] - key_width - 128
        extra_in = [tokens]
        extra_out = [
            jax.ShapeDtypeStruct((rows, width), tokens.dtype),
            jax.ShapeDtypeStruct((rows, query_width), tokens.dtype),
            jax.ShapeDtypeStruct(((back + 1) * rows, key_width), tokens.dtype),
        ]
        extra_scratch = [pltpu.VMEM(lead + shards[0].shape, shards[0].dtype)]
    results = pl.pallas_call(
        functools.partial(gather_dense_kernel, length, bits, count, back if fused else None),
        out_shape=[
            jax.ShapeDtypeStruct((length,) + (2,) * len(bits) + s.shape, s.dtype) for s in shards
        ]
        + [jax.ShapeDtypeStruct((experts // PAIR, length * depth, wide), expert.dtype)]
        + extra_out,
        in_specs=[pl.BlockSpec(memory_space=pltpu.VMEM)] * count
        + [pl.BlockSpec(memory_space=pl.ANY)]
        + [pl.BlockSpec(memory_space=pltpu.VMEM)] * len(extra_in),
        out_specs=[pl.BlockSpec(memory_space=pl.ANY)] * (count + 1)
        + [pl.BlockSpec(memory_space=pltpu.VMEM)] * len(extra_out),
        scratch_shapes=extra_scratch
        + [
            pltpu.SemaphoreType.DMA((number,)),
            pltpu.SemaphoreType.DMA((number,)),
            pltpu.SemaphoreType.DMA((count + 1,)),
        ],
        compiler_params=pltpu.CompilerParams(
            collective_id=0, has_side_effects=True, vmem_limit_bytes=60 * 2**20
        ),
        cost_estimate=pl.CostEstimate(flops=0, bytes_accessed=3 * size, transcendentals=0),
        name="gather_dense",
    )(*shards, expert, *extra_in)
    outs = [out.reshape(-1, out.shape[-1]) for out in results[:count]] + [results[count]]
    return outs + (list(results[count + 1 :]) if fused else [None] * 3)


def scatter_dense_kernel(length, bits, count, *refs):
    grads, outs = refs[:count], refs[count : 2 * count]
    far = len(bits) - 1
    per = 3 + far
    scratch = refs[2 * count : 2 * count + per * count]
    send_sems, recv_sems, local_sems = refs[2 * count + per * count :]
    seq, group = lax.axis_index("seq"), lax.axis_index("fsdp")
    own = [bit_of(group, bit) for bit in bits]
    partners = [("seq", flip_all(seq, k)) for k in range(1, length)]
    partners += [("fsdp", flip(group, bit)) for bit in bits]
    greet(partners)
    copies = Copies(send_sems, recv_sems)
    half = length // 2
    side = lax.div(seq, half)
    low = [side * half, (1 - side) * half]
    orders = [list(range(far))[::-1], list(range(far))]
    stages = far + 2
    everything = (slice(None),) * (1 + far)

    def buffers(t):
        held = scratch[per * t : per * (t + 1)]
        return held[0], held[1], held[2 : 2 + far], held[2 + far]

    waiting = [None] * count

    def add(mine, came, lead, fixed, inner_of):
        start, size = lead
        left = [d for d in range(far) if d not in fixed]

        def body(i, carry):
            z = lax.div(i, 2 ** len(left))
            where, inner = [own[d] for d in range(far)], []
            for k, d in enumerate(left):
                where[d] = lax.rem(lax.div(i, 2 ** (len(left) - 1 - k)), 2)
                inner.append(where[d])
            place = (start + z, *where)
            total = mine[place].astype(jnp.float32) + came[inner_of(start + z, z, inner)].astype(jnp.float32)
            mine[place] = total.astype(mine.dtype)
            return carry

        lax.fori_loop(0, size * 2 ** len(left), body, 0)

    def launch(t, stage):
        mine, came_core, came_far, came_seq = buffers(t)
        if stage == 0:
            local = pltpu.make_async_copy(grads[t].at[(*everything, own[far])], mine, local_sems.at[t])
            local.start()
            sent = grads[t].at[(*everything, 1 - own[far])]
            return [copies.start(sent, came_core, "fsdp", flip(group, bits[far]))], local
        if stage <= far:
            made = []
            for part in (0, 1):
                order = orders[part]
                if stage == 1:
                    add(mine, came_core, (low[part], half), [], lambda z, at, inner: (z, *inner))
                else:
                    came = came_far[stage - 2].at[part]
                    add(mine, came, (low[part], half), order[: stage - 1], lambda z, at, inner: (at, *inner))
                dim = order[stage - 1]
                where = [slice(None)] * far
                for d in order[: stage - 1]:
                    where[d] = own[d]
                where[dim] = 1 - own[dim]
                made.append(
                    copies.start(
                        mine.at[(pl.ds(low[part], half), *where)],
                        came_far[stage - 1].at[part],
                        "fsdp",
                        flip(group, bits[dim]),
                    )
                )
            return made, None
        for part in (0, 1):
            came = came_far[far - 1].at[part]
            add(mine, came, (low[part], half), orders[part], lambda z, at, inner: (at,))
        made = []
        for k in range(1, length):
            other = flip_all(seq, k)
            made.append(copies.start(mine.at[(other, *own[:far])], came_seq.at[k - 1], "seq", other))
        return made, None

    def close(t):
        mine, _, _, came_seq = buffers(t)
        total = mine[(seq, *own[:far])].astype(jnp.float32)
        for k in range(1, length):
            total = total + came_seq[k - 1].astype(jnp.float32)
        outs[t][...] = total

    for step in range(count + stages):
        for t in range(count):
            stage = step - t
            if 0 < stage <= stages:
                made, local = waiting[t]
                for copy in made:
                    copy.wait_recv()
                if local is not None:
                    local.wait()
            if 0 <= stage < stages:
                waiting[t] = launch(t, stage)
            elif stage == stages:
                close(t)
    copies.finish()


def scatter_dense(grads, collective_id):
    length, groups = lax.axis_size("seq"), lax.axis_size("fsdp")
    bits, bit = [], groups // 2
    while bit >= 1:
        bits.append(bit)
        bit //= 2
    far = len(bits) - 1
    count = len(grads)
    number = count * (1 + 2 * far + length - 1)
    size = sum(g.size * g.dtype.itemsize for g in grads)
    scratch = []
    for g in grads:
        block = g.shape[1:]
        scratch += [pltpu.VMEM((length,) + (2,) * far + block, g.dtype)] * 2
        scratch += [
            pltpu.VMEM((2, length // 2) + (2,) * (far - 1 - s) + block, g.dtype) for s in range(far)
        ]
        scratch.append(pltpu.VMEM((length - 1,) + block, g.dtype))
    return pl.pallas_call(
        functools.partial(scatter_dense_kernel, length, bits, count),
        out_shape=[jax.ShapeDtypeStruct(g.shape[1:], jnp.float32) for g in grads],
        in_specs=[pl.BlockSpec(memory_space=pl.ANY)] * count,
        out_specs=[pl.BlockSpec(memory_space=pltpu.VMEM)] * count,
        scratch_shapes=scratch
        + [
            pltpu.SemaphoreType.DMA((number,)),
            pltpu.SemaphoreType.DMA((number,)),
            pltpu.SemaphoreType.DMA((count,)),
        ],
        compiler_params=pltpu.CompilerParams(
            collective_id=collective_id, has_side_effects=True, vmem_limit_bytes=grant(scratch, 0)
        ),
        cost_estimate=pl.CostEstimate(flops=0, bytes_accessed=3 * size, transcendentals=0),
        name="scatter_dense",
    )(*[g.reshape((length,) + (2,) * len(bits) + g.shape[1:]) for g in grads])


def row_dims():
    groups = lax.axis_size("fsdp")
    dims, bit = [("seq", 1)], groups // 2
    while bit >= 1:
        dims.append(("fsdp", bit))
        bit //= 2
    return dims


def row_places(dims):
    seq, group = lax.axis_index("seq"), lax.axis_index("fsdp")
    index = {"seq": seq, "fsdp": group}
    own = [bit_of(index[axis], bit) for axis, bit in dims]
    partner = [(axis, flip(index[axis], bit)) for axis, bit in dims]
    return own, partner


def row_orders(far, light):
    if light:
        return [[0] + [1 + (i + k) % (far - 1) for k in range(far - 1)] for i in range(far - 1)]
    return [[(i + k) % far for k in range(far)] for i in range(far)]


def gather_rows_kernel(dims, orders, held, rows_ref, pick_ref, slots_ref, buffer, send_sems, recv_sems, local_sem):
    own, partner = row_places(dims)
    greet(partner)
    copies = Copies(send_sems, recv_sems)
    far = len(dims) - 1
    pieces = len(orders)
    width = rows_ref.shape[1] // pieces
    capacity = slots_ref.shape[-2]

    def view(piece, done):
        where = list(own)
        for d in done:
            where[d] = slice(None)
        return buffer.at[(piece, *where)]

    flying, local = [], []
    for piece in range(pieces):
        cut = rows_ref.at[:, pl.ds(piece * width, width)]
        flying.append(copies.start(cut, view(piece, []), *partner[orders[piece][0]]))
        local.append(pltpu.make_async_copy(cut, view(piece, []), local_sem.at[piece]))
        local[piece].start()
    for copy in local:
        copy.wait()

    def pick_block(piece, where):
        taken = jnp.dot(
            pick_ref[tuple(where)], buffer[(piece, *where)], preferred_element_type=jnp.float32
        ).astype(slots_ref.dtype)
        for e in range(held):
            slots_ref[(e, *where, slice(None), pl.ds(piece * width, width))] = taken[
                e * capacity : (e + 1) * capacity
            ]

    def pick_all(piece, core):
        def body(i, carry):
            where, rest = [], i
            for d in range(far):
                where.append(lax.rem(lax.div(rest, 2 ** (far - 1 - d)), 2))
            pick_block(piece, where + [core])
            return carry

        lax.fori_loop(0, 2**far, body, 0)

    for stage in range(1, far + 1):
        for piece in range(pieces):
            flying[piece].wait_recv()
            order = orders[piece]
            done = order[:stage]
            ref = view(piece, done)
            flying[piece] = copies.start(ref, ref, *(partner[order[stage]] if stage < far else partner[far]))
    for piece in range(pieces):
        pick_all(piece, own[far])
    for piece in range(pieces):
        flying[piece].wait_recv()
        pick_all(piece, 1 - own[far])
    copies.finish()


def gather_rows(rows, pick_low, held, collective_id, light):
    dims = row_dims()
    far = len(dims) - 1
    orders = row_orders(far, light)
    count, feat = rows.shape
    width = feat // len(orders)
    sources = 2 ** len(dims)
    capacity = pick_low.shape[1] // held
    lead = (2,) * len(dims)
    number = len(orders) * (far + 1)
    scratch = [pltpu.VMEM((len(orders),) + lead + (count, width), rows.dtype)]
    slots = pl.pallas_call(
        functools.partial(gather_rows_kernel, dims, orders, held),
        out_shape=jax.ShapeDtypeStruct((held,) + lead + (capacity, feat), rows.dtype),
        in_specs=[pl.BlockSpec(memory_space=pltpu.VMEM)] * 2,
        out_specs=pl.BlockSpec(memory_space=pltpu.VMEM),
        scratch_shapes=scratch
        + [pltpu.SemaphoreType.DMA((n,)) for n in (number, number, len(orders))],
        compiler_params=pltpu.CompilerParams(
            collective_id=collective_id,
            has_side_effects=True,
            vmem_limit_bytes=grant(scratch, 12 * 2**20),
        ),
        cost_estimate=pl.CostEstimate(
            flops=2 * sources * pick_low.shape[1] * count * feat,
            bytes_accessed=6 * sources * count * feat,
            transcendentals=0,
        ),
        name="gather_rows",
    )(rows, pick_low.reshape(lead + pick_low.shape[1:]))
    return slots.reshape(held, sources * capacity, feat)


def scatter_rows_kernel(
    dims, orders, held, slots_ref, pick_ref, out_ref, mine, other, came_core, came_far, send_sems, recv_sems
):
    own, partner = row_places(dims)
    greet(partner)
    copies = Copies(send_sems, recv_sems)
    far = len(dims) - 1
    pieces = len(orders)
    width = out_ref.shape[1] // pieces
    capacity = slots_ref.shape[-2]
    count = out_ref.shape[0]

    def spread(piece, core, target):
        def body(i, carry):
            where = [lax.rem(lax.div(i, 2 ** (far - 1 - d)), 2) for d in range(far)]
            total = jnp.zeros((count, width), jnp.float32)
            for e in range(held):
                rows = slots_ref[(e, *where, core, slice(None), pl.ds(piece * width, width))]
                chosen = pick_ref[(*where, core, pl.ds(e * capacity, capacity))]
                total = total + lax.dot_general(
                    chosen, rows, (((0,), (0,)), ((), ())), preferred_element_type=jnp.float32
                )
            target[(piece, *where)] = total.astype(target.dtype)
            return carry

        lax.fori_loop(0, 2**far, body, 0)

    flying = []
    for piece in range(pieces):
        spread(piece, 1 - own[far], other)
        flying.append(copies.start(other.at[piece], came_core.at[piece], *partner[far]))
    for piece in range(pieces):
        spread(piece, own[far], mine)

    def add_into(piece, fixed, came_view):
        left = [d for d in range(far) if d not in fixed]

        def body(i, carry):
            where, inner = [None] * far, []
            for k, d in enumerate(left):
                where[d] = lax.rem(lax.div(i, 2 ** (len(left) - 1 - k)), 2)
                inner.append(where[d])
            for d in fixed:
                where[d] = own[d]
            total = mine[(piece, *where)].astype(jnp.float32) + came_view[tuple(inner)].astype(jnp.float32)
            mine[(piece, *where)] = total.astype(mine.dtype)
            return carry

        lax.fori_loop(0, 2 ** len(left), body, 0)

    for stage in range(far):
        for piece in range(pieces):
            order = orders[piece][::-1]
            fixed = order[:stage]
            flying[piece].wait_recv()
            add_into(piece, fixed, came_core.at[piece] if stage == 0 else came_far[stage - 1].at[piece])
            dim = order[stage]
            where = [slice(None)] * far
            for d in fixed:
                where[d] = own[d]
            where[dim] = 1 - own[dim]
            flying[piece] = copies.start(
                mine.at[(piece, *where)], came_far[stage].at[piece], *partner[dim]
            )
    for piece in range(pieces):
        flying[piece].wait_recv()
        out_ref[:, pl.ds(piece * width, width)] = mine[(piece, *own[:far])].astype(jnp.float32) + came_far[far - 1][piece].astype(
            jnp.float32
        )
    copies.finish()


def scatter_rows(slots, pick_low, held, collective_id, light):
    dims = row_dims()
    far = len(dims) - 1
    orders = row_orders(far, light)
    count, feat = pick_low.shape[2], slots.shape[2]
    width = feat // len(orders)
    sources = 2 ** len(dims)
    capacity = pick_low.shape[1] // held
    lead = (2,) * len(dims)
    number = len(orders) * (far + 1)

    scratch = [pltpu.VMEM((len(orders),) + (2,) * far + (count, width), slots.dtype)] * 3
    scratch += [pltpu.VMEM((len(orders),) + (2,) * (far - 1 - s) + (count, width), slots.dtype) for s in range(far)]

    def kernel(slots_ref, pick_ref, out_ref, mine, other, came_core, *rest):
        came_far, sems = rest[:far], rest[far:]
        scatter_rows_kernel(
            dims, orders, held, slots_ref, pick_ref, out_ref, mine, other, came_core, came_far, *sems
        )

    return pl.pallas_call(
        kernel,
        out_shape=jax.ShapeDtypeStruct((count, feat), jnp.float32),
        in_specs=[pl.BlockSpec(memory_space=pltpu.VMEM)] * 2,
        out_specs=pl.BlockSpec(memory_space=pltpu.VMEM),
        scratch_shapes=scratch + [pltpu.SemaphoreType.DMA((number,)), pltpu.SemaphoreType.DMA((number,))],
        compiler_params=pltpu.CompilerParams(
            collective_id=collective_id,
            has_side_effects=True,
            vmem_limit_bytes=grant(scratch, 4 * 2**20),
        ),
        cost_estimate=pl.CostEstimate(
            flops=2 * sources * pick_low.shape[1] * count * feat,
            bytes_accessed=6 * sources * count * feat,
            transcendentals=0,
        ),
        name="scatter_rows",
    )(slots.reshape((held,) + lead + (capacity, feat)), pick_low.reshape(lead + pick_low.shape[1:]))


def allowed_keys(seg_rows_ref, seg_keys_ref, back_rows):
    shape = (seg_rows_ref.shape[0], seg_keys_ref.shape[1])
    row = lax.broadcasted_iota(jnp.int32, shape, 0) + back_rows
    key = lax.broadcasted_iota(jnp.int32, shape, 1)
    return (key <= row) & (seg_rows_ref[...] == seg_keys_ref[...])


def attend_kernel(scale, back_rows, query, key, value, seg_rows, seg_keys, out, log_total):
    allowed = allowed_keys(seg_rows, seg_keys, back_rows)
    keys, values = key[...], value[...]
    lane = lax.broadcasted_iota(jnp.int32, (query.shape[0], 128), 1)
    logs = jnp.zeros((query.shape[0], 128), jnp.float32)
    for j in range(query.shape[1] // HEAD):
        columns = slice(j * HEAD, (j + 1) * HEAD)
        scores = lax.dot_general(
            query[:, columns], keys, (((1,), (1,)), ((), ())), preferred_element_type=jnp.float32
        )
        scores = jnp.where(allowed, scores * scale, MASKED)
        top = jnp.max(scores, axis=1, keepdims=True)
        weights = jnp.exp(scores - top)
        total = jnp.sum(weights, axis=1, keepdims=True)
        prob = (weights * (1.0 / total)).astype(jnp.bfloat16)
        out[:, columns] = jnp.dot(prob, values, preferred_element_type=jnp.float32).astype(out.dtype)
        logs = jnp.where(lane == j, top + jnp.log(total), logs)
    log_total[...] = logs


def attend_back_kernel(
    scale, back_rows, query, key, value, seg_rows, seg_keys, log_total, grad, grad_query, grad_key_value
):
    allowed = allowed_keys(seg_rows, seg_keys, back_rows)
    keys, values = key[...], value[...]
    grad_keys = jnp.zeros(keys.shape, jnp.float32)
    grad_values = jnp.zeros(values.shape, jnp.float32)
    for j in range(query.shape[1] // HEAD):
        columns = slice(j * HEAD, (j + 1) * HEAD)
        rows, grad_rows = query[:, columns], grad[:, columns]
        scores = lax.dot_general(
            rows, keys, (((1,), (1,)), ((), ())), preferred_element_type=jnp.float32
        )
        scores = jnp.where(allowed, scores * scale, MASKED)
        prob = jnp.exp(scores - log_total[:, j : j + 1])
        grad_prob = lax.dot_general(
            grad_rows, values, (((1,), (1,)), ((), ())), preferred_element_type=jnp.float32
        )
        delta = jnp.sum(prob * grad_prob, axis=1, keepdims=True)
        grad_scores = (prob * (grad_prob - delta)).astype(jnp.bfloat16)
        grad_query[:, columns] = (
            jnp.dot(grad_scores, keys, preferred_element_type=jnp.float32) * scale
        ).astype(grad_query.dtype)
        grad_keys = grad_keys + lax.dot_general(
            grad_scores, rows, (((0,), (0,)), ((), ())), preferred_element_type=jnp.float32
        )
        grad_values = grad_values + lax.dot_general(
            prob.astype(jnp.bfloat16), grad_rows, (((0,), (0,)), ((), ())), preferred_element_type=jnp.float32
        )
    grad_key_value[0] = grad_keys * scale
    grad_key_value[1] = grad_values


def attend_specs(tok_rows, window, group_width):
    return [
        pl.BlockSpec((tok_rows, group_width), lambda g: (0, g)),
        pl.BlockSpec((window, HEAD), lambda g: (0, g)),
        pl.BlockSpec((window, HEAD), lambda g: (0, KV_HEADS + g)),
        pl.BlockSpec((tok_rows, 1), lambda g: (0, 0)),
        pl.BlockSpec((1, window), lambda g: (0, 0)),
    ]


def attend(query, key_value, seg_rows, seg_keys, scale):
    tok_rows, window = query.shape[0], key_value.shape[0]
    group_width = query.shape[1] // KV_HEADS
    return pl.pallas_call(
        functools.partial(attend_kernel, scale, window - tok_rows),
        grid=(KV_HEADS,),
        in_specs=attend_specs(tok_rows, window, group_width),
        out_specs=[
            pl.BlockSpec((tok_rows, group_width), lambda g: (0, g)),
            pl.BlockSpec((None, tok_rows, 128), lambda g: (g, 0, 0)),
        ],
        out_shape=[
            jax.ShapeDtypeStruct(query.shape, query.dtype),
            jax.ShapeDtypeStruct((KV_HEADS, tok_rows, 128), jnp.float32),
        ],
        compiler_params=pltpu.CompilerParams(vmem_limit_bytes=32 * 2**20),
        cost_estimate=pl.CostEstimate(
            flops=4 * HEADS * tok_rows * window * HEAD,
            bytes_accessed=8 * query.size,
            transcendentals=HEADS * tok_rows * window,
        ),
        name="attend",
    )(query, key_value, key_value, seg_rows, seg_keys)


def attend_back(query, key_value, seg_rows, seg_keys, log_total, grad, scale):
    tok_rows, window = query.shape[0], key_value.shape[0]
    group_width = query.shape[1] // KV_HEADS
    return pl.pallas_call(
        functools.partial(attend_back_kernel, scale, window - tok_rows),
        grid=(KV_HEADS,),
        in_specs=attend_specs(tok_rows, window, group_width)
        + [
            pl.BlockSpec((None, tok_rows, 128), lambda g: (g, 0, 0)),
            pl.BlockSpec((tok_rows, group_width), lambda g: (0, g)),
        ],
        out_specs=[
            pl.BlockSpec((tok_rows, group_width), lambda g: (0, g)),
            pl.BlockSpec((2, window, HEAD), lambda g: (0, 0, g)),
        ],
        out_shape=[
            jax.ShapeDtypeStruct(query.shape, query.dtype),
            jax.ShapeDtypeStruct((2, window, KV_HEADS * HEAD), jnp.float32),
        ],
        compiler_params=pltpu.CompilerParams(vmem_limit_bytes=32 * 2**20),
        cost_estimate=pl.CostEstimate(
            flops=10 * HEADS * tok_rows * window * HEAD,
            bytes_accessed=16 * query.size,
            transcendentals=HEADS * tok_rows * window,
        ),
        name="attend_back",
    )(query, key_value, key_value, seg_rows, seg_keys, log_total, grad)


def block(
    tokens,
    teacher,
    valid_mask,
    segment_ids,
    routes,
    gate_weights,
    norm1_gain,
    query_weight,
    key_weight,
    value_weight,
    output_weight,
    norm2_gain,
    shared_gate_weight,
    shared_up_weight,
    shared_down_weight,
    expert_gate_weight,
    expert_up_weight,
    expert_down_weight,
):
    length, groups = lax.axis_size("seq"), lax.axis_size("fsdp")
    seq_index, group_index = lax.axis_index("seq"), lax.axis_index("fsdp")
    devices = length * groups
    tok_rows = tokens.shape[1]
    seq_len = segment_ids.shape[1]
    score_scale = 1.0 / math.sqrt(HEAD)
    key_width = KV_HEADS * HEAD
    query_width = HEADS * HEAD
    shared_width = shared_gate_weight.shape[1]

    lanes = 128
    gains = jnp.pad(jnp.stack([norm1_gain, norm2_gain], axis=1), ((0, 0), (0, lanes - 2)))
    meta = jnp.concatenate([routes[0].T.astype(F32), gate_weights[0].T], axis=0)
    meta = jnp.pad(meta, ((0, 16 - 2 * TOP), (0, 0)))
    longest = seq_len // 2
    back = min(length - 1, -(-(longest - 1) // tok_rows))
    gathered = gather_dense(
        [
            jnp.concatenate([query_weight, key_weight, value_weight, gains], axis=1),
            output_weight,
            jnp.concatenate([shared_gate_weight, shared_up_weight], axis=1),
            shared_down_weight,
            meta,
        ],
        expert_gate_weight,
        tokens[0],
        back,
        2 * key_width,
    )
    qkv_full, output_full, gate_up_full, down_full, meta, expert_gate_full = gathered[:6]
    normed_one, query_rows, key_value_all = gathered[6:]

    def weight_grad(rows, grad_rows):
        grad = dot(rows, grad_rows, 0, 0).astype(BF16)
        return grad.reshape(devices, -1, grad.shape[1])

    qkv_width = query_width + 2 * key_width
    gain_plain = qkv_full[:, qkv_width : qkv_width + 2].T.astype(F32)
    qkv_full = qkv_full[:, :qkv_width]
    gain_one, gain_two = gain_plain[0], gain_plain[1]

    num_local = expert_gate_weight.shape[0]
    num_held = num_local // PAIR
    side = seq_index % PAIR

    def share(weight, k):
        return lax.dynamic_slice_in_dim(weight, (side ^ (k % PAIR)) * num_held, num_held, axis=0)

    def collect_start(weight, wait):
        sent = after(weight, *wait)
        return [exchange(share(sent, k), "seq", k) for k in range(1, length)]

    def collect_done(weight, came):
        part = weight.shape[1]
        full = jnp.zeros((num_held, length * part, weight.shape[2]), weight.dtype)
        for k, block in enumerate([share(weight, 0)] + came):
            full = lax.dynamic_update_slice(full, block, (0, (seq_index ^ k) * part, 0))
        return full

    x_float = tokens[0].astype(F32)
    if normed_one is None:
        normed_one = rms_norm(x_float, gain_one).astype(BF16)
        qkv_rows = dot(normed_one, qkv_full, 1, 0).astype(BF16)
        query_rows = qkv_rows[:, :query_width]
        key_value = [qkv_rows[:, query_width:]]
        for _ in range(back):
            key_value.insert(0, shift(key_value[0], "seq", 1))
        key_value_all = jnp.concatenate(key_value, axis=0)
    up_came = collect_start(expert_up_weight, [key_value_all])
    window = (back + 1) * tok_rows
    seg_padded = jnp.concatenate([jnp.full((back * tok_rows,), -1, jnp.int32), segment_ids[0]])
    seg_keys = lax.dynamic_slice_in_dim(seg_padded, seq_index * tok_rows, window)
    seg_here = seg_keys[back * tok_rows :]
    seg_rows, seg_line = seg_here[:, None], seg_keys[None, :]
    attended, log_total = attend(query_rows, key_value_all, seg_rows, seg_line, score_scale)
    mixed_rows = x_float + dot(attended, output_full, 1, 0)
    normed_two = rms_norm(mixed_rows, gain_two).astype(BF16)

    experts_all = num_local * groups
    capacity = tok_rows * TOP * 4 // (3 * experts_all)
    meta = lax.dynamic_slice_in_dim(
        meta.reshape(length, groups, 16, tok_rows), seq_index // PAIR * PAIR, PAIR, axis=0
    ).reshape(PAIR * groups, 16, tok_rows)
    route_all, gate_all = meta[:, :TOP], meta[:, TOP : 2 * TOP]
    held_ids = group_index * num_local + side * num_held + jnp.arange(num_held, dtype=jnp.int32)
    named = route_all[:, None] == held_ids.astype(F32)[None, :, None, None]
    has = jnp.any(named, axis=2)
    gate_of = jnp.sum(jnp.where(named, gate_all[:, None], 0.0), axis=2)
    token_order = jnp.arange(tok_rows, dtype=jnp.int32)
    earlier = (token_order[:, None] < token_order[None, :]).astype(BF16)
    before = lax.dot_general(
        has.astype(BF16), earlier, (((2,), (0,)), ((), ())), preferred_element_type=F32
    )
    slot_number = jnp.arange(capacity, dtype=F32)
    chosen = has[:, :, None] & (before[:, :, None] == slot_number[None, None, :, None])
    gate_slots = jnp.sum(jnp.where(chosen, gate_of[:, :, None], 0.0), axis=3)
    sources = PAIR * groups
    chosen_low = chosen.astype(BF16).reshape(sources, num_held * capacity, tok_rows)
    gate_canonical = jnp.moveaxis(gate_slots, 0, 1).reshape(num_held, sources * capacity, 1)
    down_came = collect_start(expert_down_weight, [normed_two])
    slot_rows = gather_rows(normed_two, chosen_low, num_held, 1, False)

    gate_up = dot(normed_two, gate_up_full, 1, 0)
    shared_gate, shared_up = gate_up[:, :shared_width], gate_up[:, shared_width:]
    shared_hidden = swiglu(shared_gate, shared_up).astype(BF16)
    shared_out = dot(shared_hidden, down_full, 1, 0)
    expert_gate_rows = batch_dot(slot_rows, expert_gate_full, 2, 1)
    up_came = [after(came, shared_out) for came in up_came]
    expert_up_full = collect_done(expert_up_weight, up_came)
    expert_up_rows = batch_dot(slot_rows, expert_up_full, 2, 1)
    expert_hidden = swiglu(expert_gate_rows, expert_up_rows).astype(BF16)
    expert_down_full = collect_done(
        expert_down_weight, [after(came, expert_hidden) for came in down_came]
    )
    expert_output = (gate_canonical * batch_dot(expert_hidden, expert_down_full, 2, 1)).astype(BF16)
    routed = scatter_rows(expert_output, chosen_low, num_held, 2, False)

    output = mixed_rows + shared_out + routed
    block_output = output.astype(BF16)
    valid_rows = valid_mask[0].astype(F32)[:, None]
    grad_out = valid_rows * (output - teacher[0].astype(F32))
    grad_low = grad_out.astype(BF16)

    grad_slots = gather_rows(grad_low, chosen_low, num_held, 3, False)
    grad_slots = (gate_canonical * grad_slots.astype(F32)).astype(BF16)

    def expert_grad(left, right, wait):
        grad = after(batch_dot(left, right, 1, 1).astype(BF16), *wait)
        rows = grad.shape[1] // length
        own = [None] * length
        for k in range(length):
            slab = lax.dynamic_slice_in_dim(grad, (seq_index ^ k) * rows, rows, axis=1)
            own[k] = exchange(slab, "seq", k) if k else slab
        return own

    def expert_sum(own, wait):
        own = [after(part, *wait) for part in own]
        same = sum(own[k].astype(F32) for k in range(0, length, PAIR))
        crossed = sum(own[k].astype(F32) for k in range(1, length, PAIR))
        first = (jnp.arange(PAIR) == side)[:, None, None, None]
        return jnp.where(first, same[None], crossed[None]).reshape(num_local, *same.shape[1:])

    expert_down_own = expert_grad(expert_hidden, grad_slots, [])
    grad_hidden = batch_dot(grad_slots, expert_down_full, 2, 2)
    grad_gate_rows, grad_up_rows = swiglu_backward(expert_gate_rows, expert_up_rows, grad_hidden)
    expert_gate_own = expert_grad(slot_rows, grad_gate_rows, [])
    grad_input = (
        batch_dot(grad_gate_rows, expert_gate_full, 2, 2) + batch_dot(grad_up_rows, expert_up_full, 2, 2)
    ).astype(BF16)
    grad_routed = scatter_rows(grad_input, chosen_low, num_held, 4, True)
    grad_shidden = dot(grad_low, down_full, 1, 1)
    grad_sgate_rows, grad_sup_rows = swiglu_backward(shared_gate, shared_up, grad_shidden)
    grad_gate_up = jnp.concatenate([grad_sgate_rows, grad_sup_rows], axis=1)
    grad_normed_two = dot(grad_gate_up, gate_up_full, 1, 1) + grad_routed
    _, pull_two = jax.vjp(rms_norm, mixed_rows, gain_two)
    grad_mixed_norm, grad_gain_two = pull_two(grad_normed_two)
    grad_mixed = grad_out + grad_mixed_norm
    grad_mixed_low = grad_mixed.astype(BF16)

    grad_attended = dot(grad_mixed_low, output_full, 1, 1).astype(BF16)
    grad_query, grad_key_value = attend_back(
        query_rows, key_value_all, seg_rows, seg_line, log_total, grad_attended, score_scale
    )
    grad_key_value = jnp.concatenate([grad_key_value[0], grad_key_value[1]], axis=1)
    total = grad_key_value[:tok_rows]
    for step in range(1, back + 1):
        came = shift(total.astype(BF16), "seq", -1)
        total = came.astype(F32) + grad_key_value[step * tok_rows : (step + 1) * tok_rows]
    grad_qkv = jnp.concatenate([grad_query, total.astype(BF16)], axis=1)
    expert_up_own = expert_grad(slot_rows, grad_up_rows, [total])
    grad_normed_one = dot(grad_qkv, qkv_full, 1, 1)
    _, pull_one = jax.vjp(rms_norm, x_float, gain_one)
    grad_x_norm, grad_gain_one = pull_one(grad_normed_one)
    grad_tokens = grad_mixed + grad_x_norm

    gain_grads = jnp.stack([grad_gain_one, grad_gain_two]).reshape(2, devices, -1).swapaxes(0, 1)
    gain_rows = gain_grads.shape[2]
    gain_grads = jnp.pad(gain_grads, ((0, 0), (0, 6), (0, lanes - gain_rows)))
    dense_grads = [
        weight_grad(normed_two, grad_gate_up),
        weight_grad(normed_one, grad_qkv),
        weight_grad(attended, grad_mixed_low),
        weight_grad(shared_hidden, grad_low),
        gain_grads,
    ]
    sums = scatter_dense(dense_grads, 5)
    grad_gate_up_block, grad_qkv_block, grad_output_block, grad_down_block, grad_gain_block = sums
    last = [grad_gain_block]
    grad_expert_down = expert_sum(expert_down_own, last)
    grad_expert_gate = expert_sum(expert_gate_own, last)
    grad_expert_up = expert_sum(expert_up_own, last)
    return (
        block_output[None],
        grad_tokens[None],
        grad_gain_block[0, :gain_rows],
        grad_qkv_block[:, :query_width],
        grad_qkv_block[:, query_width : query_width + key_width],
        grad_qkv_block[:, query_width + key_width :],
        grad_output_block,
        grad_gain_block[1, :gain_rows],
        grad_gate_up_block[:, :shared_width],
        grad_gate_up_block[:, shared_width:],
        grad_down_block,
        grad_expert_gate,
        grad_expert_up,
        grad_expert_down,
    )


def solution(mesh):
    rows = P("fsdp", "seq", None)
    dense = P(("seq", "fsdp"), None)
    gain = P(("seq", "fsdp"))
    return jax.shard_map(
        block,
        mesh=mesh,
        in_specs=(
            rows, rows, P("fsdp", "seq"), P("fsdp", None), rows, rows,
            gain, dense, dense, dense, dense, gain, dense, dense, dense, rows, rows, rows,
        ),
        out_specs=(
            rows, rows, gain, dense, dense, dense, dense, gain, dense, dense, dense, rows, rows, rows,
        ),
        check_vma=False,
    )
```

```python
import functools
import math

import jax
import jax.numpy as jnp
from jax import lax
from jax.experimental import pallas as pl
from jax.experimental.pallas import tpu as pltpu
from jax.sharding import PartitionSpec as P


HEADS = 12
KV_HEADS = 4
HEAD = 128
TOP = 6
EPSILON = 1e-05
MASKED = -1e30
PAIR = 2


BF16 = jnp.bfloat16
F32 = jnp.float32


def exchange(values, axis, bit):
    count = lax.axis_size(axis)
    return lax.ppermute(values, axis, [(i, i ^ bit) for i in range(count)])


def shift(values, axis, step):
    count = lax.axis_size(axis)
    pairs = [(i, i + step) for i in range(count) if 0 <= i + step < count]
    return lax.ppermute(values, axis, pairs)


def after(values, *others):
    return lax.optimization_barrier((values, *others))[0]


def dot(left, right, left_dim, right_dim):
    return lax.dot_general(
        left, right, (((left_dim,), (right_dim,)), ((), ())), preferred_element_type=F32
    )


def batch_dot(left, right, left_dim, right_dim):
    return lax.dot_general(
        left, right, (((left_dim,), (right_dim,)), ((0,), (0,))), preferred_element_type=F32
    )


def rms_norm(values, gain):
    factor = lax.rsqrt(jnp.mean(values * values, axis=-1, keepdims=True) + EPSILON)
    return values * factor * gain


def swiglu(gate_rows, up_rows):
    return jax.nn.silu(gate_rows) * up_rows


def swiglu_backward(gate_rows, up_rows, grad_rows):
    _, pull_back = jax.vjp(swiglu, gate_rows, up_rows)
    grad_gate, grad_up = pull_back(grad_rows)
    return (grad_gate.astype(BF16), grad_up.astype(BF16))


MESH = pl.DeviceIdType.MESH


def grant(scratch, extra):
    size = extra
    for ref in scratch:
        shape = list(ref.shape)
        shape[-2] = -(-shape[-2] // 16) * 16
        size += math.prod(shape) * jnp.dtype(ref.dtype).itemsize
    return min(size + 6 * 2**20, 66 * 10**6)


class Copies:
    def __init__(self, send_sems, recv_sems):
        self.send_sems, self.recv_sems, self.made = send_sems, recv_sems, []

    def start(self, source, target, axis, partner, when=None):
        number = len(self.made)
        copy = pltpu.make_async_remote_copy(
            src_ref=source,
            dst_ref=target,
            send_sem=self.send_sems.at[number],
            recv_sem=self.recv_sems.at[number],
            device_id={axis: partner},
            device_id_type=MESH,
        )
        if when is None:
            copy.start()
        else:
            pl.when(when)(copy.start)
        self.made.append((copy, when))
        return copy

    def finish(self):
        for copy, when in self.made:
            if when is None:
                copy.wait_send()
            else:
                pl.when(when)(copy.wait_send)


def greet(partners):
    barrier = pltpu.get_barrier_semaphore()
    for axis, partner in partners:
        pl.semaphore_signal(barrier, inc=1, device_id={axis: partner}, device_id_type=MESH)
    pl.semaphore_wait(barrier, len(partners))


def bit_of(index, bit):
    return lax.rem(lax.div(index, bit), 2)


def flip(index, bit):
    return index + bit - 2 * bit * bit_of(index, bit)


def flip_all(index, mask):
    bit = 1
    while bit <= mask:
        if mask & bit:
            index = flip(index, bit)
        bit *= 2
    return index


def gather_dense_kernel(length, bits, count, back, *refs):
    extra = 0 if back is None else 1
    shards, expert = refs[:count], refs[count]
    outs, expert_full = refs[count + 1 + extra : 2 * count + 1 + extra], refs[2 * count + 1 + extra]
    if back is None:
        send_sems, recv_sems, local_sems = refs[2 * count + 2 :]
        places = list(outs)
    else:
        tokens = refs[count + 1]
        normed_ref, query_ref, window_ref, held, send_sems, recv_sems, local_sems = refs[2 * count + 3 :]
        places = [held] + list(outs[1:])
    seq, group = lax.axis_index("seq"), lax.axis_index("fsdp")
    own = [bit_of(group, bit) for bit in bits]
    partners = [("seq", flip_all(seq, k)) for k in range(1, length)]
    partners += [("fsdp", flip(group, bit)) for bit in bits]
    greet(partners)
    copies = Copies(send_sems, recv_sems)
    far = len(bits) - 1
    half = length // 2
    side = lax.div(seq, half)
    low = [side * half, (1 - side) * half]
    orders = [list(range(far)), list(range(far))[::-1]]
    hops = length - 1
    stages = hops + far + 1
    waiting = [[] for _ in range(count)]
    right, left = lax.rem(seq + 1, length), lax.rem(seq + length - 1, length)

    def launch(t, stage):
        if stage < hops:
            back_block = lax.rem(seq - stage + length, length)
            next_block = lax.rem(seq + stage, length)
            if stage == 0:
                local = pltpu.make_async_copy(shards[t], places[t].at[(seq, *own)], local_sems.at[t])
                local.start()
            made = []
            for block, target, sends, comes in (
                (back_block, right, (seq >= stage) & (seq + 1 < length), seq > stage),
                (next_block, left, (seq + stage < length) & (seq >= 1), seq + 1 + stage < length),
            ):
                view = places[t].at[(block, *own)]
                source = shards[t] if stage == 0 else view
                made.append((copies.start(source, view, "seq", target, sends).wait_recv, comes))
            if stage == 0:
                made.append((local.wait, None))
            return made
        made = []
        for part in (0, 1):
            where = [pl.ds(low[part], half)] + list(own)
            for done in orders[part][: stage - hops]:
                where[1 + done] = slice(None)
            dim = orders[part][stage - hops] if stage < hops + far else far
            view = places[t].at[tuple(where)]
            made.append((copies.start(view, view, "fsdp", flip(group, bits[dim])).wait_recv, None))
        return made

    def settle(made):
        for wait, when in made:
            if when is None:
                wait()
            else:
                pl.when(when)(wait)

    def ship_expert():
        held_experts, depth = expert.shape[0] // PAIR, expert.shape[1]
        rows = pl.ds(pl.multiple_of(seq * depth, depth), depth)
        parity = lax.rem(seq, PAIR)
        local = pltpu.make_async_copy(
            expert.at[pl.ds(parity * held_experts, held_experts)], expert_full.at[:, rows], local_sems.at[count]
        )
        local.start()
        made = [(local.wait, None)]
        for k in range(1, length):
            mine = pl.ds(lax.rem(parity + k, PAIR) * held_experts, held_experts)
            copy = copies.start(expert.at[mine], expert_full.at[:, rows], "seq", flip_all(seq, k))
            made.append((copy.wait_recv, None))
        return made

    def project():
        rows, width = normed_ref.shape
        query_width = query_ref.shape[1]
        key_width = window_ref.shape[1]

        def columns(start, size):
            return held[(slice(None),) * (2 + far) + (slice(None), pl.ds(start, size))].reshape(width, size)

        gain = columns(query_width + key_width, 128).astype(jnp.float32).T[0:1]
        values = tokens[...].astype(jnp.float32)
        factor = lax.rsqrt(jnp.mean(values * values, axis=-1, keepdims=True) + EPSILON)
        normed_ref[...] = (values * factor * gain).astype(normed_ref.dtype)
        here = pl.ds(back * rows, rows)
        for start in range(0, key_width, 512):
            tile = jnp.dot(
                normed_ref[...], columns(query_width + start, 512), preferred_element_type=jnp.float32
            )
            window_ref[here, pl.ds(start, 512)] = tile.astype(window_ref.dtype)
        for j in range(1, back + 1):

            @pl.when(seq < j)
            def _(j=j):
                window_ref[pl.ds((back - j) * rows, rows)] = jnp.zeros((rows, key_width), window_ref.dtype)

        first = pass_keys(1)
        for start in range(0, query_width, 512):
            tile = jnp.dot(normed_ref[...], columns(start, 512), preferred_element_type=jnp.float32)
            query_ref[:, pl.ds(start, 512)] = tile.astype(query_ref.dtype)
        kept = pltpu.make_async_copy(held, outs[0], local_sems.at[0])
        kept.start()
        return first, kept

    def pass_keys(j):
        rows = normed_ref.shape[0]
        source = window_ref.at[pl.ds((back - j + 1) * rows, rows)]
        target = window_ref.at[pl.ds((back - j) * rows, rows)]
        sends = (seq >= j - 1) & (seq + 1 < length)
        return [(copies.start(source, target, "seq", right, sends).wait_recv, seq >= j)]

    passing, passed = [], 0
    for step in range(count + stages):
        if step == hops + 1:
            expert_waiting = ship_expert()
        if passing:
            settle(passing)
            passing = []
            if passed < back:
                passed += 1
                passing = pass_keys(passed)
        for t in range(count):
            stage = step - t
            if 0 < stage <= stages:
                settle(waiting[t])
            if 0 <= stage < stages:
                waiting[t] = launch(t, stage)
        if step == stages and back is not None:
            passing, kept = project()
            passed = 1
    while passing:
        settle(passing)
        passed += 1
        passing = pass_keys(passed) if passed <= back else []
    settle(expert_waiting)
    copies.finish()
    if back is not None:
        kept.wait()


def gather_dense(shards, expert, tokens, back, key_width):
    length, groups = lax.axis_size("seq"), lax.axis_size("fsdp")
    bits, bit = [], groups // 2
    while bit >= 1:
        bits.append(bit)
        bit //= 2
    count = len(shards)
    number = count * 2 * (length - 1 + len(bits)) + length - 1 + back
    size = sum(s.size * s.dtype.itemsize for s in shards) * length * groups
    experts, depth, wide = expert.shape
    lead = (length,) + (2,) * len(bits)
    rows, width = tokens.shape
    fused = shards[0].shape[0] % 16 == 0
    extra_in, extra_out, extra_scratch = [], [], []
    if fused:
        query_width = shards[0].shape[1] - key_width - 128
        extra_in = [tokens]
        extra_out = [
            jax.ShapeDtypeStruct((rows, width), tokens.dtype),
            jax.ShapeDtypeStruct((rows, query_width), tokens.dtype),
            jax.ShapeDtypeStruct(((back + 1) * rows, key_width), tokens.dtype),
        ]
        extra_scratch = [pltpu.VMEM(lead + shards[0].shape, shards[0].dtype)]
    results = pl.pallas_call(
        functools.partial(gather_dense_kernel, length, bits, count, back if fused else None),
        out_shape=[
            jax.ShapeDtypeStruct((length,) + (2,) * len(bits) + s.shape, s.dtype) for s in shards
        ]
        + [jax.ShapeDtypeStruct((experts // PAIR, length * depth, wide), expert.dtype)]
        + extra_out,
        in_specs=[pl.BlockSpec(memory_space=pltpu.VMEM)] * count
        + [pl.BlockSpec(memory_space=pl.ANY)]
        + [pl.BlockSpec(memory_space=pltpu.VMEM)] * len(extra_in),
        out_specs=[pl.BlockSpec(memory_space=pl.ANY)] * (count + 1)
        + [pl.BlockSpec(memory_space=pltpu.VMEM)] * len(extra_out),
        scratch_shapes=extra_scratch
        + [
            pltpu.SemaphoreType.DMA((number,)),
            pltpu.SemaphoreType.DMA((number,)),
            pltpu.SemaphoreType.DMA((count + 1,)),
        ],
        compiler_params=pltpu.CompilerParams(
            collective_id=0, has_side_effects=True, vmem_limit_bytes=60 * 2**20
        ),
        cost_estimate=pl.CostEstimate(flops=0, bytes_accessed=3 * size, transcendentals=0),
        name="gather_dense",
    )(*shards, expert, *extra_in)
    outs = [out.reshape(-1, out.shape[-1]) for out in results[:count]] + [results[count]]
    return outs + (list(results[count + 1 :]) if fused else [None] * 3)


def scatter_dense_kernel(length, bits, count, *refs):
    grads, outs = refs[:count], refs[count : 2 * count]
    far = len(bits) - 1
    per = 3 + far
    scratch = refs[2 * count : 2 * count + per * count]
    send_sems, recv_sems, local_sems = refs[2 * count + per * count :]
    seq, group = lax.axis_index("seq"), lax.axis_index("fsdp")
    own = [bit_of(group, bit) for bit in bits]
    partners = [("seq", flip_all(seq, k)) for k in range(1, length)]
    partners += [("fsdp", flip(group, bit)) for bit in bits]
    greet(partners)
    copies = Copies(send_sems, recv_sems)
    half = length // 2
    side = lax.div(seq, half)
    low = [side * half, (1 - side) * half]
    orders = [list(range(far))[::-1], list(range(far))]
    stages = far + 2
    everything = (slice(None),) * (1 + far)

    def buffers(t):
        held = scratch[per * t : per * (t + 1)]
        return held[0], held[1], held[2 : 2 + far], held[2 + far]

    waiting = [None] * count

    def add(mine, came, lead, fixed, inner_of):
        start, size = lead
        left = [d for d in range(far) if d not in fixed]

        def body(i, carry):
            z = lax.div(i, 2 ** len(left))
            where, inner = [own[d] for d in range(far)], []
            for k, d in enumerate(left):
                where[d] = lax.rem(lax.div(i, 2 ** (len(left) - 1 - k)), 2)
                inner.append(where[d])
            place = (start + z, *where)
            total = mine[place].astype(jnp.float32) + came[inner_of(start + z, z, inner)].astype(jnp.float32)
            mine[place] = total.astype(mine.dtype)
            return carry

        lax.fori_loop(0, size * 2 ** len(left), body, 0)

    def launch(t, stage):
        mine, came_core, came_far, came_seq = buffers(t)
        if stage == 0:
            local = pltpu.make_async_copy(grads[t].at[(*everything, own[far])], mine, local_sems.at[t])
            local.start()
            sent = grads[t].at[(*everything, 1 - own[far])]
            return [copies.start(sent, came_core, "fsdp", flip(group, bits[far]))], local
        if stage <= far:
            made = []
            for part in (0, 1):
                order = orders[part]
                if stage == 1:
                    add(mine, came_core, (low[part], half), [], lambda z, at, inner: (z, *inner))
                else:
                    came = came_far[stage - 2].at[part]
                    add(mine, came, (low[part], half), order[: stage - 1], lambda z, at, inner: (at, *inner))
                dim = order[stage - 1]
                where = [slice(None)] * far
                for d in order[: stage - 1]:
                    where[d] = own[d]
                where[dim] = 1 - own[dim]
                made.append(
                    copies.start(
                        mine.at[(pl.ds(low[part], half), *where)],
                        came_far[stage - 1].at[part],
                        "fsdp",
                        flip(group, bits[dim]),
                    )
                )
            return made, None
        for part in (0, 1):
            came = came_far[far - 1].at[part]
            add(mine, came, (low[part], half), orders[part], lambda z, at, inner: (at,))
        made = []
        for k in range(1, length):
            other = flip_all(seq, k)
            made.append(copies.start(mine.at[(other, *own[:far])], came_seq.at[k - 1], "seq", other))
        return made, None

    def close(t):
        mine, _, _, came_seq = buffers(t)
        total = mine[(seq, *own[:far])].astype(jnp.float32)
        for k in range(1, length):
            total = total + came_seq[k - 1].astype(jnp.float32)
        outs[t][...] = total

    for step in range(count + stages):
        for t in range(count):
            stage = step - t
            if 0 < stage <= stages:
                made, local = waiting[t]
                for copy in made:
                    copy.wait_recv()
                if local is not None:
                    local.wait()
            if 0 <= stage < stages:
                waiting[t] = launch(t, stage)
            elif stage == stages:
                close(t)
    copies.finish()


def scatter_dense(grads, collective_id):
    length, groups = lax.axis_size("seq"), lax.axis_size("fsdp")
    bits, bit = [], groups // 2
    while bit >= 1:
        bits.append(bit)
        bit //= 2
    far = len(bits) - 1
    count = len(grads)
    number = count * (1 + 2 * far + length - 1)
    size = sum(g.size * g.dtype.itemsize for g in grads)
    scratch = []
    for g in grads:
        block = g.shape[1:]
        scratch += [pltpu.VMEM((length,) + (2,) * far + block, g.dtype)] * 2
        scratch += [
            pltpu.VMEM((2, length // 2) + (2,) * (far - 1 - s) + block, g.dtype) for s in range(far)
        ]
        scratch.append(pltpu.VMEM((length - 1,) + block, g.dtype))
    return pl.pallas_call(
        functools.partial(scatter_dense_kernel, length, bits, count),
        out_shape=[jax.ShapeDtypeStruct(g.shape[1:], jnp.float32) for g in grads],
        in_specs=[pl.BlockSpec(memory_space=pl.ANY)] * count,
        out_specs=[pl.BlockSpec(memory_space=pltpu.VMEM)] * count,
        scratch_shapes=scratch
        + [
            pltpu.SemaphoreType.DMA((number,)),
            pltpu.SemaphoreType.DMA((number,)),
            pltpu.SemaphoreType.DMA((count,)),
        ],
        compiler_params=pltpu.CompilerParams(
            collective_id=collective_id, has_side_effects=True, vmem_limit_bytes=grant(scratch, 0)
        ),
        cost_estimate=pl.CostEstimate(flops=0, bytes_accessed=3 * size, transcendentals=0),
        name="scatter_dense",
    )(*[g.reshape((length,) + (2,) * len(bits) + g.shape[1:]) for g in grads])


def sum_dense_kernel(length, bits, cuts, plan, keys_at, back, *refs):
    count = len(cuts)
    weights = count - 1
    act_count = 1 + max(a for group in plan for a, _ in group)
    grad_count = 1 + max(g for group in plan for _, g in group if g is not None)
    acts, grads = refs[:act_count], refs[act_count : act_count + grad_count]
    ready, window, *refs = refs[act_count + grad_count :]
    number = sum(len(cut) for cut in cuts)
    flat_outs, keys_out, refs = list(refs[:number]), refs[number], refs[number + 1 :]
    outs = [[flat_outs.pop(0) for _ in cut] for cut in cuts]
    far = len(bits) - 1
    per = 3 + far
    scratch = refs[: per * count]
    keys_sum, keys_sent, keys_came, send_sems, recv_sems = refs[per * count :]
    seq, group = lax.axis_index("seq"), lax.axis_index("fsdp")
    own = [bit_of(group, bit) for bit in bits]
    partners = [("seq", flip_all(seq, k)) for k in range(1, length)]
    partners += [("fsdp", flip(group, bit)) for bit in bits]
    greet(partners)
    copies = Copies(send_sems, recv_sems)
    half = length // 2
    side = lax.div(seq, half)
    low = [side * half, (1 - side) * half]
    orders = [list(range(far))[::-1], list(range(far))]
    stages = far + 2
    everything = (slice(None),) * (1 + far)
    rows, key_width = keys_sum.shape[0], window.shape[2]
    left = lax.rem(seq + length - 1, length)

    def buffers(t):
        held = scratch[per * t : per * (t + 1)]
        return held[0], held[1], held[2 : 2 + far], held[2 + far]

    def key_piece(b, part):
        return window[part, pl.ds(b * rows, rows)]

    def send_keys(j):
        copy = copies.start(keys_sent.at[j], keys_came.at[j], "seq", left, seq >= 1)
        return copy

    def advance_keys(j, copy):
        for part in (0, 1):
            keys_sum[:, pl.ds(part * key_width, key_width)] = key_piece(j, part)

        @pl.when(seq + 1 < length)
        def _():
            copy.wait_recv()
            keys_sum[...] = keys_sum[...] + keys_came[j - 1].astype(jnp.float32)

        if j < back:
            keys_sent[j] = keys_sum[...].astype(keys_sent.dtype)
            return send_keys(j)
        keys_out[...] = keys_sum[...].astype(keys_out.dtype)
        return None

    def produce(t):
        held = buffers(t)[0]
        if t == weights:
            held[...] = ready[...]
            return
        block = held.shape[-2]

        def body(z, carry):
            start = 0
            for a, g in plan[t]:
                depth = acts[a].shape[0] // length
                left_rows = acts[a][pl.ds(pl.multiple_of(z * depth, depth), depth)]
                source = keys_out if g is None else grads[g]
                for c in range(0, source.shape[1], 512):
                    tile = jnp.dot(left_rows, source[:, c : c + 512], preferred_element_type=jnp.float32)
                    tile = tile.astype(held.dtype).reshape((2,) * (far + 1) + (block, 512))
                    held[(z, *(slice(None),) * (far + 2), pl.ds(start, 512))] = tile
                    start += 512
            return carry

        lax.fori_loop(0, length, body, 0)

    def add(held, came, lead, fixed, inner_of):
        start, size = lead
        free = [d for d in range(far) if d not in fixed]

        def body(i, carry):
            z = lax.div(i, 2 ** len(free))
            where, inner = [own[d] for d in range(far)], []
            for k, d in enumerate(free):
                where[d] = lax.rem(lax.div(i, 2 ** (len(free) - 1 - k)), 2)
                inner.append(where[d])
            place = (start + z, *where, own[far])
            total = held[place].astype(jnp.float32) + came[inner_of(start + z, z, inner)].astype(jnp.float32)
            held[place] = total.astype(held.dtype)
            return carry

        lax.fori_loop(0, size * 2 ** len(free), body, 0)

    def launch(t, stage):
        held, came_core, came_far, came_seq = buffers(t)
        if stage == 0:
            produce(t)
            return [copies.start(held.at[(*everything, 1 - own[far])], came_core, "fsdp", flip(group, bits[far]))]
        made = []
        if stage <= far:
            for part in (0, 1):
                order = orders[part]
                if stage == 1:
                    add(held, came_core, (low[part], half), [], lambda z, at, inner: (z, *inner))
                else:
                    came = came_far[stage - 2].at[part]
                    add(held, came, (low[part], half), order[: stage - 1], lambda z, at, inner: (at, *inner))
                dim = order[stage - 1]
                where = [slice(None)] * far
                for d in order[: stage - 1]:
                    where[d] = own[d]
                where[dim] = 1 - own[dim]
                source = held.at[(pl.ds(low[part], half), *where, own[far])]
                made.append(
                    copies.start(source, came_far[stage - 1].at[part], "fsdp", flip(group, bits[dim]))
                )
            return made
        for part in (0, 1):
            add(held, came_far[far - 1].at[part], (low[part], half), orders[part], lambda z, at, inner: (at,))
        for k in range(1, length):
            other = flip_all(seq, k)
            made.append(copies.start(held.at[(other, *own)], came_seq.at[k - 1], "seq", other))
        return made

    def close(t):
        held, _, _, came_seq = buffers(t)
        total = held[(seq, *own)].astype(jnp.float32)
        for k in range(1, length):
            total = total + came_seq[k - 1].astype(jnp.float32)
        start = 0
        for out, size in zip(outs[t], cuts[t]):
            out[...] = total[:, start : start + size]
            start += size

    for part in (0, 1):
        keys_sent[0, :, pl.ds(part * key_width, key_width)] = key_piece(0, part).astype(keys_sent.dtype)
    flying = send_keys(0)
    waiting = [[] for _ in range(count)]
    for step in range(count + stages - 1):
        for t in range(count):
            stage = step - t
            if 0 < stage < stages:
                for copy in waiting[t]:
                    copy.wait_recv()
            if stage == 0 and t == keys_at:
                advance_keys(back, flying)
            if 0 <= stage < stages:
                waiting[t] = launch(t, stage)
        if 1 <= step < back:
            flying = advance_keys(step, flying)
    for t in range(count):
        for copy in waiting[t]:
            copy.wait_recv()
        close(t)
    copies.finish()


def sum_dense(acts, grads, ready, window, cuts, plan, collective_id):
    length, groups = lax.axis_size("seq"), lax.axis_size("fsdp")
    bits, bit = [], groups // 2
    while bit >= 1:
        bits.append(bit)
        bit //= 2
    far = len(bits) - 1
    devices = length * groups
    rows = grads[0].shape[0]
    back = window.shape[1] // rows - 1
    key_width = 2 * window.shape[2]
    blocks = [
        ((acts[group[0][0]].shape[0] // devices, sum(cut)), grads[0].dtype) for group, cut in zip(plan, cuts)
    ]
    keys_at = [any(g is None for _, g in group) for group in plan].index(True)
    blocks.append((ready.shape[1:], ready.dtype))
    count = len(blocks)
    number = count * (1 + 2 * far + length - 1) + back
    scratch = []
    for block, dtype in blocks:
        scratch.append(pltpu.VMEM((length,) + (2,) * (far + 1) + block, dtype))
        scratch.append(pltpu.VMEM((length,) + (2,) * far + block, dtype))
        scratch += [pltpu.VMEM((2, length // 2) + (2,) * (far - 1 - s) + block, dtype) for s in range(far)]
        scratch.append(pltpu.VMEM((length - 1,) + block, dtype))
    scratch.append(pltpu.VMEM((rows, key_width), jnp.float32))
    scratch += [pltpu.VMEM((back, rows, key_width), grads[0].dtype)] * 2
    elements = sum(math.prod(block) for block, _ in blocks) * devices
    return pl.pallas_call(
        functools.partial(sum_dense_kernel, length, bits, cuts, plan, keys_at, back),
        out_shape=[
            jax.ShapeDtypeStruct((block[0], size), jnp.float32)
            for (block, _), cut in zip(blocks, cuts)
            for size in cut
        ]
        + [jax.ShapeDtypeStruct((rows, key_width), grads[0].dtype)],
        in_specs=[pl.BlockSpec(memory_space=pltpu.VMEM)] * (len(acts) + len(grads) + 2),
        out_specs=[pl.BlockSpec(memory_space=pltpu.VMEM)] * (sum(len(cut) for cut in cuts) + 1),
        scratch_shapes=scratch + [pltpu.SemaphoreType.DMA((number,))] * 2,
        compiler_params=pltpu.CompilerParams(
            collective_id=collective_id, has_side_effects=True, vmem_limit_bytes=67 * 10**6
        ),
        cost_estimate=pl.CostEstimate(
            flops=2 * elements * rows, bytes_accessed=4 * elements, transcendentals=0
        ),
        name="sum_dense",
    )(*acts, *grads, ready.reshape((length,) + (2,) * len(bits) + ready.shape[1:]), window)


def row_dims():
    groups = lax.axis_size("fsdp")
    dims, bit = [("seq", 1)], groups // 2
    while bit >= 1:
        dims.append(("fsdp", bit))
        bit //= 2
    return dims


def row_places(dims):
    seq, group = lax.axis_index("seq"), lax.axis_index("fsdp")
    index = {"seq": seq, "fsdp": group}
    own = [bit_of(index[axis], bit) for axis, bit in dims]
    partner = [(axis, flip(index[axis], bit)) for axis, bit in dims]
    return own, partner


def row_orders(far, light):
    if light:
        return [[0] + [1 + (i + k) % (far - 1) for k in range(far - 1)] for i in range(far - 1)]
    return [[(i + k) % far for k in range(far)] for i in range(far)]


def gather_rows_kernel(dims, orders, held, rows_ref, pick_ref, slots_ref, buffer, send_sems, recv_sems, local_sem):
    own, partner = row_places(dims)
    greet(partner)
    copies = Copies(send_sems, recv_sems)
    far = len(dims) - 1
    pieces = len(orders)
    width = rows_ref.shape[1] // pieces
    capacity = slots_ref.shape[-2]

    def view(piece, done):
        where = list(own)
        for d in done:
            where[d] = slice(None)
        return buffer.at[(piece, *where)]

    flying, local = [], []
    for piece in range(pieces):
        cut = rows_ref.at[:, pl.ds(piece * width, width)]
        flying.append(copies.start(cut, view(piece, []), *partner[orders[piece][0]]))
        local.append(pltpu.make_async_copy(cut, view(piece, []), local_sem.at[piece]))
        local[piece].start()
    for copy in local:
        copy.wait()

    def pick_block(piece, where):
        taken = jnp.dot(
            pick_ref[tuple(where)], buffer[(piece, *where)], preferred_element_type=jnp.float32
        ).astype(slots_ref.dtype)
        for e in range(held):
            slots_ref[(e, *where, slice(None), pl.ds(piece * width, width))] = taken[
                e * capacity : (e + 1) * capacity
            ]

    def pick_all(piece, core):
        def body(i, carry):
            where, rest = [], i
            for d in range(far):
                where.append(lax.rem(lax.div(rest, 2 ** (far - 1 - d)), 2))
            pick_block(piece, where + [core])
            return carry

        lax.fori_loop(0, 2**far, body, 0)

    for stage in range(1, far + 1):
        for piece in range(pieces):
            flying[piece].wait_recv()
            order = orders[piece]
            done = order[:stage]
            ref = view(piece, done)
            flying[piece] = copies.start(ref, ref, *(partner[order[stage]] if stage < far else partner[far]))
    for piece in range(pieces):
        pick_all(piece, own[far])
    for piece in range(pieces):
        flying[piece].wait_recv()
        pick_all(piece, 1 - own[far])
    copies.finish()


def gather_rows(rows, pick_low, held, collective_id, light):
    dims = row_dims()
    far = len(dims) - 1
    orders = row_orders(far, light)
    count, feat = rows.shape
    width = feat // len(orders)
    sources = 2 ** len(dims)
    capacity = pick_low.shape[1] // held
    lead = (2,) * len(dims)
    number = len(orders) * (far + 1)
    scratch = [pltpu.VMEM((len(orders),) + lead + (count, width), rows.dtype)]
    slots = pl.pallas_call(
        functools.partial(gather_rows_kernel, dims, orders, held),
        out_shape=jax.ShapeDtypeStruct((held,) + lead + (capacity, feat), rows.dtype),
        in_specs=[pl.BlockSpec(memory_space=pltpu.VMEM)] * 2,
        out_specs=pl.BlockSpec(memory_space=pltpu.VMEM),
        scratch_shapes=scratch
        + [pltpu.SemaphoreType.DMA((n,)) for n in (number, number, len(orders))],
        compiler_params=pltpu.CompilerParams(
            collective_id=collective_id,
            has_side_effects=True,
            vmem_limit_bytes=grant(scratch, 12 * 2**20),
        ),
        cost_estimate=pl.CostEstimate(
            flops=2 * sources * pick_low.shape[1] * count * feat,
            bytes_accessed=6 * sources * count * feat,
            transcendentals=0,
        ),
        name="gather_rows",
    )(rows, pick_low.reshape(lead + pick_low.shape[1:]))
    return slots.reshape(held, sources * capacity, feat)


def scatter_rows_kernel(
    dims, orders, held, slots_ref, pick_ref, out_ref, mine, other, came_core, came_far, send_sems, recv_sems
):
    own, partner = row_places(dims)
    greet(partner)
    copies = Copies(send_sems, recv_sems)
    far = len(dims) - 1
    pieces = len(orders)
    width = out_ref.shape[1] // pieces
    capacity = slots_ref.shape[-2]
    count = out_ref.shape[0]

    def spread(piece, core, target):
        def body(i, carry):
            where = [lax.rem(lax.div(i, 2 ** (far - 1 - d)), 2) for d in range(far)]
            total = jnp.zeros((count, width), jnp.float32)
            for e in range(held):
                rows = slots_ref[(e, *where, core, slice(None), pl.ds(piece * width, width))]
                chosen = pick_ref[(*where, core, pl.ds(e * capacity, capacity))]
                total = total + lax.dot_general(
                    chosen, rows, (((0,), (0,)), ((), ())), preferred_element_type=jnp.float32
                )
            target[(piece, *where)] = total.astype(target.dtype)
            return carry

        lax.fori_loop(0, 2**far, body, 0)

    flying = []
    for piece in range(pieces):
        spread(piece, 1 - own[far], other)
        flying.append(copies.start(other.at[piece], came_core.at[piece], *partner[far]))
    for piece in range(pieces):
        spread(piece, own[far], mine)

    def add_into(piece, fixed, came_view):
        left = [d for d in range(far) if d not in fixed]

        def body(i, carry):
            where, inner = [None] * far, []
            for k, d in enumerate(left):
                where[d] = lax.rem(lax.div(i, 2 ** (len(left) - 1 - k)), 2)
                inner.append(where[d])
            for d in fixed:
                where[d] = own[d]
            total = mine[(piece, *where)].astype(jnp.float32) + came_view[tuple(inner)].astype(jnp.float32)
            mine[(piece, *where)] = total.astype(mine.dtype)
            return carry

        lax.fori_loop(0, 2 ** len(left), body, 0)

    for stage in range(far):
        for piece in range(pieces):
            order = orders[piece][::-1]
            fixed = order[:stage]
            flying[piece].wait_recv()
            add_into(piece, fixed, came_core.at[piece] if stage == 0 else came_far[stage - 1].at[piece])
            dim = order[stage]
            where = [slice(None)] * far
            for d in fixed:
                where[d] = own[d]
            where[dim] = 1 - own[dim]
            flying[piece] = copies.start(
                mine.at[(piece, *where)], came_far[stage].at[piece], *partner[dim]
            )
    for piece in range(pieces):
        flying[piece].wait_recv()
        out_ref[:, pl.ds(piece * width, width)] = mine[(piece, *own[:far])].astype(jnp.float32) + came_far[far - 1][piece].astype(
            jnp.float32
        )
    copies.finish()


def scatter_rows(slots, pick_low, held, collective_id, light):
    dims = row_dims()
    far = len(dims) - 1
    orders = row_orders(far, light)
    count, feat = pick_low.shape[2], slots.shape[2]
    width = feat // len(orders)
    sources = 2 ** len(dims)
    capacity = pick_low.shape[1] // held
    lead = (2,) * len(dims)
    number = len(orders) * (far + 1)

    scratch = [pltpu.VMEM((len(orders),) + (2,) * far + (count, width), slots.dtype)] * 3
    scratch += [pltpu.VMEM((len(orders),) + (2,) * (far - 1 - s) + (count, width), slots.dtype) for s in range(far)]

    def kernel(slots_ref, pick_ref, out_ref, mine, other, came_core, *rest):
        came_far, sems = rest[:far], rest[far:]
        scatter_rows_kernel(
            dims, orders, held, slots_ref, pick_ref, out_ref, mine, other, came_core, came_far, *sems
        )

    return pl.pallas_call(
        kernel,
        out_shape=jax.ShapeDtypeStruct((count, feat), jnp.float32),
        in_specs=[pl.BlockSpec(memory_space=pltpu.VMEM)] * 2,
        out_specs=pl.BlockSpec(memory_space=pltpu.VMEM),
        scratch_shapes=scratch + [pltpu.SemaphoreType.DMA((number,)), pltpu.SemaphoreType.DMA((number,))],
        compiler_params=pltpu.CompilerParams(
            collective_id=collective_id,
            has_side_effects=True,
            vmem_limit_bytes=grant(scratch, 4 * 2**20),
        ),
        cost_estimate=pl.CostEstimate(
            flops=2 * sources * pick_low.shape[1] * count * feat,
            bytes_accessed=6 * sources * count * feat,
            transcendentals=0,
        ),
        name="scatter_rows",
    )(slots.reshape((held,) + lead + (capacity, feat)), pick_low.reshape(lead + pick_low.shape[1:]))


def allowed_keys(seg_rows_ref, seg_keys_ref, back_rows):
    shape = (seg_rows_ref.shape[0], seg_keys_ref.shape[1])
    row = lax.broadcasted_iota(jnp.int32, shape, 0) + back_rows
    key = lax.broadcasted_iota(jnp.int32, shape, 1)
    return (key <= row) & (seg_rows_ref[...] == seg_keys_ref[...])


def attend_kernel(scale, back_rows, query, key, value, seg_rows, seg_keys, out, log_total):
    allowed = allowed_keys(seg_rows, seg_keys, back_rows)
    keys, values = key[...], value[...]
    lane = lax.broadcasted_iota(jnp.int32, (query.shape[0], 128), 1)
    logs = jnp.zeros((query.shape[0], 128), jnp.float32)
    for j in range(query.shape[1] // HEAD):
        columns = slice(j * HEAD, (j + 1) * HEAD)
        scores = lax.dot_general(
            query[:, columns], keys, (((1,), (1,)), ((), ())), preferred_element_type=jnp.float32
        )
        scores = jnp.where(allowed, scores * scale, MASKED)
        top = jnp.max(scores, axis=1, keepdims=True)
        weights = jnp.exp(scores - top)
        total = jnp.sum(weights, axis=1, keepdims=True)
        prob = (weights * (1.0 / total)).astype(jnp.bfloat16)
        out[:, columns] = jnp.dot(prob, values, preferred_element_type=jnp.float32).astype(out.dtype)
        logs = jnp.where(lane == j, top + jnp.log(total), logs)
    log_total[...] = logs


def attend_back_kernel(
    scale, back_rows, query, key, value, seg_rows, seg_keys, log_total, grad, grad_query, grad_key_value
):
    allowed = allowed_keys(seg_rows, seg_keys, back_rows)
    keys, values = key[...], value[...]
    grad_keys = jnp.zeros(keys.shape, jnp.float32)
    grad_values = jnp.zeros(values.shape, jnp.float32)
    for j in range(query.shape[1] // HEAD):
        columns = slice(j * HEAD, (j + 1) * HEAD)
        rows, grad_rows = query[:, columns], grad[:, columns]
        scores = lax.dot_general(
            rows, keys, (((1,), (1,)), ((), ())), preferred_element_type=jnp.float32
        )
        scores = jnp.where(allowed, scores * scale, MASKED)
        prob = jnp.exp(scores - log_total[:, j : j + 1])
        grad_prob = lax.dot_general(
            grad_rows, values, (((1,), (1,)), ((), ())), preferred_element_type=jnp.float32
        )
        delta = jnp.sum(prob * grad_prob, axis=1, keepdims=True)
        grad_scores = (prob * (grad_prob - delta)).astype(jnp.bfloat16)
        grad_query[:, columns] = (
            jnp.dot(grad_scores, keys, preferred_element_type=jnp.float32) * scale
        ).astype(grad_query.dtype)
        grad_keys = grad_keys + lax.dot_general(
            grad_scores, rows, (((0,), (0,)), ((), ())), preferred_element_type=jnp.float32
        )
        grad_values = grad_values + lax.dot_general(
            prob.astype(jnp.bfloat16), grad_rows, (((0,), (0,)), ((), ())), preferred_element_type=jnp.float32
        )
    grad_key_value[0] = grad_keys * scale
    grad_key_value[1] = grad_values


def attend_specs(tok_rows, window, group_width):
    return [
        pl.BlockSpec((tok_rows, group_width), lambda g: (0, g)),
        pl.BlockSpec((window, HEAD), lambda g: (0, g)),
        pl.BlockSpec((window, HEAD), lambda g: (0, KV_HEADS + g)),
        pl.BlockSpec((tok_rows, 1), lambda g: (0, 0)),
        pl.BlockSpec((1, window), lambda g: (0, 0)),
    ]


def attend(query, key_value, seg_rows, seg_keys, scale):
    tok_rows, window = query.shape[0], key_value.shape[0]
    group_width = query.shape[1] // KV_HEADS
    return pl.pallas_call(
        functools.partial(attend_kernel, scale, window - tok_rows),
        grid=(KV_HEADS,),
        in_specs=attend_specs(tok_rows, window, group_width),
        out_specs=[
            pl.BlockSpec((tok_rows, group_width), lambda g: (0, g)),
            pl.BlockSpec((None, tok_rows, 128), lambda g: (g, 0, 0)),
        ],
        out_shape=[
            jax.ShapeDtypeStruct(query.shape, query.dtype),
            jax.ShapeDtypeStruct((KV_HEADS, tok_rows, 128), jnp.float32),
        ],
        compiler_params=pltpu.CompilerParams(vmem_limit_bytes=32 * 2**20),
        cost_estimate=pl.CostEstimate(
            flops=4 * HEADS * tok_rows * window * HEAD,
            bytes_accessed=8 * query.size,
            transcendentals=HEADS * tok_rows * window,
        ),
        name="attend",
    )(query, key_value, key_value, seg_rows, seg_keys)


def attend_back(query, key_value, seg_rows, seg_keys, log_total, grad, scale):
    tok_rows, window = query.shape[0], key_value.shape[0]
    group_width = query.shape[1] // KV_HEADS
    return pl.pallas_call(
        functools.partial(attend_back_kernel, scale, window - tok_rows),
        grid=(KV_HEADS,),
        in_specs=attend_specs(tok_rows, window, group_width)
        + [
            pl.BlockSpec((None, tok_rows, 128), lambda g: (g, 0, 0)),
            pl.BlockSpec((tok_rows, group_width), lambda g: (0, g)),
        ],
        out_specs=[
            pl.BlockSpec((tok_rows, group_width), lambda g: (0, g)),
            pl.BlockSpec((2, window, HEAD), lambda g: (0, 0, g)),
        ],
        out_shape=[
            jax.ShapeDtypeStruct(query.shape, query.dtype),
            jax.ShapeDtypeStruct((2, window, KV_HEADS * HEAD), jnp.float32),
        ],
        compiler_params=pltpu.CompilerParams(vmem_limit_bytes=32 * 2**20),
        cost_estimate=pl.CostEstimate(
            flops=10 * HEADS * tok_rows * window * HEAD,
            bytes_accessed=16 * query.size,
            transcendentals=HEADS * tok_rows * window,
        ),
        name="attend_back",
    )(query, key_value, key_value, seg_rows, seg_keys, log_total, grad)


def block(
    tokens,
    teacher,
    valid_mask,
    segment_ids,
    routes,
    gate_weights,
    norm1_gain,
    query_weight,
    key_weight,
    value_weight,
    output_weight,
    norm2_gain,
    shared_gate_weight,
    shared_up_weight,
    shared_down_weight,
    expert_gate_weight,
    expert_up_weight,
    expert_down_weight,
):
    length, groups = lax.axis_size("seq"), lax.axis_size("fsdp")
    seq_index, group_index = lax.axis_index("seq"), lax.axis_index("fsdp")
    devices = length * groups
    tok_rows, feat_width = tokens.shape[1], tokens.shape[2]
    seq_len = segment_ids.shape[1]
    score_scale = 1.0 / math.sqrt(HEAD)
    key_width = KV_HEADS * HEAD
    query_width = HEADS * HEAD
    shared_width = shared_gate_weight.shape[1]

    lanes = 128
    gains = jnp.pad(jnp.stack([norm1_gain, norm2_gain], axis=1), ((0, 0), (0, lanes - 2)))
    meta = jnp.concatenate([routes[0].T.astype(F32), gate_weights[0].T], axis=0)
    meta = jnp.pad(meta, ((0, 16 - 2 * TOP), (0, 0)))
    longest = seq_len // 2
    back = min(length - 1, -(-(longest - 1) // tok_rows))
    gathered = gather_dense(
        [
            jnp.concatenate([query_weight, key_weight, value_weight, gains], axis=1),
            output_weight,
            jnp.concatenate([shared_gate_weight, shared_up_weight], axis=1),
            shared_down_weight,
            meta,
        ],
        expert_gate_weight,
        tokens[0],
        back,
        2 * key_width,
    )
    qkv_full, output_full, gate_up_full, down_full, meta, expert_gate_full = gathered[:6]
    normed_one, query_rows, key_value_all = gathered[6:]

    def weight_grad(rows, grad_rows):
        grad = dot(rows, grad_rows, 0, 0).astype(BF16)
        return grad.reshape(devices, -1, grad.shape[1])

    qkv_width = query_width + 2 * key_width
    gain_plain = qkv_full[:, qkv_width : qkv_width + 2].T.astype(F32)
    qkv_full = qkv_full[:, :qkv_width]
    gain_one, gain_two = gain_plain[0], gain_plain[1]

    num_local = expert_gate_weight.shape[0]
    num_held = num_local // PAIR
    side = seq_index % PAIR

    def share(weight, k):
        return lax.dynamic_slice_in_dim(weight, (side ^ (k % PAIR)) * num_held, num_held, axis=0)

    def collect_start(weight, wait):
        sent = after(weight, *wait)
        return [exchange(share(sent, k), "seq", k) for k in range(1, length)]

    def collect_done(weight, came):
        part = weight.shape[1]
        full = jnp.zeros((num_held, length * part, weight.shape[2]), weight.dtype)
        for k, block in enumerate([share(weight, 0)] + came):
            full = lax.dynamic_update_slice(full, block, (0, (seq_index ^ k) * part, 0))
        return full

    x_float = tokens[0].astype(F32)
    if normed_one is None:
        normed_one = rms_norm(x_float, gain_one).astype(BF16)
        qkv_rows = dot(normed_one, qkv_full, 1, 0).astype(BF16)
        query_rows = qkv_rows[:, :query_width]
        key_value = [qkv_rows[:, query_width:]]
        for _ in range(back):
            key_value.insert(0, shift(key_value[0], "seq", 1))
        key_value_all = jnp.concatenate(key_value, axis=0)
    up_came = collect_start(expert_up_weight, [key_value_all])
    window = (back + 1) * tok_rows
    seg_padded = jnp.concatenate([jnp.full((back * tok_rows,), -1, jnp.int32), segment_ids[0]])
    seg_keys = lax.dynamic_slice_in_dim(seg_padded, seq_index * tok_rows, window)
    seg_here = seg_keys[back * tok_rows :]
    seg_rows, seg_line = seg_here[:, None], seg_keys[None, :]
    attended, log_total = attend(query_rows, key_value_all, seg_rows, seg_line, score_scale)
    mixed_rows = x_float + dot(attended, output_full, 1, 0)
    normed_two = rms_norm(mixed_rows, gain_two).astype(BF16)

    experts_all = num_local * groups
    capacity = tok_rows * TOP * 4 // (3 * experts_all)
    meta = lax.dynamic_slice_in_dim(
        meta.reshape(length, groups, 16, tok_rows), seq_index // PAIR * PAIR, PAIR, axis=0
    ).reshape(PAIR * groups, 16, tok_rows)
    route_all, gate_all = meta[:, :TOP], meta[:, TOP : 2 * TOP]
    held_ids = group_index * num_local + side * num_held + jnp.arange(num_held, dtype=jnp.int32)
    named = route_all[:, None] == held_ids.astype(F32)[None, :, None, None]
    has = jnp.any(named, axis=2)
    gate_of = jnp.sum(jnp.where(named, gate_all[:, None], 0.0), axis=2)
    token_order = jnp.arange(tok_rows, dtype=jnp.int32)
    earlier = (token_order[:, None] < token_order[None, :]).astype(BF16)
    before = lax.dot_general(
        has.astype(BF16), earlier, (((2,), (0,)), ((), ())), preferred_element_type=F32
    )
    slot_number = jnp.arange(capacity, dtype=F32)
    chosen = has[:, :, None] & (before[:, :, None] == slot_number[None, None, :, None])
    gate_slots = jnp.sum(jnp.where(chosen, gate_of[:, :, None], 0.0), axis=3)
    sources = PAIR * groups
    chosen_low = chosen.astype(BF16).reshape(sources, num_held * capacity, tok_rows)
    gate_canonical = jnp.moveaxis(gate_slots, 0, 1).reshape(num_held, sources * capacity, 1)
    down_came = collect_start(expert_down_weight, [normed_two])
    slot_rows = gather_rows(normed_two, chosen_low, num_held, 1, False)

    gate_up = dot(normed_two, gate_up_full, 1, 0)
    shared_gate, shared_up = gate_up[:, :shared_width], gate_up[:, shared_width:]
    shared_hidden = swiglu(shared_gate, shared_up).astype(BF16)
    shared_out = dot(shared_hidden, down_full, 1, 0)
    expert_gate_rows = batch_dot(slot_rows, expert_gate_full, 2, 1)
    up_came = [after(came, shared_out) for came in up_came]
    expert_up_full = collect_done(expert_up_weight, up_came)
    expert_up_rows = batch_dot(slot_rows, expert_up_full, 2, 1)
    expert_hidden = swiglu(expert_gate_rows, expert_up_rows).astype(BF16)
    expert_down_full = collect_done(
        expert_down_weight, [after(came, expert_hidden) for came in down_came]
    )
    expert_output = (gate_canonical * batch_dot(expert_hidden, expert_down_full, 2, 1)).astype(BF16)
    routed = scatter_rows(expert_output, chosen_low, num_held, 2, False)

    output = mixed_rows + shared_out + routed
    block_output = output.astype(BF16)
    valid_rows = valid_mask[0].astype(F32)[:, None]
    grad_out = valid_rows * (output - teacher[0].astype(F32))
    grad_low = grad_out.astype(BF16)

    grad_slots = gather_rows(grad_low, chosen_low, num_held, 3, False)
    grad_slots = (gate_canonical * grad_slots.astype(F32)).astype(BF16)

    def expert_grad(left, right, wait):
        grad = after(batch_dot(left, right, 1, 1).astype(BF16), *wait)
        rows = grad.shape[1] // length
        own = [None] * length
        for k in range(length):
            slab = lax.dynamic_slice_in_dim(grad, (seq_index ^ k) * rows, rows, axis=1)
            own[k] = exchange(slab, "seq", k) if k else slab
        return own

    def expert_sum(own, wait):
        own = [after(part, *wait) for part in own]
        same = sum(own[k].astype(F32) for k in range(0, length, PAIR))
        crossed = sum(own[k].astype(F32) for k in range(1, length, PAIR))
        first = (jnp.arange(PAIR) == side)[:, None, None, None]
        return jnp.where(first, same[None], crossed[None]).reshape(num_local, *same.shape[1:])

    expert_down_own = expert_grad(expert_hidden, grad_slots, [])
    grad_hidden = batch_dot(grad_slots, expert_down_full, 2, 2)
    grad_gate_rows, grad_up_rows = swiglu_backward(expert_gate_rows, expert_up_rows, grad_hidden)
    expert_gate_own = expert_grad(slot_rows, grad_gate_rows, [])
    grad_input = (
        batch_dot(grad_gate_rows, expert_gate_full, 2, 2) + batch_dot(grad_up_rows, expert_up_full, 2, 2)
    ).astype(BF16)
    grad_routed = scatter_rows(grad_input, chosen_low, num_held, 4, True)
    grad_shidden = dot(grad_low, down_full, 1, 1)
    grad_sgate_rows, grad_sup_rows = swiglu_backward(shared_gate, shared_up, grad_shidden)
    grad_gate_up = jnp.concatenate([grad_sgate_rows, grad_sup_rows], axis=1)
    grad_normed_two = dot(grad_gate_up, gate_up_full, 1, 1) + grad_routed
    _, pull_two = jax.vjp(rms_norm, mixed_rows, gain_two)
    grad_mixed_norm, grad_gain_two = pull_two(grad_normed_two)
    grad_mixed = grad_out + grad_mixed_norm
    grad_mixed_low = grad_mixed.astype(BF16)

    grad_attended = dot(grad_mixed_low, output_full, 1, 1).astype(BF16)
    grad_query, grad_key_value = attend_back(
        query_rows, key_value_all, seg_rows, seg_line, log_total, grad_attended, score_scale
    )
    expert_up_own = expert_grad(slot_rows, grad_up_rows, [])
    gain_grads = jnp.pad(grad_gain_two.reshape(devices, 1, -1), ((0, 0), (0, 7), (0, 0)))
    gain_rows = gain_grads.shape[2]
    gain_grads = jnp.pad(gain_grads, ((0, 0), (0, 0), (0, lanes - gain_rows)))
    if gain_rows % 16 == 0:
        sums = sum_dense(
            [normed_two.T, attended.T, shared_hidden.T, normed_one.T],
            [grad_gate_up, grad_mixed_low, grad_low, grad_query],
            gain_grads,
            grad_key_value,
            ((shared_width, shared_width), (query_width, feat_width), (key_width, key_width), (feat_width,), (lanes,)),
            (((0, 0),), ((3, 3), (1, 1)), ((3, None),), ((2, 2),)),
            5,
        )
        gate_up_blocks, query_block, grad_output_block = sums[:2], sums[2], sums[3]
        qkv_blocks = [query_block, sums[4], sums[5]]
        grad_down_block, grad_gain_block = sums[6:8]
        grad_qkv = jnp.concatenate([grad_query, sums[8]], axis=1)
    else:
        grad_key_value = jnp.concatenate([grad_key_value[0], grad_key_value[1]], axis=1)
        total = grad_key_value[:tok_rows]
        for step in range(1, back + 1):
            came = shift(total.astype(BF16), "seq", -1)
            total = came.astype(F32) + grad_key_value[step * tok_rows : (step + 1) * tok_rows]
        grad_qkv = jnp.concatenate([grad_query, total.astype(BF16)], axis=1)
        dense_grads = [
            weight_grad(normed_two, grad_gate_up),
            weight_grad(attended, grad_mixed_low),
            weight_grad(shared_hidden, grad_low),
            weight_grad(normed_one, grad_qkv),
            gain_grads,
        ]
        sums = scatter_dense(dense_grads, 5)
        gate_up_blocks, grad_output_block, grad_down_block, qkv_blocks, grad_gain_block = sums
        gate_up_blocks = jnp.split(gate_up_blocks, [shared_width], axis=1)
        qkv_blocks = jnp.split(qkv_blocks, [query_width, query_width + key_width], axis=1)
    grad_normed_one = dot(grad_qkv, qkv_full, 1, 1)
    _, pull_one = jax.vjp(lambda values: rms_norm(values, gain_one), x_float)
    grad_tokens = grad_mixed + pull_one(grad_normed_one)[0]
    grad_gain_one = sum(
        jnp.sum(weight.astype(F32) * grad, axis=1)
        for weight, grad in zip((query_weight, key_weight, value_weight), qkv_blocks)
    ) / norm1_gain.astype(F32)
    last = [grad_gain_block]
    grad_expert_down = expert_sum(expert_down_own, last)
    grad_expert_gate = expert_sum(expert_gate_own, last)
    grad_expert_up = expert_sum(expert_up_own, last)
    return (
        block_output[None],
        grad_tokens[None],
        grad_gain_one,
        *qkv_blocks,
        grad_output_block,
        grad_gain_block[0, :gain_rows],
        *gate_up_blocks,
        grad_down_block,
        grad_expert_gate,
        grad_expert_up,
        grad_expert_down,
    )


def solution(mesh):
    rows = P("fsdp", "seq", None)
    dense = P(("seq", "fsdp"), None)
    gain = P(("seq", "fsdp"))
    return jax.shard_map(
        block,
        mesh=mesh,
        in_specs=(
            rows, rows, P("fsdp", "seq"), P("fsdp", None), rows, rows,
            gain, dense, dense, dense, dense, gain, dense, dense, dense, rows, rows, rows,
        ),
        out_specs=(
            rows, rows, gain, dense, dense, dense, dense, gain, dense, dense, dense, rows, rows, rows,
        ),
        check_vma=False,
    )
```

```python
import functools
import math

import jax
import jax.numpy as jnp
from jax import lax
from jax.experimental import pallas as pl
from jax.experimental.pallas import tpu as pltpu
from jax.sharding import PartitionSpec as P


HEADS = 12
KV_HEADS = 4
HEAD = 128
TOP = 6
EPSILON = 1e-05
MASKED = -1e30
PAIR = 2


BF16 = jnp.bfloat16
F32 = jnp.float32


def exchange(values, axis, bit):
    count = lax.axis_size(axis)
    return lax.ppermute(values, axis, [(i, i ^ bit) for i in range(count)])


def shift(values, axis, step):
    count = lax.axis_size(axis)
    pairs = [(i, i + step) for i in range(count) if 0 <= i + step < count]
    return lax.ppermute(values, axis, pairs)


def after(values, *others):
    return lax.optimization_barrier((values, *others))[0]


def dot(left, right, left_dim, right_dim):
    return lax.dot_general(
        left, right, (((left_dim,), (right_dim,)), ((), ())), preferred_element_type=F32
    )


def batch_dot(left, right, left_dim, right_dim):
    return lax.dot_general(
        left, right, (((left_dim,), (right_dim,)), ((0,), (0,))), preferred_element_type=F32
    )


def rms_norm(values, gain):
    factor = lax.rsqrt(jnp.mean(values * values, axis=-1, keepdims=True) + EPSILON)
    return values * factor * gain


def swiglu(gate_rows, up_rows):
    return jax.nn.silu(gate_rows) * up_rows


def swiglu_backward(gate_rows, up_rows, grad_rows):
    _, pull_back = jax.vjp(swiglu, gate_rows, up_rows)
    grad_gate, grad_up = pull_back(grad_rows)
    return (grad_gate.astype(BF16), grad_up.astype(BF16))


MESH = pl.DeviceIdType.MESH


def grant(scratch, extra):
    size = extra
    for ref in scratch:
        shape = list(ref.shape)
        shape[-2] = -(-shape[-2] // 16) * 16
        size += math.prod(shape) * jnp.dtype(ref.dtype).itemsize
    return min(size + 6 * 2**20, 66 * 10**6)


class Copies:
    def __init__(self, send_sems, recv_sems):
        self.send_sems, self.recv_sems, self.made = send_sems, recv_sems, []

    def start(self, source, target, axis, partner, when=None):
        number = len(self.made)
        copy = pltpu.make_async_remote_copy(
            src_ref=source,
            dst_ref=target,
            send_sem=self.send_sems.at[number],
            recv_sem=self.recv_sems.at[number],
            device_id={axis: partner},
            device_id_type=MESH,
        )
        if when is None:
            copy.start()
        else:
            pl.when(when)(copy.start)
        self.made.append((copy, when))
        return copy

    def finish(self):
        for copy, when in self.made:
            if when is None:
                copy.wait_send()
            else:
                pl.when(when)(copy.wait_send)


def greet(partners):
    barrier = pltpu.get_barrier_semaphore()
    for axis, partner in partners:
        pl.semaphore_signal(barrier, inc=1, device_id={axis: partner}, device_id_type=MESH)
    pl.semaphore_wait(barrier, len(partners))


def bit_of(index, bit):
    return lax.rem(lax.div(index, bit), 2)


def flip(index, bit):
    return index + bit - 2 * bit * bit_of(index, bit)


def flip_all(index, mask):
    bit = 1
    while bit <= mask:
        if mask & bit:
            index = flip(index, bit)
        bit *= 2
    return index


def gather_dense_kernel(length, bits, count, back, *refs):
    extra = 0 if back is None else 1
    shards, expert = refs[:count], refs[count]
    outs, expert_full = refs[count + 1 + extra : 2 * count + 1 + extra], refs[2 * count + 1 + extra]
    if back is None:
        send_sems, recv_sems, local_sems = refs[2 * count + 2 :]
        places = list(outs)
    else:
        tokens = refs[count + 1]
        normed_ref, query_ref, window_ref, held, send_sems, recv_sems, local_sems = refs[2 * count + 3 :]
        places = [held] + list(outs[1:])
    seq, group = lax.axis_index("seq"), lax.axis_index("fsdp")
    own = [bit_of(group, bit) for bit in bits]
    partners = [("seq", flip_all(seq, k)) for k in range(1, length)]
    partners += [("fsdp", flip(group, bit)) for bit in bits]
    greet(partners)
    copies = Copies(send_sems, recv_sems)
    far = len(bits) - 1
    half = length // 2
    side = lax.div(seq, half)
    low = [side * half, (1 - side) * half]
    orders = [list(range(far)), list(range(far))[::-1]]
    hops = length - 1
    stages = hops + far + 1
    waiting = [[] for _ in range(count)]
    right, left = lax.rem(seq + 1, length), lax.rem(seq + length - 1, length)

    def launch(t, stage):
        if stage < hops:
            back_block = lax.rem(seq - stage + length, length)
            next_block = lax.rem(seq + stage, length)
            if stage == 0:
                local = pltpu.make_async_copy(shards[t], places[t].at[(seq, *own)], local_sems.at[t])
                local.start()
            made = []
            for block, target, sends, comes in (
                (back_block, right, (seq >= stage) & (seq + 1 < length), seq > stage),
                (next_block, left, (seq + stage < length) & (seq >= 1), seq + 1 + stage < length),
            ):
                view = places[t].at[(block, *own)]
                source = shards[t] if stage == 0 else view
                made.append((copies.start(source, view, "seq", target, sends).wait_recv, comes))
            if stage == 0:
                made.append((local.wait, None))
            return made
        made = []
        for part in (0, 1):
            where = [pl.ds(low[part], half)] + list(own)
            for done in orders[part][: stage - hops]:
                where[1 + done] = slice(None)
            dim = orders[part][stage - hops] if stage < hops + far else far
            view = places[t].at[tuple(where)]
            made.append((copies.start(view, view, "fsdp", flip(group, bits[dim])).wait_recv, None))
        return made

    def settle(made):
        for wait, when in made:
            if when is None:
                wait()
            else:
                pl.when(when)(wait)

    def ship_expert():
        held_experts, depth = expert.shape[0] // PAIR, expert.shape[1]
        rows = pl.ds(pl.multiple_of(seq * depth, depth), depth)
        parity = lax.rem(seq, PAIR)
        local = pltpu.make_async_copy(
            expert.at[pl.ds(parity * held_experts, held_experts)], expert_full.at[:, rows], local_sems.at[count]
        )
        local.start()
        made = [(local.wait, None)]
        for k in range(1, length):
            mine = pl.ds(lax.rem(parity + k, PAIR) * held_experts, held_experts)
            copy = copies.start(expert.at[mine], expert_full.at[:, rows], "seq", flip_all(seq, k))
            made.append((copy.wait_recv, None))
        return made

    def project():
        rows, width = normed_ref.shape
        query_width = query_ref.shape[1]
        key_width = window_ref.shape[1]

        def columns(start, size):
            return held[(slice(None),) * (2 + far) + (slice(None), pl.ds(start, size))].reshape(width, size)

        gain = columns(query_width + key_width, 128).astype(jnp.float32).T[0:1]
        values = tokens[...].astype(jnp.float32)
        factor = lax.rsqrt(jnp.mean(values * values, axis=-1, keepdims=True) + EPSILON)
        normed_ref[...] = (values * factor * gain).astype(normed_ref.dtype)
        here = pl.ds(back * rows, rows)
        for start in range(0, key_width, 512):
            tile = jnp.dot(
                normed_ref[...], columns(query_width + start, 512), preferred_element_type=jnp.float32
            )
            window_ref[here, pl.ds(start, 512)] = tile.astype(window_ref.dtype)
        for j in range(1, back + 1):

            @pl.when(seq < j)
            def _(j=j):
                window_ref[pl.ds((back - j) * rows, rows)] = jnp.zeros((rows, key_width), window_ref.dtype)

        first = pass_keys(1)
        for start in range(0, query_width, 512):
            tile = jnp.dot(normed_ref[...], columns(start, 512), preferred_element_type=jnp.float32)
            query_ref[:, pl.ds(start, 512)] = tile.astype(query_ref.dtype)
        kept = pltpu.make_async_copy(held, outs[0], local_sems.at[0])
        kept.start()
        return first, kept

    def pass_keys(j):
        rows = normed_ref.shape[0]
        source = window_ref.at[pl.ds((back - j + 1) * rows, rows)]
        target = window_ref.at[pl.ds((back - j) * rows, rows)]
        sends = (seq >= j - 1) & (seq + 1 < length)
        return [(copies.start(source, target, "seq", right, sends).wait_recv, seq >= j)]

    passing, passed = [], 0
    starts = [(t + 1) // 2 for t in range(count)]
    for step in range(starts[-1] + stages + 1):
        for t in range(count):
            stage = step - starts[t]
            if 0 < stage <= stages:
                settle(waiting[t])
            if 0 <= stage < stages:
                waiting[t] = launch(t, stage)
        if step == starts[-1] + hops - 1:
            expert_waiting = ship_expert()
        if step == stages and back is not None:
            passing, kept = project()
            passed = 1
        elif passing and passed < back and step == stages + 2 * passed:
            settle(passing)
            passed += 1
            passing = pass_keys(passed)
    while passing:
        settle(passing)
        passed += 1
        passing = pass_keys(passed) if passed <= back else []
    settle(expert_waiting)
    copies.finish()
    if back is not None:
        kept.wait()


def gather_dense(shards, expert, tokens, back, key_width):
    length, groups = lax.axis_size("seq"), lax.axis_size("fsdp")
    bits, bit = [], groups // 2
    while bit >= 1:
        bits.append(bit)
        bit //= 2
    count = len(shards)
    number = count * 2 * (length - 1 + len(bits)) + length - 1 + back
    size = sum(s.size * s.dtype.itemsize for s in shards) * length * groups
    experts, depth, wide = expert.shape
    lead = (length,) + (2,) * len(bits)
    rows, width = tokens.shape
    fused = shards[0].shape[0] % 16 == 0
    extra_in, extra_out, extra_scratch = [], [], []
    if fused:
        query_width = shards[0].shape[1] - key_width - 128
        extra_in = [tokens]
        extra_out = [
            jax.ShapeDtypeStruct((rows, width), tokens.dtype),
            jax.ShapeDtypeStruct((rows, query_width), tokens.dtype),
            jax.ShapeDtypeStruct(((back + 1) * rows, key_width), tokens.dtype),
        ]
        extra_scratch = [pltpu.VMEM(lead + shards[0].shape, shards[0].dtype)]
    results = pl.pallas_call(
        functools.partial(gather_dense_kernel, length, bits, count, back if fused else None),
        out_shape=[
            jax.ShapeDtypeStruct((length,) + (2,) * len(bits) + s.shape, s.dtype) for s in shards
        ]
        + [jax.ShapeDtypeStruct((experts // PAIR, length * depth, wide), expert.dtype)]
        + extra_out,
        in_specs=[pl.BlockSpec(memory_space=pltpu.VMEM)] * count
        + [pl.BlockSpec(memory_space=pl.ANY)]
        + [pl.BlockSpec(memory_space=pltpu.VMEM)] * len(extra_in),
        out_specs=[pl.BlockSpec(memory_space=pl.ANY)] * (count + 1)
        + [pl.BlockSpec(memory_space=pltpu.VMEM)] * len(extra_out),
        scratch_shapes=extra_scratch
        + [
            pltpu.SemaphoreType.DMA((number,)),
            pltpu.SemaphoreType.DMA((number,)),
            pltpu.SemaphoreType.DMA((count + 1,)),
        ],
        compiler_params=pltpu.CompilerParams(
            collective_id=0, has_side_effects=True, vmem_limit_bytes=60 * 2**20
        ),
        cost_estimate=pl.CostEstimate(flops=0, bytes_accessed=3 * size, transcendentals=0),
        name="gather_dense",
    )(*shards, expert, *extra_in)
    outs = [out.reshape(-1, out.shape[-1]) for out in results[:count]] + [results[count]]
    return outs + (list(results[count + 1 :]) if fused else [None] * 3)


def scatter_dense_kernel(length, bits, count, *refs):
    grads, outs = refs[:count], refs[count : 2 * count]
    far = len(bits) - 1
    per = 3 + far
    scratch = refs[2 * count : 2 * count + per * count]
    send_sems, recv_sems, local_sems = refs[2 * count + per * count :]
    seq, group = lax.axis_index("seq"), lax.axis_index("fsdp")
    own = [bit_of(group, bit) for bit in bits]
    partners = [("seq", flip_all(seq, k)) for k in range(1, length)]
    partners += [("fsdp", flip(group, bit)) for bit in bits]
    greet(partners)
    copies = Copies(send_sems, recv_sems)
    half = length // 2
    side = lax.div(seq, half)
    low = [side * half, (1 - side) * half]
    orders = [list(range(far))[::-1], list(range(far))]
    stages = far + 2
    everything = (slice(None),) * (1 + far)

    def buffers(t):
        held = scratch[per * t : per * (t + 1)]
        return held[0], held[1], held[2 : 2 + far], held[2 + far]

    waiting = [None] * count

    def add(mine, came, lead, fixed, inner_of):
        start, size = lead
        left = [d for d in range(far) if d not in fixed]

        def body(i, carry):
            z = lax.div(i, 2 ** len(left))
            where, inner = [own[d] for d in range(far)], []
            for k, d in enumerate(left):
                where[d] = lax.rem(lax.div(i, 2 ** (len(left) - 1 - k)), 2)
                inner.append(where[d])
            place = (start + z, *where)
            total = mine[place].astype(jnp.float32) + came[inner_of(start + z, z, inner)].astype(jnp.float32)
            mine[place] = total.astype(mine.dtype)
            return carry

        lax.fori_loop(0, size * 2 ** len(left), body, 0)

    def launch(t, stage):
        mine, came_core, came_far, came_seq = buffers(t)
        if stage == 0:
            local = pltpu.make_async_copy(grads[t].at[(*everything, own[far])], mine, local_sems.at[t])
            local.start()
            sent = grads[t].at[(*everything, 1 - own[far])]
            return [copies.start(sent, came_core, "fsdp", flip(group, bits[far]))], local
        if stage <= far:
            made = []
            for part in (0, 1):
                order = orders[part]
                if stage == 1:
                    add(mine, came_core, (low[part], half), [], lambda z, at, inner: (z, *inner))
                else:
                    came = came_far[stage - 2].at[part]
                    add(mine, came, (low[part], half), order[: stage - 1], lambda z, at, inner: (at, *inner))
                dim = order[stage - 1]
                where = [slice(None)] * far
                for d in order[: stage - 1]:
                    where[d] = own[d]
                where[dim] = 1 - own[dim]
                made.append(
                    copies.start(
                        mine.at[(pl.ds(low[part], half), *where)],
                        came_far[stage - 1].at[part],
                        "fsdp",
                        flip(group, bits[dim]),
                    )
                )
            return made, None
        for part in (0, 1):
            came = came_far[far - 1].at[part]
            add(mine, came, (low[part], half), orders[part], lambda z, at, inner: (at,))
        made = []
        for k in range(1, length):
            other = flip_all(seq, k)
            made.append(copies.start(mine.at[(other, *own[:far])], came_seq.at[k - 1], "seq", other))
        return made, None

    def close(t):
        mine, _, _, came_seq = buffers(t)
        total = mine[(seq, *own[:far])].astype(jnp.float32)
        for k in range(1, length):
            total = total + came_seq[k - 1].astype(jnp.float32)
        outs[t][...] = total

    for step in range(count + stages):
        for t in range(count):
            stage = step - t
            if 0 < stage <= stages:
                made, local = waiting[t]
                for copy in made:
                    copy.wait_recv()
                if local is not None:
                    local.wait()
            if 0 <= stage < stages:
                waiting[t] = launch(t, stage)
            elif stage == stages:
                close(t)
    copies.finish()


def scatter_dense(grads, collective_id):
    length, groups = lax.axis_size("seq"), lax.axis_size("fsdp")
    bits, bit = [], groups // 2
    while bit >= 1:
        bits.append(bit)
        bit //= 2
    far = len(bits) - 1
    count = len(grads)
    number = count * (1 + 2 * far + length - 1)
    size = sum(g.size * g.dtype.itemsize for g in grads)
    scratch = []
    for g in grads:
        block = g.shape[1:]
        scratch += [pltpu.VMEM((length,) + (2,) * far + block, g.dtype)] * 2
        scratch += [
            pltpu.VMEM((2, length // 2) + (2,) * (far - 1 - s) + block, g.dtype) for s in range(far)
        ]
        scratch.append(pltpu.VMEM((length - 1,) + block, g.dtype))
    return pl.pallas_call(
        functools.partial(scatter_dense_kernel, length, bits, count),
        out_shape=[jax.ShapeDtypeStruct(g.shape[1:], jnp.float32) for g in grads],
        in_specs=[pl.BlockSpec(memory_space=pl.ANY)] * count,
        out_specs=[pl.BlockSpec(memory_space=pltpu.VMEM)] * count,
        scratch_shapes=scratch
        + [
            pltpu.SemaphoreType.DMA((number,)),
            pltpu.SemaphoreType.DMA((number,)),
            pltpu.SemaphoreType.DMA((count,)),
        ],
        compiler_params=pltpu.CompilerParams(
            collective_id=collective_id, has_side_effects=True, vmem_limit_bytes=grant(scratch, 0)
        ),
        cost_estimate=pl.CostEstimate(flops=0, bytes_accessed=3 * size, transcendentals=0),
        name="scatter_dense",
    )(*[g.reshape((length,) + (2,) * len(bits) + g.shape[1:]) for g in grads])


def sum_dense_kernel(length, bits, cuts, plan, keys_at, back, *refs):
    count = len(cuts)
    weights = count - 1
    act_count = 1 + max(a for group in plan for a, _ in group)
    grad_count = 1 + max(g for group in plan for _, g in group if g is not None)
    acts, grads = refs[:act_count], refs[act_count : act_count + grad_count]
    ready, window, *refs = refs[act_count + grad_count :]
    number = sum(len(cut) for cut in cuts)
    flat_outs, keys_out, refs = list(refs[:number]), refs[number], refs[number + 1 :]
    outs = [[flat_outs.pop(0) for _ in cut] for cut in cuts]
    far = len(bits) - 1
    per = 3 + far
    scratch = refs[: per * count]
    keys_sum, keys_sent, keys_came, send_sems, recv_sems = refs[per * count :]
    seq, group = lax.axis_index("seq"), lax.axis_index("fsdp")
    own = [bit_of(group, bit) for bit in bits]
    partners = [("seq", flip_all(seq, k)) for k in range(1, length)]
    partners += [("fsdp", flip(group, bit)) for bit in bits]
    greet(partners)
    copies = Copies(send_sems, recv_sems)
    half = length // 2
    side = lax.div(seq, half)
    low = [side * half, (1 - side) * half]
    orders = [list(range(far))[::-1], list(range(far))]
    stages = far + 2
    everything = (slice(None),) * (1 + far)
    rows, key_width = keys_sum.shape[0], window.shape[2]
    left = lax.rem(seq + length - 1, length)

    def buffers(t):
        held = scratch[per * t : per * (t + 1)]
        return held[0], held[1], held[2 : 2 + far], held[2 + far]

    def key_piece(b, part):
        return window[part, pl.ds(b * rows, rows)]

    def send_keys(j):
        copy = copies.start(keys_sent.at[j], keys_came.at[j], "seq", left, seq >= 1)
        return copy

    def advance_keys(j, copy):
        for part in (0, 1):
            keys_sum[:, pl.ds(part * key_width, key_width)] = key_piece(j, part)

        @pl.when(seq + 1 < length)
        def _():
            copy.wait_recv()
            keys_sum[...] = keys_sum[...] + keys_came[j - 1].astype(jnp.float32)

        if j < back:
            keys_sent[j] = keys_sum[...].astype(keys_sent.dtype)
            return send_keys(j)
        keys_out[...] = keys_sum[...].astype(keys_out.dtype)
        return None

    def produce(t):
        held = buffers(t)[0]
        if t == weights:
            held[...] = ready[...]
            return
        block = held.shape[-2]

        def body(z, carry):
            start = 0
            for a, g in plan[t]:
                depth = acts[a].shape[0] // length
                left_rows = acts[a][pl.ds(pl.multiple_of(z * depth, depth), depth)]
                source = keys_out if g is None else grads[g]
                for c in range(0, source.shape[1], 512):
                    tile = jnp.dot(left_rows, source[:, c : c + 512], preferred_element_type=jnp.float32)
                    tile = tile.astype(held.dtype).reshape((2,) * (far + 1) + (block, 512))
                    held[(z, *(slice(None),) * (far + 2), pl.ds(start, 512))] = tile
                    start += 512
            return carry

        lax.fori_loop(0, length, body, 0)

    def add(held, came, lead, fixed, inner_of):
        start, size = lead
        free = [d for d in range(far) if d not in fixed]

        def body(i, carry):
            z = lax.div(i, 2 ** len(free))
            where, inner = [own[d] for d in range(far)], []
            for k, d in enumerate(free):
                where[d] = lax.rem(lax.div(i, 2 ** (len(free) - 1 - k)), 2)
                inner.append(where[d])
            place = (start + z, *where, own[far])
            total = held[place].astype(jnp.float32) + came[inner_of(start + z, z, inner)].astype(jnp.float32)
            held[place] = total.astype(held.dtype)
            return carry

        lax.fori_loop(0, size * 2 ** len(free), body, 0)

    def launch(t, stage):
        held, came_core, came_far, came_seq = buffers(t)
        if stage == 0:
            produce(t)
            return [copies.start(held.at[(*everything, 1 - own[far])], came_core, "fsdp", flip(group, bits[far]))]
        made = []
        if stage <= far:
            for part in (0, 1):
                order = orders[part]
                if stage == 1:
                    add(held, came_core, (low[part], half), [], lambda z, at, inner: (z, *inner))
                else:
                    came = came_far[stage - 2].at[part]
                    add(held, came, (low[part], half), order[: stage - 1], lambda z, at, inner: (at, *inner))
                dim = order[stage - 1]
                where = [slice(None)] * far
                for d in order[: stage - 1]:
                    where[d] = own[d]
                where[dim] = 1 - own[dim]
                source = held.at[(pl.ds(low[part], half), *where, own[far])]
                made.append(
                    copies.start(source, came_far[stage - 1].at[part], "fsdp", flip(group, bits[dim]))
                )
            return made
        for part in (0, 1):
            add(held, came_far[far - 1].at[part], (low[part], half), orders[part], lambda z, at, inner: (at,))
        for k in range(1, length):
            other = flip_all(seq, k)
            made.append(copies.start(held.at[(other, *own)], came_seq.at[k - 1], "seq", other))
        return made

    def close(t):
        held, _, _, came_seq = buffers(t)
        total = held[(seq, *own)].astype(jnp.float32)
        for k in range(1, length):
            total = total + came_seq[k - 1].astype(jnp.float32)
        start = 0
        for out, size in zip(outs[t], cuts[t]):
            out[...] = total[:, start : start + size]
            start += size

    for part in (0, 1):
        keys_sent[0, :, pl.ds(part * key_width, key_width)] = key_piece(0, part).astype(keys_sent.dtype)
    flying = send_keys(0)
    waiting = [[] for _ in range(count)]
    starts = [min(t, count - 2) for t in range(count)]
    for step in range(starts[-1] + stages):
        for t in range(count):
            stage = step - starts[t]
            if 0 < stage < stages:
                for copy in waiting[t]:
                    copy.wait_recv()
            if stage == 0 and t == keys_at:
                advance_keys(back, flying)
            if 0 <= stage < stages:
                waiting[t] = launch(t, stage)
        hop = step - starts[keys_at] + back
        if 1 <= hop < back:
            flying = advance_keys(hop, flying)
    for t in range(count):
        for copy in waiting[t]:
            copy.wait_recv()
        close(t)
    copies.finish()


def sum_dense(acts, grads, ready, window, cuts, plan, collective_id):
    length, groups = lax.axis_size("seq"), lax.axis_size("fsdp")
    bits, bit = [], groups // 2
    while bit >= 1:
        bits.append(bit)
        bit //= 2
    far = len(bits) - 1
    devices = length * groups
    rows = grads[0].shape[0]
    back = window.shape[1] // rows - 1
    key_width = 2 * window.shape[2]
    blocks = [
        ((acts[group[0][0]].shape[0] // devices, sum(cut)), grads[0].dtype) for group, cut in zip(plan, cuts)
    ]
    keys_at = [any(g is None for _, g in group) for group in plan].index(True)
    blocks.append((ready.shape[1:], ready.dtype))
    count = len(blocks)
    number = count * (1 + 2 * far + length - 1) + back
    scratch = []
    for block, dtype in blocks:
        scratch.append(pltpu.VMEM((length,) + (2,) * (far + 1) + block, dtype))
        scratch.append(pltpu.VMEM((length,) + (2,) * far + block, dtype))
        scratch += [pltpu.VMEM((2, length // 2) + (2,) * (far - 1 - s) + block, dtype) for s in range(far)]
        scratch.append(pltpu.VMEM((length - 1,) + block, dtype))
    scratch.append(pltpu.VMEM((rows, key_width), jnp.float32))
    scratch += [pltpu.VMEM((back, rows, key_width), grads[0].dtype)] * 2
    elements = sum(math.prod(block) for block, _ in blocks) * devices
    return pl.pallas_call(
        functools.partial(sum_dense_kernel, length, bits, cuts, plan, keys_at, back),
        out_shape=[
            jax.ShapeDtypeStruct((block[0], size), jnp.float32)
            for (block, _), cut in zip(blocks, cuts)
            for size in cut
        ]
        + [jax.ShapeDtypeStruct((rows, key_width), grads[0].dtype)],
        in_specs=[pl.BlockSpec(memory_space=pltpu.VMEM)] * (len(acts) + len(grads) + 2),
        out_specs=[pl.BlockSpec(memory_space=pltpu.VMEM)] * (sum(len(cut) for cut in cuts) + 1),
        scratch_shapes=scratch + [pltpu.SemaphoreType.DMA((number,))] * 2,
        compiler_params=pltpu.CompilerParams(
            collective_id=collective_id, has_side_effects=True, vmem_limit_bytes=67 * 10**6
        ),
        cost_estimate=pl.CostEstimate(
            flops=2 * elements * rows, bytes_accessed=4 * elements, transcendentals=0
        ),
        name="sum_dense",
    )(*acts, *grads, ready.reshape((length,) + (2,) * len(bits) + ready.shape[1:]), window)


def row_dims():
    groups = lax.axis_size("fsdp")
    dims, bit = [("seq", 1)], groups // 2
    while bit >= 1:
        dims.append(("fsdp", bit))
        bit //= 2
    return dims


def row_places(dims):
    seq, group = lax.axis_index("seq"), lax.axis_index("fsdp")
    index = {"seq": seq, "fsdp": group}
    own = [bit_of(index[axis], bit) for axis, bit in dims]
    partner = [(axis, flip(index[axis], bit)) for axis, bit in dims]
    return own, partner


def row_orders(far, light):
    if light:
        return [[0] + [1 + (i + k) % (far - 1) for k in range(far - 1)] for i in range(far - 1)]
    return [[(i + k) % far for k in range(far)] for i in range(far)]


def gather_rows_kernel(dims, orders, held, rows_ref, pick_ref, slots_ref, buffer, send_sems, recv_sems, local_sem):
    own, partner = row_places(dims)
    greet(partner)
    copies = Copies(send_sems, recv_sems)
    far = len(dims) - 1
    pieces = len(orders)
    width = rows_ref.shape[1] // pieces
    capacity = slots_ref.shape[-2]

    def view(piece, done):
        where = list(own)
        for d in done:
            where[d] = slice(None)
        return buffer.at[(piece, *where)]

    flying, local = [], []
    for piece in range(pieces):
        cut = rows_ref.at[:, pl.ds(piece * width, width)]
        flying.append(copies.start(cut, view(piece, []), *partner[orders[piece][0]]))
        local.append(pltpu.make_async_copy(cut, view(piece, []), local_sem.at[piece]))
        local[piece].start()
    for copy in local:
        copy.wait()

    def pick_block(piece, where):
        taken = jnp.dot(
            pick_ref[tuple(where)], buffer[(piece, *where)], preferred_element_type=jnp.float32
        ).astype(slots_ref.dtype)
        for e in range(held):
            slots_ref[(e, *where, slice(None), pl.ds(piece * width, width))] = taken[
                e * capacity : (e + 1) * capacity
            ]

    def pick_all(piece, core):
        def body(i, carry):
            where, rest = [], i
            for d in range(far):
                where.append(lax.rem(lax.div(rest, 2 ** (far - 1 - d)), 2))
            pick_block(piece, where + [core])
            return carry

        lax.fori_loop(0, 2**far, body, 0)

    for stage in range(1, far + 1):
        for piece in range(pieces):
            flying[piece].wait_recv()
            order = orders[piece]
            done = order[:stage]
            ref = view(piece, done)
            flying[piece] = copies.start(ref, ref, *(partner[order[stage]] if stage < far else partner[far]))
    for piece in range(pieces):
        pick_all(piece, own[far])
    for piece in range(pieces):
        flying[piece].wait_recv()
        pick_all(piece, 1 - own[far])
    copies.finish()


def gather_rows(rows, pick_low, held, collective_id, light):
    dims = row_dims()
    far = len(dims) - 1
    orders = row_orders(far, light)
    count, feat = rows.shape
    width = feat // len(orders)
    sources = 2 ** len(dims)
    capacity = pick_low.shape[1] // held
    lead = (2,) * len(dims)
    number = len(orders) * (far + 1)
    scratch = [pltpu.VMEM((len(orders),) + lead + (count, width), rows.dtype)]
    slots = pl.pallas_call(
        functools.partial(gather_rows_kernel, dims, orders, held),
        out_shape=jax.ShapeDtypeStruct((held,) + lead + (capacity, feat), rows.dtype),
        in_specs=[pl.BlockSpec(memory_space=pltpu.VMEM)] * 2,
        out_specs=pl.BlockSpec(memory_space=pltpu.VMEM),
        scratch_shapes=scratch
        + [pltpu.SemaphoreType.DMA((n,)) for n in (number, number, len(orders))],
        compiler_params=pltpu.CompilerParams(
            collective_id=collective_id,
            has_side_effects=True,
            vmem_limit_bytes=grant(scratch, 12 * 2**20),
        ),
        cost_estimate=pl.CostEstimate(
            flops=2 * sources * pick_low.shape[1] * count * feat,
            bytes_accessed=6 * sources * count * feat,
            transcendentals=0,
        ),
        name="gather_rows",
    )(rows, pick_low.reshape(lead + pick_low.shape[1:]))
    return slots.reshape(held, sources * capacity, feat)


def scatter_rows_kernel(
    dims, orders, held, slots_ref, pick_ref, out_ref, mine, other, came_core, came_far, send_sems, recv_sems
):
    own, partner = row_places(dims)
    greet(partner)
    copies = Copies(send_sems, recv_sems)
    far = len(dims) - 1
    pieces = len(orders)
    width = out_ref.shape[1] // pieces
    capacity = slots_ref.shape[-2]
    count = out_ref.shape[0]

    def spread(piece, core, target):
        def body(i, carry):
            where = [lax.rem(lax.div(i, 2 ** (far - 1 - d)), 2) for d in range(far)]
            total = jnp.zeros((count, width), jnp.float32)
            for e in range(held):
                rows = slots_ref[(e, *where, core, slice(None), pl.ds(piece * width, width))]
                chosen = pick_ref[(*where, core, pl.ds(e * capacity, capacity))]
                total = total + lax.dot_general(
                    chosen, rows, (((0,), (0,)), ((), ())), preferred_element_type=jnp.float32
                )
            target[(piece, *where)] = total.astype(target.dtype)
            return carry

        lax.fori_loop(0, 2**far, body, 0)

    flying = []
    for piece in range(pieces):
        spread(piece, 1 - own[far], other)
        flying.append(copies.start(other.at[piece], came_core.at[piece], *partner[far]))
    for piece in range(pieces):
        spread(piece, own[far], mine)

    def add_into(piece, fixed, came_view):
        left = [d for d in range(far) if d not in fixed]

        def body(i, carry):
            where, inner = [None] * far, []
            for k, d in enumerate(left):
                where[d] = lax.rem(lax.div(i, 2 ** (len(left) - 1 - k)), 2)
                inner.append(where[d])
            for d in fixed:
                where[d] = own[d]
            total = mine[(piece, *where)].astype(jnp.float32) + came_view[tuple(inner)].astype(jnp.float32)
            mine[(piece, *where)] = total.astype(mine.dtype)
            return carry

        lax.fori_loop(0, 2 ** len(left), body, 0)

    for stage in range(far):
        for piece in range(pieces):
            order = orders[piece][::-1]
            fixed = order[:stage]
            flying[piece].wait_recv()
            add_into(piece, fixed, came_core.at[piece] if stage == 0 else came_far[stage - 1].at[piece])
            dim = order[stage]
            where = [slice(None)] * far
            for d in fixed:
                where[d] = own[d]
            where[dim] = 1 - own[dim]
            flying[piece] = copies.start(
                mine.at[(piece, *where)], came_far[stage].at[piece], *partner[dim]
            )
    for piece in range(pieces):
        flying[piece].wait_recv()
        out_ref[:, pl.ds(piece * width, width)] = mine[(piece, *own[:far])].astype(jnp.float32) + came_far[far - 1][piece].astype(
            jnp.float32
        )
    copies.finish()


def scatter_rows(slots, pick_low, held, collective_id, light):
    dims = row_dims()
    far = len(dims) - 1
    orders = row_orders(far, light)
    count, feat = pick_low.shape[2], slots.shape[2]
    width = feat // len(orders)
    sources = 2 ** len(dims)
    capacity = pick_low.shape[1] // held
    lead = (2,) * len(dims)
    number = len(orders) * (far + 1)

    scratch = [pltpu.VMEM((len(orders),) + (2,) * far + (count, width), slots.dtype)] * 3
    scratch += [pltpu.VMEM((len(orders),) + (2,) * (far - 1 - s) + (count, width), slots.dtype) for s in range(far)]

    def kernel(slots_ref, pick_ref, out_ref, mine, other, came_core, *rest):
        came_far, sems = rest[:far], rest[far:]
        scatter_rows_kernel(
            dims, orders, held, slots_ref, pick_ref, out_ref, mine, other, came_core, came_far, *sems
        )

    return pl.pallas_call(
        kernel,
        out_shape=jax.ShapeDtypeStruct((count, feat), jnp.float32),
        in_specs=[pl.BlockSpec(memory_space=pltpu.VMEM)] * 2,
        out_specs=pl.BlockSpec(memory_space=pltpu.VMEM),
        scratch_shapes=scratch + [pltpu.SemaphoreType.DMA((number,)), pltpu.SemaphoreType.DMA((number,))],
        compiler_params=pltpu.CompilerParams(
            collective_id=collective_id,
            has_side_effects=True,
            vmem_limit_bytes=grant(scratch, 4 * 2**20),
        ),
        cost_estimate=pl.CostEstimate(
            flops=2 * sources * pick_low.shape[1] * count * feat,
            bytes_accessed=6 * sources * count * feat,
            transcendentals=0,
        ),
        name="scatter_rows",
    )(slots.reshape((held,) + lead + (capacity, feat)), pick_low.reshape(lead + pick_low.shape[1:]))


def allowed_keys(seg_rows_ref, seg_keys_ref, back_rows):
    shape = (seg_rows_ref.shape[0], seg_keys_ref.shape[1])
    row = lax.broadcasted_iota(jnp.int32, shape, 0) + back_rows
    key = lax.broadcasted_iota(jnp.int32, shape, 1)
    return (key <= row) & (seg_rows_ref[...] == seg_keys_ref[...])


def attend_kernel(scale, back_rows, query, key, value, seg_rows, seg_keys, out, log_total):
    allowed = allowed_keys(seg_rows, seg_keys, back_rows)
    keys, values = key[...], value[...]
    lane = lax.broadcasted_iota(jnp.int32, (query.shape[0], 128), 1)
    logs = jnp.zeros((query.shape[0], 128), jnp.float32)
    for j in range(query.shape[1] // HEAD):
        columns = slice(j * HEAD, (j + 1) * HEAD)
        scores = lax.dot_general(
            query[:, columns], keys, (((1,), (1,)), ((), ())), preferred_element_type=jnp.float32
        )
        scores = jnp.where(allowed, scores * scale, MASKED)
        top = jnp.max(scores, axis=1, keepdims=True)
        weights = jnp.exp(scores - top)
        total = jnp.sum(weights, axis=1, keepdims=True)
        prob = (weights * (1.0 / total)).astype(jnp.bfloat16)
        out[:, columns] = jnp.dot(prob, values, preferred_element_type=jnp.float32).astype(out.dtype)
        logs = jnp.where(lane == j, top + jnp.log(total), logs)
    log_total[...] = logs


def attend_back_kernel(
    scale, back_rows, query, key, value, seg_rows, seg_keys, log_total, grad, grad_query, grad_key_value
):
    allowed = allowed_keys(seg_rows, seg_keys, back_rows)
    keys, values = key[...], value[...]
    grad_keys = jnp.zeros(keys.shape, jnp.float32)
    grad_values = jnp.zeros(values.shape, jnp.float32)
    for j in range(query.shape[1] // HEAD):
        columns = slice(j * HEAD, (j + 1) * HEAD)
        rows, grad_rows = query[:, columns], grad[:, columns]
        scores = lax.dot_general(
            rows, keys, (((1,), (1,)), ((), ())), preferred_element_type=jnp.float32
        )
        scores = jnp.where(allowed, scores * scale, MASKED)
        prob = jnp.exp(scores - log_total[:, j : j + 1])
        grad_prob = lax.dot_general(
            grad_rows, values, (((1,), (1,)), ((), ())), preferred_element_type=jnp.float32
        )
        delta = jnp.sum(prob * grad_prob, axis=1, keepdims=True)
        grad_scores = (prob * (grad_prob - delta)).astype(jnp.bfloat16)
        grad_query[:, columns] = (
            jnp.dot(grad_scores, keys, preferred_element_type=jnp.float32) * scale
        ).astype(grad_query.dtype)
        grad_keys = grad_keys + lax.dot_general(
            grad_scores, rows, (((0,), (0,)), ((), ())), preferred_element_type=jnp.float32
        )
        grad_values = grad_values + lax.dot_general(
            prob.astype(jnp.bfloat16), grad_rows, (((0,), (0,)), ((), ())), preferred_element_type=jnp.float32
        )
    grad_key_value[0] = grad_keys * scale
    grad_key_value[1] = grad_values


def attend_specs(tok_rows, window, group_width):
    return [
        pl.BlockSpec((tok_rows, group_width), lambda g: (0, g)),
        pl.BlockSpec((window, HEAD), lambda g: (0, g)),
        pl.BlockSpec((window, HEAD), lambda g: (0, KV_HEADS + g)),
        pl.BlockSpec((tok_rows, 1), lambda g: (0, 0)),
        pl.BlockSpec((1, window), lambda g: (0, 0)),
    ]


def attend(query, key_value, seg_rows, seg_keys, scale):
    tok_rows, window = query.shape[0], key_value.shape[0]
    group_width = query.shape[1] // KV_HEADS
    return pl.pallas_call(
        functools.partial(attend_kernel, scale, window - tok_rows),
        grid=(KV_HEADS,),
        in_specs=attend_specs(tok_rows, window, group_width),
        out_specs=[
            pl.BlockSpec((tok_rows, group_width), lambda g: (0, g)),
            pl.BlockSpec((None, tok_rows, 128), lambda g: (g, 0, 0)),
        ],
        out_shape=[
            jax.ShapeDtypeStruct(query.shape, query.dtype),
            jax.ShapeDtypeStruct((KV_HEADS, tok_rows, 128), jnp.float32),
        ],
        compiler_params=pltpu.CompilerParams(vmem_limit_bytes=32 * 2**20),
        cost_estimate=pl.CostEstimate(
            flops=4 * HEADS * tok_rows * window * HEAD,
            bytes_accessed=8 * query.size,
            transcendentals=HEADS * tok_rows * window,
        ),
        name="attend",
    )(query, key_value, key_value, seg_rows, seg_keys)


def attend_back(query, key_value, seg_rows, seg_keys, log_total, grad, scale):
    tok_rows, window = query.shape[0], key_value.shape[0]
    group_width = query.shape[1] // KV_HEADS
    return pl.pallas_call(
        functools.partial(attend_back_kernel, scale, window - tok_rows),
        grid=(KV_HEADS,),
        in_specs=attend_specs(tok_rows, window, group_width)
        + [
            pl.BlockSpec((None, tok_rows, 128), lambda g: (g, 0, 0)),
            pl.BlockSpec((tok_rows, group_width), lambda g: (0, g)),
        ],
        out_specs=[
            pl.BlockSpec((tok_rows, group_width), lambda g: (0, g)),
            pl.BlockSpec((2, window, HEAD), lambda g: (0, 0, g)),
        ],
        out_shape=[
            jax.ShapeDtypeStruct(query.shape, query.dtype),
            jax.ShapeDtypeStruct((2, window, KV_HEADS * HEAD), jnp.float32),
        ],
        compiler_params=pltpu.CompilerParams(vmem_limit_bytes=32 * 2**20),
        cost_estimate=pl.CostEstimate(
            flops=10 * HEADS * tok_rows * window * HEAD,
            bytes_accessed=16 * query.size,
            transcendentals=HEADS * tok_rows * window,
        ),
        name="attend_back",
    )(query, key_value, key_value, seg_rows, seg_keys, log_total, grad)


def block(
    tokens,
    teacher,
    valid_mask,
    segment_ids,
    routes,
    gate_weights,
    norm1_gain,
    query_weight,
    key_weight,
    value_weight,
    output_weight,
    norm2_gain,
    shared_gate_weight,
    shared_up_weight,
    shared_down_weight,
    expert_gate_weight,
    expert_up_weight,
    expert_down_weight,
):
    length, groups = lax.axis_size("seq"), lax.axis_size("fsdp")
    seq_index, group_index = lax.axis_index("seq"), lax.axis_index("fsdp")
    devices = length * groups
    tok_rows, feat_width = tokens.shape[1], tokens.shape[2]
    seq_len = segment_ids.shape[1]
    score_scale = 1.0 / math.sqrt(HEAD)
    key_width = KV_HEADS * HEAD
    query_width = HEADS * HEAD
    shared_width = shared_gate_weight.shape[1]

    lanes = 128
    gains = jnp.pad(jnp.stack([norm1_gain, norm2_gain], axis=1), ((0, 0), (0, lanes - 2)))
    meta = jnp.concatenate([routes[0].T.astype(F32), gate_weights[0].T], axis=0)
    meta = jnp.pad(meta, ((0, 16 - 2 * TOP), (0, 0)))
    longest = seq_len // 2
    back = min(length - 1, -(-(longest - 1) // tok_rows))
    gathered = gather_dense(
        [
            jnp.concatenate([query_weight, key_weight, value_weight, gains], axis=1),
            output_weight,
            jnp.concatenate([shared_gate_weight, shared_up_weight], axis=1),
            shared_down_weight,
            meta,
        ],
        expert_gate_weight,
        tokens[0],
        back,
        2 * key_width,
    )
    qkv_full, output_full, gate_up_full, down_full, meta, expert_gate_full = gathered[:6]
    normed_one, query_rows, key_value_all = gathered[6:]

    def weight_grad(rows, grad_rows):
        grad = dot(rows, grad_rows, 0, 0).astype(BF16)
        return grad.reshape(devices, -1, grad.shape[1])

    qkv_width = query_width + 2 * key_width
    gain_plain = qkv_full[:, qkv_width : qkv_width + 2].T.astype(F32)
    qkv_full = qkv_full[:, :qkv_width]
    gain_one, gain_two = gain_plain[0], gain_plain[1]

    num_local = expert_gate_weight.shape[0]
    num_held = num_local // PAIR
    side = seq_index % PAIR

    def share(weight, k):
        return lax.dynamic_slice_in_dim(weight, (side ^ (k % PAIR)) * num_held, num_held, axis=0)

    def collect_start(weight, wait):
        sent = after(weight, *wait)
        return [exchange(share(sent, k), "seq", k) for k in range(1, length)]

    def collect_done(weight, came):
        part = weight.shape[1]
        full = jnp.zeros((num_held, length * part, weight.shape[2]), weight.dtype)
        for k, block in enumerate([share(weight, 0)] + came):
            full = lax.dynamic_update_slice(full, block, (0, (seq_index ^ k) * part, 0))
        return full

    x_float = tokens[0].astype(F32)
    if normed_one is None:
        normed_one = rms_norm(x_float, gain_one).astype(BF16)
        qkv_rows = dot(normed_one, qkv_full, 1, 0).astype(BF16)
        query_rows = qkv_rows[:, :query_width]
        key_value = [qkv_rows[:, query_width:]]
        for _ in range(back):
            key_value.insert(0, shift(key_value[0], "seq", 1))
        key_value_all = jnp.concatenate(key_value, axis=0)
    up_came = collect_start(expert_up_weight, [key_value_all])
    window = (back + 1) * tok_rows
    seg_padded = jnp.concatenate([jnp.full((back * tok_rows,), -1, jnp.int32), segment_ids[0]])
    seg_keys = lax.dynamic_slice_in_dim(seg_padded, seq_index * tok_rows, window)
    seg_here = seg_keys[back * tok_rows :]
    seg_rows, seg_line = seg_here[:, None], seg_keys[None, :]
    attended, log_total = attend(query_rows, key_value_all, seg_rows, seg_line, score_scale)
    mixed_rows = x_float + dot(attended, output_full, 1, 0)
    normed_two = rms_norm(mixed_rows, gain_two).astype(BF16)

    experts_all = num_local * groups
    capacity = tok_rows * TOP * 4 // (3 * experts_all)
    meta = lax.dynamic_slice_in_dim(
        meta.reshape(length, groups, 16, tok_rows), seq_index // PAIR * PAIR, PAIR, axis=0
    ).reshape(PAIR * groups, 16, tok_rows)
    route_all, gate_all = meta[:, :TOP], meta[:, TOP : 2 * TOP]
    held_ids = group_index * num_local + side * num_held + jnp.arange(num_held, dtype=jnp.int32)
    named = route_all[:, None] == held_ids.astype(F32)[None, :, None, None]
    has = jnp.any(named, axis=2)
    gate_of = jnp.sum(jnp.where(named, gate_all[:, None], 0.0), axis=2)
    token_order = jnp.arange(tok_rows, dtype=jnp.int32)
    earlier = (token_order[:, None] < token_order[None, :]).astype(BF16)
    before = lax.dot_general(
        has.astype(BF16), earlier, (((2,), (0,)), ((), ())), preferred_element_type=F32
    )
    slot_number = jnp.arange(capacity, dtype=F32)
    chosen = has[:, :, None] & (before[:, :, None] == slot_number[None, None, :, None])
    gate_slots = jnp.sum(jnp.where(chosen, gate_of[:, :, None], 0.0), axis=3)
    sources = PAIR * groups
    chosen_low = chosen.astype(BF16).reshape(sources, num_held * capacity, tok_rows)
    gate_canonical = jnp.moveaxis(gate_slots, 0, 1).reshape(num_held, sources * capacity, 1)
    down_came = collect_start(expert_down_weight, [normed_two])
    slot_rows = gather_rows(normed_two, chosen_low, num_held, 1, False)

    gate_up = dot(normed_two, gate_up_full, 1, 0)
    shared_gate, shared_up = gate_up[:, :shared_width], gate_up[:, shared_width:]
    shared_hidden = swiglu(shared_gate, shared_up).astype(BF16)
    shared_out = dot(shared_hidden, down_full, 1, 0)
    expert_gate_rows = batch_dot(slot_rows, expert_gate_full, 2, 1)
    up_came = [after(came, shared_out) for came in up_came]
    expert_up_full = collect_done(expert_up_weight, up_came)
    expert_up_rows = batch_dot(slot_rows, expert_up_full, 2, 1)
    expert_hidden = swiglu(expert_gate_rows, expert_up_rows).astype(BF16)
    expert_down_full = collect_done(
        expert_down_weight, [after(came, expert_hidden) for came in down_came]
    )
    expert_output = (gate_canonical * batch_dot(expert_hidden, expert_down_full, 2, 1)).astype(BF16)
    routed = scatter_rows(expert_output, chosen_low, num_held, 2, False)

    output = mixed_rows + shared_out + routed
    block_output = output.astype(BF16)
    valid_rows = valid_mask[0].astype(F32)[:, None]
    grad_out = valid_rows * (output - teacher[0].astype(F32))
    grad_low = grad_out.astype(BF16)

    grad_slots = gather_rows(grad_low, chosen_low, num_held, 3, False)
    grad_slots = (gate_canonical * grad_slots.astype(F32)).astype(BF16)

    def expert_grad(left, right, wait):
        grad = after(batch_dot(left, right, 1, 1).astype(BF16), *wait)
        rows = grad.shape[1] // length
        own = [None] * length
        for k in range(length):
            slab = lax.dynamic_slice_in_dim(grad, (seq_index ^ k) * rows, rows, axis=1)
            own[k] = exchange(slab, "seq", k) if k else slab
        return own

    def expert_sum(own, wait):
        own = [after(part, *wait) for part in own]
        same = sum(own[k].astype(F32) for k in range(0, length, PAIR))
        crossed = sum(own[k].astype(F32) for k in range(1, length, PAIR))
        first = (jnp.arange(PAIR) == side)[:, None, None, None]
        return jnp.where(first, same[None], crossed[None]).reshape(num_local, *same.shape[1:])

    expert_down_own = expert_grad(expert_hidden, grad_slots, [])
    grad_hidden = batch_dot(grad_slots, expert_down_full, 2, 2)
    grad_gate_rows, grad_up_rows = swiglu_backward(expert_gate_rows, expert_up_rows, grad_hidden)
    expert_gate_own = expert_grad(slot_rows, grad_gate_rows, [])
    grad_input = (
        batch_dot(grad_gate_rows, expert_gate_full, 2, 2) + batch_dot(grad_up_rows, expert_up_full, 2, 2)
    ).astype(BF16)
    grad_routed = scatter_rows(grad_input, chosen_low, num_held, 4, True)
    grad_shidden = dot(grad_low, down_full, 1, 1)
    grad_sgate_rows, grad_sup_rows = swiglu_backward(shared_gate, shared_up, grad_shidden)
    grad_gate_up = jnp.concatenate([grad_sgate_rows, grad_sup_rows], axis=1)
    grad_normed_two = dot(grad_gate_up, gate_up_full, 1, 1) + grad_routed
    _, pull_two = jax.vjp(rms_norm, mixed_rows, gain_two)
    grad_mixed_norm, grad_gain_two = pull_two(grad_normed_two)
    grad_mixed = grad_out + grad_mixed_norm
    grad_mixed_low = grad_mixed.astype(BF16)

    grad_attended = dot(grad_mixed_low, output_full, 1, 1).astype(BF16)
    grad_query, grad_key_value = attend_back(
        query_rows, key_value_all, seg_rows, seg_line, log_total, grad_attended, score_scale
    )
    expert_up_own = expert_grad(slot_rows, grad_up_rows, [])
    gain_grads = jnp.pad(grad_gain_two.reshape(devices, 1, -1), ((0, 0), (0, 7), (0, 0)))
    gain_rows = gain_grads.shape[2]
    gain_grads = jnp.pad(gain_grads, ((0, 0), (0, 0), (0, lanes - gain_rows)))
    if gain_rows % 16 == 0:
        sums = sum_dense(
            [normed_two.T, attended.T, shared_hidden.T, normed_one.T],
            [grad_gate_up, grad_mixed_low, grad_low, grad_query],
            gain_grads,
            grad_key_value,
            ((shared_width, shared_width), (query_width, feat_width), (feat_width,), (key_width, key_width), (lanes,)),
            (((0, 0),), ((3, 3), (1, 1)), ((2, 2),), ((3, None),)),
            5,
        )
        gate_up_blocks, query_block, grad_output_block = sums[:2], sums[2], sums[3]
        qkv_blocks = [query_block, sums[5], sums[6]]
        grad_down_block, grad_gain_block = sums[4], sums[7]
        grad_qkv = jnp.concatenate([grad_query, sums[8]], axis=1)
    else:
        grad_key_value = jnp.concatenate([grad_key_value[0], grad_key_value[1]], axis=1)
        total = grad_key_value[:tok_rows]
        for step in range(1, back + 1):
            came = shift(total.astype(BF16), "seq", -1)
            total = came.astype(F32) + grad_key_value[step * tok_rows : (step + 1) * tok_rows]
        grad_qkv = jnp.concatenate([grad_query, total.astype(BF16)], axis=1)
        dense_grads = [
            weight_grad(normed_two, grad_gate_up),
            weight_grad(attended, grad_mixed_low),
            weight_grad(shared_hidden, grad_low),
            weight_grad(normed_one, grad_qkv),
            gain_grads,
        ]
        sums = scatter_dense(dense_grads, 5)
        gate_up_blocks, grad_output_block, grad_down_block, qkv_blocks, grad_gain_block = sums
        gate_up_blocks = jnp.split(gate_up_blocks, [shared_width], axis=1)
        qkv_blocks = jnp.split(qkv_blocks, [query_width, query_width + key_width], axis=1)
    grad_normed_one = dot(grad_qkv, qkv_full, 1, 1)
    _, pull_one = jax.vjp(lambda values: rms_norm(values, gain_one), x_float)
    grad_tokens = grad_mixed + pull_one(grad_normed_one)[0]
    grad_gain_one = sum(
        jnp.sum(weight.astype(F32) * grad, axis=1)
        for weight, grad in zip((query_weight, key_weight, value_weight), qkv_blocks)
    ) / norm1_gain.astype(F32)
    last = [grad_gain_block]
    grad_expert_down = expert_sum(expert_down_own, last)
    grad_expert_gate = expert_sum(expert_gate_own, last)
    grad_expert_up = expert_sum(expert_up_own, last)
    return (
        block_output[None],
        grad_tokens[None],
        grad_gain_one,
        *qkv_blocks,
        grad_output_block,
        grad_gain_block[0, :gain_rows],
        *gate_up_blocks,
        grad_down_block,
        grad_expert_gate,
        grad_expert_up,
        grad_expert_down,
    )


def solution(mesh):
    rows = P("fsdp", "seq", None)
    dense = P(("seq", "fsdp"), None)
    gain = P(("seq", "fsdp"))
    return jax.shard_map(
        block,
        mesh=mesh,
        in_specs=(
            rows, rows, P("fsdp", "seq"), P("fsdp", None), rows, rows,
            gain, dense, dense, dense, dense, gain, dense, dense, dense, rows, rows, rows,
        ),
        out_specs=(
            rows, rows, gain, dense, dense, dense, dense, gain, dense, dense, dense, rows, rows, rows,
        ),
        check_vma=False,
    )
```

```python
import functools
import math

import jax
import jax.numpy as jnp
from jax import lax
from jax.experimental import pallas as pl
from jax.experimental.pallas import tpu as pltpu
from jax.sharding import PartitionSpec as P


HEADS = 12
KV_HEADS = 4
HEAD = 128
TOP = 6
EPSILON = 1e-05
MASKED = -1e30
PAIR = 2


BF16 = jnp.bfloat16
F32 = jnp.float32


def exchange(values, axis, bit):
    count = lax.axis_size(axis)
    return lax.ppermute(values, axis, [(i, i ^ bit) for i in range(count)])


def shift(values, axis, step):
    count = lax.axis_size(axis)
    pairs = [(i, i + step) for i in range(count) if 0 <= i + step < count]
    return lax.ppermute(values, axis, pairs)


def after(values, *others):
    return lax.optimization_barrier((values, *others))[0]


def dot(left, right, left_dim, right_dim):
    return lax.dot_general(
        left, right, (((left_dim,), (right_dim,)), ((), ())), preferred_element_type=F32
    )


def batch_dot(left, right, left_dim, right_dim):
    return lax.dot_general(
        left, right, (((left_dim,), (right_dim,)), ((0,), (0,))), preferred_element_type=F32
    )


def rms_norm(values, gain):
    factor = lax.rsqrt(jnp.mean(values * values, axis=-1, keepdims=True) + EPSILON)
    return values * factor * gain


def swiglu(gate_rows, up_rows):
    return jax.nn.silu(gate_rows) * up_rows


def swiglu_backward(gate_rows, up_rows, grad_rows):
    _, pull_back = jax.vjp(swiglu, gate_rows, up_rows)
    grad_gate, grad_up = pull_back(grad_rows)
    return (grad_gate.astype(BF16), grad_up.astype(BF16))


MESH = pl.DeviceIdType.MESH


def grant(scratch, extra):
    size = extra
    for ref in scratch:
        shape = list(ref.shape)
        shape[-2] = -(-shape[-2] // 16) * 16
        size += math.prod(shape) * jnp.dtype(ref.dtype).itemsize
    return min(size + 6 * 2**20, 66 * 10**6)


class Copies:
    def __init__(self, send_sems, recv_sems):
        self.send_sems, self.recv_sems, self.made = send_sems, recv_sems, []

    def start(self, source, target, axis, partner, when=None):
        number = len(self.made)
        copy = pltpu.make_async_remote_copy(
            src_ref=source,
            dst_ref=target,
            send_sem=self.send_sems.at[number],
            recv_sem=self.recv_sems.at[number],
            device_id={axis: partner},
            device_id_type=MESH,
        )
        if when is None:
            copy.start()
        else:
            pl.when(when)(copy.start)
        self.made.append((copy, when))
        return copy

    def finish(self):
        for copy, when in self.made:
            if when is None:
                copy.wait_send()
            else:
                pl.when(when)(copy.wait_send)


def greet(partners):
    barrier = pltpu.get_barrier_semaphore()
    for axis, partner in partners:
        pl.semaphore_signal(barrier, inc=1, device_id={axis: partner}, device_id_type=MESH)
    pl.semaphore_wait(barrier, len(partners))


def bit_of(index, bit):
    return lax.rem(lax.div(index, bit), 2)


def flip(index, bit):
    return index + bit - 2 * bit * bit_of(index, bit)


def flip_all(index, mask):
    bit = 1
    while bit <= mask:
        if mask & bit:
            index = flip(index, bit)
        bit *= 2
    return index


def gather_dense_kernel(length, bits, count, back, *refs):
    extra = 0 if back is None else 1
    shards, expert = refs[:count], refs[count]
    outs, expert_full = refs[count + 1 + extra : 2 * count + 1 + extra], refs[2 * count + 1 + extra]
    if back is None:
        send_sems, recv_sems, local_sems = refs[2 * count + 2 :]
        places = list(outs)
    else:
        tokens = refs[count + 1]
        normed_ref, query_ref, window_ref, held, send_sems, recv_sems, local_sems = refs[2 * count + 3 :]
        places = [held] + list(outs[1:])
    seq, group = lax.axis_index("seq"), lax.axis_index("fsdp")
    own = [bit_of(group, bit) for bit in bits]
    partners = [("seq", flip_all(seq, k)) for k in range(1, length)]
    partners += [("fsdp", flip(group, bit)) for bit in bits]
    greet(partners)
    copies = Copies(send_sems, recv_sems)
    far = len(bits) - 1
    half = length // 2
    side = lax.div(seq, half)
    low = [side * half, (1 - side) * half]
    orders = [list(range(far)), list(range(far))[::-1]]
    hops = length - 1
    stages = hops + far + 1
    waiting = [[] for _ in range(count)]
    right, left = lax.rem(seq + 1, length), lax.rem(seq + length - 1, length)

    def launch(t, stage):
        if stage < hops:
            back_block = lax.rem(seq - stage + length, length)
            next_block = lax.rem(seq + stage, length)
            if stage == 0:
                local = pltpu.make_async_copy(shards[t], places[t].at[(seq, *own)], local_sems.at[t])
                local.start()
            made = []
            for block, target, sends, comes in (
                (back_block, right, (seq >= stage) & (seq + 1 < length), seq > stage),
                (next_block, left, (seq + stage < length) & (seq >= 1), seq + 1 + stage < length),
            ):
                view = places[t].at[(block, *own)]
                source = shards[t] if stage == 0 else view
                made.append((copies.start(source, view, "seq", target, sends).wait_recv, comes))
            if stage == 0:
                made.append((local.wait, None))
            return made
        made = []
        for part in (0, 1):
            where = [pl.ds(low[part], half)] + list(own)
            for done in orders[part][: stage - hops]:
                where[1 + done] = slice(None)
            dim = orders[part][stage - hops] if stage < hops + far else far
            view = places[t].at[tuple(where)]
            made.append((copies.start(view, view, "fsdp", flip(group, bits[dim])).wait_recv, None))
        return made

    def settle(made):
        for wait, when in made:
            if when is None:
                wait()
            else:
                pl.when(when)(wait)

    def ship_expert():
        held_experts, depth = expert.shape[0] // PAIR, expert.shape[1]
        rows = pl.ds(pl.multiple_of(seq * depth, depth), depth)
        parity = lax.rem(seq, PAIR)
        local = pltpu.make_async_copy(
            expert.at[pl.ds(parity * held_experts, held_experts)], expert_full.at[:, rows], local_sems.at[count]
        )
        local.start()
        made = [(local.wait, None)]
        for k in range(1, length):
            mine = pl.ds(lax.rem(parity + k, PAIR) * held_experts, held_experts)
            copy = copies.start(expert.at[mine], expert_full.at[:, rows], "seq", flip_all(seq, k))
            made.append((copy.wait_recv, None))
        return made

    def project():
        rows, width = normed_ref.shape
        query_width = query_ref.shape[1]
        key_width = window_ref.shape[1]

        def columns(start, size):
            return held[(slice(None),) * (2 + far) + (slice(None), pl.ds(start, size))].reshape(width, size)

        gain = columns(query_width + key_width, 128).astype(jnp.float32).T[0:1]
        values = tokens[...].astype(jnp.float32)
        factor = lax.rsqrt(jnp.mean(values * values, axis=-1, keepdims=True) + EPSILON)
        normed_ref[...] = (values * factor * gain).astype(normed_ref.dtype)
        here = pl.ds(back * rows, rows)
        for start in range(0, key_width, 512):
            tile = jnp.dot(
                normed_ref[...], columns(query_width + start, 512), preferred_element_type=jnp.float32
            )
            window_ref[here, pl.ds(start, 512)] = tile.astype(window_ref.dtype)
        for j in range(1, back + 1):

            @pl.when(seq < j)
            def _(j=j):
                window_ref[pl.ds((back - j) * rows, rows)] = jnp.zeros((rows, key_width), window_ref.dtype)

        first = pass_keys(1)
        for start in range(0, query_width, 512):
            tile = jnp.dot(normed_ref[...], columns(start, 512), preferred_element_type=jnp.float32)
            query_ref[:, pl.ds(start, 512)] = tile.astype(query_ref.dtype)
        kept = pltpu.make_async_copy(held, outs[0], local_sems.at[0])
        kept.start()
        return first, kept

    def pass_keys(j):
        rows = normed_ref.shape[0]
        source = window_ref.at[pl.ds((back - j + 1) * rows, rows)]
        target = window_ref.at[pl.ds((back - j) * rows, rows)]
        sends = (seq >= j - 1) & (seq + 1 < length)
        return [(copies.start(source, target, "seq", right, sends).wait_recv, seq >= j)]

    passing, passed = [], 0
    starts = [(t + 1) // 2 for t in range(count)]
    for step in range(starts[-1] + stages + 1):
        for t in range(count):
            stage = step - starts[t]
            if 0 < stage <= stages:
                settle(waiting[t])
            if 0 <= stage < stages:
                waiting[t] = launch(t, stage)
        if step == starts[-1] + hops - 1:
            expert_waiting = ship_expert()
        if step == stages and back is not None:
            passing, kept = project()
            passed = 1
        elif passing and passed < back and step == stages + 2 * passed:
            settle(passing)
            passed += 1
            passing = pass_keys(passed)
    while passing:
        settle(passing)
        passed += 1
        passing = pass_keys(passed) if passed <= back else []
    settle(expert_waiting)
    copies.finish()
    if back is not None:
        kept.wait()


def gather_dense(shards, expert, tokens, back, key_width):
    length, groups = lax.axis_size("seq"), lax.axis_size("fsdp")
    bits, bit = [], groups // 2
    while bit >= 1:
        bits.append(bit)
        bit //= 2
    count = len(shards)
    number = count * 2 * (length - 1 + len(bits)) + length - 1 + back
    size = sum(s.size * s.dtype.itemsize for s in shards) * length * groups
    experts, depth, wide = expert.shape
    lead = (length,) + (2,) * len(bits)
    rows, width = tokens.shape
    fused = shards[0].shape[0] % 16 == 0
    extra_in, extra_out, extra_scratch = [], [], []
    if fused:
        query_width = shards[0].shape[1] - key_width - 128
        extra_in = [tokens]
        extra_out = [
            jax.ShapeDtypeStruct((rows, width), tokens.dtype),
            jax.ShapeDtypeStruct((rows, query_width), tokens.dtype),
            jax.ShapeDtypeStruct(((back + 1) * rows, key_width), tokens.dtype),
        ]
        extra_scratch = [pltpu.VMEM(lead + shards[0].shape, shards[0].dtype)]
    results = pl.pallas_call(
        functools.partial(gather_dense_kernel, length, bits, count, back if fused else None),
        out_shape=[
            jax.ShapeDtypeStruct((length,) + (2,) * len(bits) + s.shape, s.dtype) for s in shards
        ]
        + [jax.ShapeDtypeStruct((experts // PAIR, length * depth, wide), expert.dtype)]
        + extra_out,
        in_specs=[pl.BlockSpec(memory_space=pltpu.VMEM)] * count
        + [pl.BlockSpec(memory_space=pl.ANY)]
        + [pl.BlockSpec(memory_space=pltpu.VMEM)] * len(extra_in),
        out_specs=[pl.BlockSpec(memory_space=pl.ANY)] * (count + 1)
        + [pl.BlockSpec(memory_space=pltpu.VMEM)] * len(extra_out),
        scratch_shapes=extra_scratch
        + [
            pltpu.SemaphoreType.DMA((number,)),
            pltpu.SemaphoreType.DMA((number,)),
            pltpu.SemaphoreType.DMA((count + 1,)),
        ],
        compiler_params=pltpu.CompilerParams(
            collective_id=0, has_side_effects=True, vmem_limit_bytes=60 * 2**20
        ),
        cost_estimate=pl.CostEstimate(flops=0, bytes_accessed=3 * size, transcendentals=0),
        name="gather_dense",
    )(*shards, expert, *extra_in)
    outs = [out.reshape(-1, out.shape[-1]) for out in results[:count]] + [results[count]]
    return outs + (list(results[count + 1 :]) if fused else [None] * 3)


def scatter_dense_kernel(length, bits, count, *refs):
    grads, outs = refs[:count], refs[count : 2 * count]
    far = len(bits) - 1
    per = 3 + far
    scratch = refs[2 * count : 2 * count + per * count]
    send_sems, recv_sems, local_sems = refs[2 * count + per * count :]
    seq, group = lax.axis_index("seq"), lax.axis_index("fsdp")
    own = [bit_of(group, bit) for bit in bits]
    partners = [("seq", flip_all(seq, k)) for k in range(1, length)]
    partners += [("fsdp", flip(group, bit)) for bit in bits]
    greet(partners)
    copies = Copies(send_sems, recv_sems)
    half = length // 2
    side = lax.div(seq, half)
    low = [side * half, (1 - side) * half]
    orders = [list(range(far))[::-1], list(range(far))]
    stages = far + 2
    everything = (slice(None),) * (1 + far)

    def buffers(t):
        held = scratch[per * t : per * (t + 1)]
        return held[0], held[1], held[2 : 2 + far], held[2 + far]

    waiting = [None] * count

    def add(mine, came, lead, fixed, inner_of):
        start, size = lead
        left = [d for d in range(far) if d not in fixed]

        def body(i, carry):
            z = lax.div(i, 2 ** len(left))
            where, inner = [own[d] for d in range(far)], []
            for k, d in enumerate(left):
                where[d] = lax.rem(lax.div(i, 2 ** (len(left) - 1 - k)), 2)
                inner.append(where[d])
            place = (start + z, *where)
            total = mine[place].astype(jnp.float32) + came[inner_of(start + z, z, inner)].astype(jnp.float32)
            mine[place] = total.astype(mine.dtype)
            return carry

        lax.fori_loop(0, size * 2 ** len(left), body, 0)

    def launch(t, stage):
        mine, came_core, came_far, came_seq = buffers(t)
        if stage == 0:
            local = pltpu.make_async_copy(grads[t].at[(*everything, own[far])], mine, local_sems.at[t])
            local.start()
            sent = grads[t].at[(*everything, 1 - own[far])]
            return [copies.start(sent, came_core, "fsdp", flip(group, bits[far]))], local
        if stage <= far:
            made = []
            for part in (0, 1):
                order = orders[part]
                if stage == 1:
                    add(mine, came_core, (low[part], half), [], lambda z, at, inner: (z, *inner))
                else:
                    came = came_far[stage - 2].at[part]
                    add(mine, came, (low[part], half), order[: stage - 1], lambda z, at, inner: (at, *inner))
                dim = order[stage - 1]
                where = [slice(None)] * far
                for d in order[: stage - 1]:
                    where[d] = own[d]
                where[dim] = 1 - own[dim]
                made.append(
                    copies.start(
                        mine.at[(pl.ds(low[part], half), *where)],
                        came_far[stage - 1].at[part],
                        "fsdp",
                        flip(group, bits[dim]),
                    )
                )
            return made, None
        for part in (0, 1):
            came = came_far[far - 1].at[part]
            add(mine, came, (low[part], half), orders[part], lambda z, at, inner: (at,))
        made = []
        for k in range(1, length):
            other = flip_all(seq, k)
            made.append(copies.start(mine.at[(other, *own[:far])], came_seq.at[k - 1], "seq", other))
        return made, None

    def close(t):
        mine, _, _, came_seq = buffers(t)
        total = mine[(seq, *own[:far])].astype(jnp.float32)
        for k in range(1, length):
            total = total + came_seq[k - 1].astype(jnp.float32)
        outs[t][...] = total

    for step in range(count + stages):
        for t in range(count):
            stage = step - t
            if 0 < stage <= stages:
                made, local = waiting[t]
                for copy in made:
                    copy.wait_recv()
                if local is not None:
                    local.wait()
            if 0 <= stage < stages:
                waiting[t] = launch(t, stage)
            elif stage == stages:
                close(t)
    copies.finish()


def scatter_dense(grads, collective_id):
    length, groups = lax.axis_size("seq"), lax.axis_size("fsdp")
    bits, bit = [], groups // 2
    while bit >= 1:
        bits.append(bit)
        bit //= 2
    far = len(bits) - 1
    count = len(grads)
    number = count * (1 + 2 * far + length - 1)
    size = sum(g.size * g.dtype.itemsize for g in grads)
    scratch = []
    for g in grads:
        block = g.shape[1:]
        scratch += [pltpu.VMEM((length,) + (2,) * far + block, g.dtype)] * 2
        scratch += [
            pltpu.VMEM((2, length // 2) + (2,) * (far - 1 - s) + block, g.dtype) for s in range(far)
        ]
        scratch.append(pltpu.VMEM((length - 1,) + block, g.dtype))
    return pl.pallas_call(
        functools.partial(scatter_dense_kernel, length, bits, count),
        out_shape=[jax.ShapeDtypeStruct(g.shape[1:], jnp.float32) for g in grads],
        in_specs=[pl.BlockSpec(memory_space=pl.ANY)] * count,
        out_specs=[pl.BlockSpec(memory_space=pltpu.VMEM)] * count,
        scratch_shapes=scratch
        + [
            pltpu.SemaphoreType.DMA((number,)),
            pltpu.SemaphoreType.DMA((number,)),
            pltpu.SemaphoreType.DMA((count,)),
        ],
        compiler_params=pltpu.CompilerParams(
            collective_id=collective_id, has_side_effects=True, vmem_limit_bytes=grant(scratch, 0)
        ),
        cost_estimate=pl.CostEstimate(flops=0, bytes_accessed=3 * size, transcendentals=0),
        name="scatter_dense",
    )(*[g.reshape((length,) + (2,) * len(bits) + g.shape[1:]) for g in grads])


def sum_dense_kernel(length, bits, cuts, plan, keys_at, back, *refs):
    count = len(cuts)
    weights = count - 1
    act_count = 1 + max(a for group in plan for a, _ in group)
    grad_count = 1 + max(g for group in plan for _, g in group if g is not None)
    acts, grads = refs[:act_count], refs[act_count : act_count + grad_count]
    ready, window, *refs = refs[act_count + grad_count :]
    number = sum(len(cut) for cut in cuts)
    flat_outs, keys_out, refs = list(refs[:number]), refs[number], refs[number + 1 :]
    outs = [[flat_outs.pop(0) for _ in cut] for cut in cuts]
    far = len(bits) - 1
    per = 3 + far
    scratch = refs[: per * count]
    keys_sum, keys_sent, keys_came, send_sems, recv_sems = refs[per * count :]
    seq, group = lax.axis_index("seq"), lax.axis_index("fsdp")
    own = [bit_of(group, bit) for bit in bits]
    partners = [("seq", flip_all(seq, k)) for k in range(1, length)]
    partners += [("fsdp", flip(group, bit)) for bit in bits]
    greet(partners)
    copies = Copies(send_sems, recv_sems)
    half = length // 2
    side = lax.div(seq, half)
    low = [side * half, (1 - side) * half]
    orders = [list(range(far))[::-1], list(range(far))]
    stages = far + 2
    everything = (slice(None),) * (1 + far)
    rows, key_width = keys_sum.shape[0], window.shape[2]
    left = lax.rem(seq + length - 1, length)

    def buffers(t):
        held = scratch[per * t : per * (t + 1)]
        return held[0], held[1], held[2 : 2 + far], held[2 + far]

    def key_piece(b, part):
        return window[part, pl.ds(b * rows, rows)]

    def send_keys(j):
        copy = copies.start(keys_sent.at[j], keys_came.at[j], "seq", left, seq >= 1)
        return copy

    def advance_keys(j, copy):
        for part in (0, 1):
            keys_sum[:, pl.ds(part * key_width, key_width)] = key_piece(j, part)

        @pl.when(seq + 1 < length)
        def _():
            copy.wait_recv()
            keys_sum[...] = keys_sum[...] + keys_came[j - 1].astype(jnp.float32)

        if j < back:
            keys_sent[j] = keys_sum[...].astype(keys_sent.dtype)
            return send_keys(j)
        keys_out[...] = keys_sum[...].astype(keys_out.dtype)
        return None

    def produce(t):
        held = buffers(t)[0]
        if t == weights:
            held[...] = ready[...]
            return
        block = held.shape[-2]

        def body(z, carry):
            start = 0
            for a, g in plan[t]:
                depth = acts[a].shape[0] // length
                left_rows = acts[a][pl.ds(pl.multiple_of(z * depth, depth), depth)]
                source = keys_out if g is None else grads[g]
                for c in range(0, source.shape[1], 512):
                    tile = jnp.dot(left_rows, source[:, c : c + 512], preferred_element_type=jnp.float32)
                    tile = tile.astype(held.dtype).reshape((2,) * (far + 1) + (block, 512))
                    held[(z, *(slice(None),) * (far + 2), pl.ds(start, 512))] = tile
                    start += 512
            return carry

        lax.fori_loop(0, length, body, 0)

    def add(held, came, lead, fixed, inner_of):
        start, size = lead
        free = [d for d in range(far) if d not in fixed]

        def body(i, carry):
            z = lax.div(i, 2 ** len(free))
            where, inner = [own[d] for d in range(far)], []
            for k, d in enumerate(free):
                where[d] = lax.rem(lax.div(i, 2 ** (len(free) - 1 - k)), 2)
                inner.append(where[d])
            place = (start + z, *where, own[far])
            total = held[place].astype(jnp.float32) + came[inner_of(start + z, z, inner)].astype(jnp.float32)
            held[place] = total.astype(held.dtype)
            return carry

        lax.fori_loop(0, size * 2 ** len(free), body, 0)

    def launch(t, stage):
        held, came_core, came_far, came_seq = buffers(t)
        if stage == 0:
            produce(t)
            return [copies.start(held.at[(*everything, 1 - own[far])], came_core, "fsdp", flip(group, bits[far]))]
        made = []
        if stage <= far:
            for part in (0, 1):
                order = orders[part]
                if stage == 1:
                    add(held, came_core, (low[part], half), [], lambda z, at, inner: (z, *inner))
                else:
                    came = came_far[stage - 2].at[part]
                    add(held, came, (low[part], half), order[: stage - 1], lambda z, at, inner: (at, *inner))
                dim = order[stage - 1]
                where = [slice(None)] * far
                for d in order[: stage - 1]:
                    where[d] = own[d]
                where[dim] = 1 - own[dim]
                source = held.at[(pl.ds(low[part], half), *where, own[far])]
                made.append(
                    copies.start(source, came_far[stage - 1].at[part], "fsdp", flip(group, bits[dim]))
                )
            return made
        for part in (0, 1):
            add(held, came_far[far - 1].at[part], (low[part], half), orders[part], lambda z, at, inner: (at,))
        for k in range(1, length):
            other = flip_all(seq, k)
            made.append(copies.start(held.at[(other, *own)], came_seq.at[k - 1], "seq", other))
        return made

    def close(t):
        held, _, _, came_seq = buffers(t)
        total = held[(seq, *own)].astype(jnp.float32)
        for k in range(1, length):
            total = total + came_seq[k - 1].astype(jnp.float32)
        start = 0
        for out, size in zip(outs[t], cuts[t]):
            out[...] = total[:, start : start + size]
            start += size

    for part in (0, 1):
        keys_sent[0, :, pl.ds(part * key_width, key_width)] = key_piece(0, part).astype(keys_sent.dtype)
    flying = send_keys(0)
    waiting = [[] for _ in range(count)]
    starts = [min(t, count - 2) for t in range(count)]
    for step in range(starts[-1] + stages):
        for t in range(count):
            stage = step - starts[t]
            if 0 < stage < stages:
                for copy in waiting[t]:
                    copy.wait_recv()
            if stage == 0 and t == keys_at:
                advance_keys(back, flying)
            if 0 <= stage < stages:
                waiting[t] = launch(t, stage)
        hop = step - starts[keys_at] + back
        if 1 <= hop < back:
            flying = advance_keys(hop, flying)
    for t in range(count):
        for copy in waiting[t]:
            copy.wait_recv()
        close(t)
    copies.finish()


def sum_dense(acts, grads, ready, window, cuts, plan, collective_id):
    length, groups = lax.axis_size("seq"), lax.axis_size("fsdp")
    bits, bit = [], groups // 2
    while bit >= 1:
        bits.append(bit)
        bit //= 2
    far = len(bits) - 1
    devices = length * groups
    rows = grads[0].shape[0]
    back = window.shape[1] // rows - 1
    key_width = 2 * window.shape[2]
    blocks = [
        ((acts[group[0][0]].shape[0] // devices, sum(cut)), grads[0].dtype) for group, cut in zip(plan, cuts)
    ]
    keys_at = [any(g is None for _, g in group) for group in plan].index(True)
    blocks.append((ready.shape[1:], ready.dtype))
    count = len(blocks)
    number = count * (1 + 2 * far + length - 1) + back
    scratch = []
    for block, dtype in blocks:
        scratch.append(pltpu.VMEM((length,) + (2,) * (far + 1) + block, dtype))
        scratch.append(pltpu.VMEM((length,) + (2,) * far + block, dtype))
        scratch += [pltpu.VMEM((2, length // 2) + (2,) * (far - 1 - s) + block, dtype) for s in range(far)]
        scratch.append(pltpu.VMEM((length - 1,) + block, dtype))
    scratch.append(pltpu.VMEM((rows, key_width), jnp.float32))
    scratch += [pltpu.VMEM((back, rows, key_width), grads[0].dtype)] * 2
    elements = sum(math.prod(block) for block, _ in blocks) * devices
    return pl.pallas_call(
        functools.partial(sum_dense_kernel, length, bits, cuts, plan, keys_at, back),
        out_shape=[
            jax.ShapeDtypeStruct((block[0], size), jnp.float32)
            for (block, _), cut in zip(blocks, cuts)
            for size in cut
        ]
        + [jax.ShapeDtypeStruct((rows, key_width), grads[0].dtype)],
        in_specs=[pl.BlockSpec(memory_space=pltpu.VMEM)] * (len(acts) + len(grads) + 2),
        out_specs=[pl.BlockSpec(memory_space=pltpu.VMEM)] * (sum(len(cut) for cut in cuts) + 1),
        scratch_shapes=scratch + [pltpu.SemaphoreType.DMA((number,))] * 2,
        compiler_params=pltpu.CompilerParams(
            collective_id=collective_id, has_side_effects=True, vmem_limit_bytes=67 * 10**6
        ),
        cost_estimate=pl.CostEstimate(
            flops=2 * elements * rows, bytes_accessed=4 * elements, transcendentals=0
        ),
        name="sum_dense",
    )(*acts, *grads, ready.reshape((length,) + (2,) * len(bits) + ready.shape[1:]), window)


def row_dims():
    groups = lax.axis_size("fsdp")
    dims, bit = [("seq", 1)], groups // 2
    while bit >= 1:
        dims.append(("fsdp", bit))
        bit //= 2
    return dims


def row_places(dims):
    seq, group = lax.axis_index("seq"), lax.axis_index("fsdp")
    index = {"seq": seq, "fsdp": group}
    own = [bit_of(index[axis], bit) for axis, bit in dims]
    partner = [(axis, flip(index[axis], bit)) for axis, bit in dims]
    return own, partner


def row_orders(far, light):
    if light:
        return [[0] + [1 + (i + k) % (far - 1) for k in range(far - 1)] for i in range(far - 1)]
    return [[(i + k) % far for k in range(far)] for i in range(far)]


def gather_rows_kernel(dims, orders, held, rows_ref, pick_ref, slots_ref, buffer, send_sems, recv_sems, local_sem):
    own, partner = row_places(dims)
    greet(partner)
    copies = Copies(send_sems, recv_sems)
    far = len(dims) - 1
    pieces = len(orders)
    width = rows_ref.shape[1] // pieces
    capacity = slots_ref.shape[-2]

    def view(piece, done):
        where = list(own)
        for d in done:
            where[d] = slice(None)
        return buffer.at[(piece, *where)]

    flying, local = [], []
    for piece in range(pieces):
        cut = rows_ref.at[:, pl.ds(piece * width, width)]
        flying.append(copies.start(cut, view(piece, []), *partner[orders[piece][0]]))
        local.append(pltpu.make_async_copy(cut, view(piece, []), local_sem.at[piece]))
        local[piece].start()
    for copy in local:
        copy.wait()

    def pick_block(piece, where):
        taken = jnp.dot(
            pick_ref[tuple(where)], buffer[(piece, *where)], preferred_element_type=jnp.float32
        ).astype(slots_ref.dtype)
        for e in range(held):
            slots_ref[(e, *where, slice(None), pl.ds(piece * width, width))] = taken[
                e * capacity : (e + 1) * capacity
            ]

    def pick_all(piece, core):
        def body(i, carry):
            where, rest = [], i
            for d in range(far):
                where.append(lax.rem(lax.div(rest, 2 ** (far - 1 - d)), 2))
            pick_block(piece, where + [core])
            return carry

        lax.fori_loop(0, 2**far, body, 0)

    for stage in range(1, far + 1):
        for piece in range(pieces):
            flying[piece].wait_recv()
            order = orders[piece]
            done = order[:stage]
            ref = view(piece, done)
            flying[piece] = copies.start(ref, ref, *(partner[order[stage]] if stage < far else partner[far]))
    for piece in range(pieces):
        pick_all(piece, own[far])
    for piece in range(pieces):
        flying[piece].wait_recv()
        pick_all(piece, 1 - own[far])
    copies.finish()


def gather_rows(rows, pick_low, held, collective_id, light):
    dims = row_dims()
    far = len(dims) - 1
    orders = row_orders(far, light)
    count, feat = rows.shape
    width = feat // len(orders)
    sources = 2 ** len(dims)
    capacity = pick_low.shape[1] // held
    lead = (2,) * len(dims)
    number = len(orders) * (far + 1)
    scratch = [pltpu.VMEM((len(orders),) + lead + (count, width), rows.dtype)]
    slots = pl.pallas_call(
        functools.partial(gather_rows_kernel, dims, orders, held),
        out_shape=jax.ShapeDtypeStruct((held,) + lead + (capacity, feat), rows.dtype),
        in_specs=[pl.BlockSpec(memory_space=pltpu.VMEM)] * 2,
        out_specs=pl.BlockSpec(memory_space=pltpu.VMEM),
        scratch_shapes=scratch
        + [pltpu.SemaphoreType.DMA((n,)) for n in (number, number, len(orders))],
        compiler_params=pltpu.CompilerParams(
            collective_id=collective_id,
            has_side_effects=True,
            vmem_limit_bytes=grant(scratch, 12 * 2**20),
        ),
        cost_estimate=pl.CostEstimate(
            flops=2 * sources * pick_low.shape[1] * count * feat,
            bytes_accessed=6 * sources * count * feat,
            transcendentals=0,
        ),
        name="gather_rows",
    )(rows, pick_low.reshape(lead + pick_low.shape[1:]))
    return slots.reshape(held, sources * capacity, feat)


def scatter_rows_kernel(
    dims, orders, held, base, slots_ref, pick_ref, out_ref, mine, other, came_core, came_far, send_sems, recv_sems
):
    own, partner = row_places(dims)
    greet(partner)
    copies = Copies(send_sems, recv_sems)
    far = len(dims) - 1
    pieces = len(orders)
    width = out_ref.shape[1] // pieces
    capacity = slots_ref.shape[-2]
    count = out_ref.shape[0]

    def spread(piece, core, target):
        def body(i, carry):
            where = [lax.rem(lax.div(i, 2 ** (far - 1 - d)), 2) for d in range(far)]
            total = jnp.zeros((count, width), jnp.float32)
            for e in range(held):
                rows = slots_ref[(e, *where, core, slice(None), pl.ds(piece * width, width))]
                chosen = pick_ref[(*where, core, pl.ds(e * capacity, capacity))]
                total = total + lax.dot_general(
                    chosen, rows, (((0,), (0,)), ((), ())), preferred_element_type=jnp.float32
                )
            target[(piece, *where)] = total.astype(target.dtype)
            return carry

        lax.fori_loop(0, 2**far, body, 0)

    flying = []
    for piece in range(pieces):
        spread(piece, 1 - own[far], other)
        flying.append(copies.start(other.at[piece], came_core.at[piece], *partner[far]))
    for piece in range(pieces):
        spread(piece, own[far], mine)

    def add_into(piece, fixed, came_view):
        left = [d for d in range(far) if d not in fixed]

        def body(i, carry):
            where, inner = [None] * far, []
            for k, d in enumerate(left):
                where[d] = lax.rem(lax.div(i, 2 ** (len(left) - 1 - k)), 2)
                inner.append(where[d])
            for d in fixed:
                where[d] = own[d]
            total = mine[(piece, *where)].astype(jnp.float32) + came_view[tuple(inner)].astype(jnp.float32)
            mine[(piece, *where)] = total.astype(mine.dtype)
            return carry

        lax.fori_loop(0, 2 ** len(left), body, 0)

    for stage in range(far):
        for piece in range(pieces):
            order = orders[piece][::-1]
            fixed = order[:stage]
            flying[piece].wait_recv()
            add_into(piece, fixed, came_core.at[piece] if stage == 0 else came_far[stage - 1].at[piece])
            dim = order[stage]
            where = [slice(None)] * far
            for d in fixed:
                where[d] = own[d]
            where[dim] = 1 - own[dim]
            flying[piece] = copies.start(
                mine.at[(piece, *where)], came_far[stage].at[piece], *partner[dim]
            )
    for piece in range(pieces):
        flying[piece].wait_recv()
        columns = pl.ds(piece * width, width)
        total = mine[(piece, *own[:far])].astype(jnp.float32) + came_far[far - 1][piece].astype(jnp.float32)
        out_ref[:, columns] = total if base is None else base[:, columns] + total
    copies.finish()


def scatter_rows(slots, pick_low, held, collective_id, light, base=None):
    dims = row_dims()
    far = len(dims) - 1
    orders = row_orders(far, light)
    count, feat = pick_low.shape[2], slots.shape[2]
    width = feat // len(orders)
    sources = 2 ** len(dims)
    capacity = pick_low.shape[1] // held
    lead = (2,) * len(dims)
    number = len(orders) * (far + 1)

    scratch = [pltpu.VMEM((len(orders),) + (2,) * far + (count, width), slots.dtype)] * 3
    scratch += [pltpu.VMEM((len(orders),) + (2,) * (far - 1 - s) + (count, width), slots.dtype) for s in range(far)]

    extra = [] if base is None else [base]

    def kernel(slots_ref, pick_ref, *refs):
        base_ref, refs = (None, refs) if base is None else (refs[0], refs[1:])
        out_ref, mine, other, came_core, *rest = refs
        came_far, sems = rest[:far], rest[far:]
        scatter_rows_kernel(
            dims, orders, held, base_ref, slots_ref, pick_ref, out_ref, mine, other, came_core, came_far, *sems
        )

    return pl.pallas_call(
        kernel,
        out_shape=jax.ShapeDtypeStruct((count, feat), jnp.float32),
        in_specs=[pl.BlockSpec(memory_space=pltpu.VMEM)] * (2 + len(extra)),
        out_specs=pl.BlockSpec(memory_space=pltpu.VMEM),
        scratch_shapes=scratch + [pltpu.SemaphoreType.DMA((number,)), pltpu.SemaphoreType.DMA((number,))],
        compiler_params=pltpu.CompilerParams(
            collective_id=collective_id,
            has_side_effects=True,
            vmem_limit_bytes=grant(scratch, 4 * 2**20),
        ),
        cost_estimate=pl.CostEstimate(
            flops=2 * sources * pick_low.shape[1] * count * feat,
            bytes_accessed=6 * sources * count * feat,
            transcendentals=0,
        ),
        name="scatter_rows",
    )(slots.reshape((held,) + lead + (capacity, feat)), pick_low.reshape(lead + pick_low.shape[1:]), *extra)


def allowed_keys(seg_rows_ref, seg_keys_ref, back_rows):
    shape = (seg_rows_ref.shape[0], seg_keys_ref.shape[1])
    row = lax.broadcasted_iota(jnp.int32, shape, 0) + back_rows
    key = lax.broadcasted_iota(jnp.int32, shape, 1)
    return (key <= row) & (seg_rows_ref[...] == seg_keys_ref[...])


def attend_kernel(scale, back_rows, query, key, value, seg_rows, seg_keys, out, log_total):
    allowed = allowed_keys(seg_rows, seg_keys, back_rows)
    keys, values = key[...], value[...]
    lane = lax.broadcasted_iota(jnp.int32, (query.shape[0], 128), 1)
    logs = jnp.zeros((query.shape[0], 128), jnp.float32)
    for j in range(query.shape[1] // HEAD):
        columns = slice(j * HEAD, (j + 1) * HEAD)
        scores = lax.dot_general(
            query[:, columns], keys, (((1,), (1,)), ((), ())), preferred_element_type=jnp.float32
        )
        scores = jnp.where(allowed, scores * scale, MASKED)
        top = jnp.max(scores, axis=1, keepdims=True)
        weights = jnp.exp(scores - top)
        total = jnp.sum(weights, axis=1, keepdims=True)
        prob = (weights * (1.0 / total)).astype(jnp.bfloat16)
        out[:, columns] = jnp.dot(prob, values, preferred_element_type=jnp.float32).astype(out.dtype)
        logs = jnp.where(lane == j, top + jnp.log(total), logs)
    log_total[...] = logs


def attend_back_kernel(
    scale, back_rows, query, key, value, seg_rows, seg_keys, log_total, grad, grad_query, grad_key_value
):
    allowed = allowed_keys(seg_rows, seg_keys, back_rows)
    keys, values = key[...], value[...]
    grad_keys = jnp.zeros(keys.shape, jnp.float32)
    grad_values = jnp.zeros(values.shape, jnp.float32)
    for j in range(query.shape[1] // HEAD):
        columns = slice(j * HEAD, (j + 1) * HEAD)
        rows, grad_rows = query[:, columns], grad[:, columns]
        scores = lax.dot_general(
            rows, keys, (((1,), (1,)), ((), ())), preferred_element_type=jnp.float32
        )
        scores = jnp.where(allowed, scores * scale, MASKED)
        prob = jnp.exp(scores - log_total[:, j : j + 1])
        grad_prob = lax.dot_general(
            grad_rows, values, (((1,), (1,)), ((), ())), preferred_element_type=jnp.float32
        )
        delta = jnp.sum(prob * grad_prob, axis=1, keepdims=True)
        grad_scores = (prob * (grad_prob - delta)).astype(jnp.bfloat16)
        grad_query[:, columns] = (
            jnp.dot(grad_scores, keys, preferred_element_type=jnp.float32) * scale
        ).astype(grad_query.dtype)
        grad_keys = grad_keys + lax.dot_general(
            grad_scores, rows, (((0,), (0,)), ((), ())), preferred_element_type=jnp.float32
        )
        grad_values = grad_values + lax.dot_general(
            prob.astype(jnp.bfloat16), grad_rows, (((0,), (0,)), ((), ())), preferred_element_type=jnp.float32
        )
    grad_key_value[0] = grad_keys * scale
    grad_key_value[1] = grad_values


def attend_specs(tok_rows, window, group_width):
    return [
        pl.BlockSpec((tok_rows, group_width), lambda g: (0, g)),
        pl.BlockSpec((window, HEAD), lambda g: (0, g)),
        pl.BlockSpec((window, HEAD), lambda g: (0, KV_HEADS + g)),
        pl.BlockSpec((tok_rows, 1), lambda g: (0, 0)),
        pl.BlockSpec((1, window), lambda g: (0, 0)),
    ]


def attend(query, key_value, seg_rows, seg_keys, scale):
    tok_rows, window = query.shape[0], key_value.shape[0]
    group_width = query.shape[1] // KV_HEADS
    return pl.pallas_call(
        functools.partial(attend_kernel, scale, window - tok_rows),
        grid=(KV_HEADS,),
        in_specs=attend_specs(tok_rows, window, group_width),
        out_specs=[
            pl.BlockSpec((tok_rows, group_width), lambda g: (0, g)),
            pl.BlockSpec((None, tok_rows, 128), lambda g: (g, 0, 0)),
        ],
        out_shape=[
            jax.ShapeDtypeStruct(query.shape, query.dtype),
            jax.ShapeDtypeStruct((KV_HEADS, tok_rows, 128), jnp.float32),
        ],
        compiler_params=pltpu.CompilerParams(vmem_limit_bytes=32 * 2**20),
        cost_estimate=pl.CostEstimate(
            flops=4 * HEADS * tok_rows * window * HEAD,
            bytes_accessed=8 * query.size,
            transcendentals=HEADS * tok_rows * window,
        ),
        name="attend",
    )(query, key_value, key_value, seg_rows, seg_keys)


def attend_back(query, key_value, seg_rows, seg_keys, log_total, grad, scale):
    tok_rows, window = query.shape[0], key_value.shape[0]
    group_width = query.shape[1] // KV_HEADS
    return pl.pallas_call(
        functools.partial(attend_back_kernel, scale, window - tok_rows),
        grid=(KV_HEADS,),
        in_specs=attend_specs(tok_rows, window, group_width)
        + [
            pl.BlockSpec((None, tok_rows, 128), lambda g: (g, 0, 0)),
            pl.BlockSpec((tok_rows, group_width), lambda g: (0, g)),
        ],
        out_specs=[
            pl.BlockSpec((tok_rows, group_width), lambda g: (0, g)),
            pl.BlockSpec((2, window, HEAD), lambda g: (0, 0, g)),
        ],
        out_shape=[
            jax.ShapeDtypeStruct(query.shape, query.dtype),
            jax.ShapeDtypeStruct((2, window, KV_HEADS * HEAD), jnp.float32),
        ],
        compiler_params=pltpu.CompilerParams(vmem_limit_bytes=32 * 2**20),
        cost_estimate=pl.CostEstimate(
            flops=10 * HEADS * tok_rows * window * HEAD,
            bytes_accessed=16 * query.size,
            transcendentals=HEADS * tok_rows * window,
        ),
        name="attend_back",
    )(query, key_value, key_value, seg_rows, seg_keys, log_total, grad)


def block(
    tokens,
    teacher,
    valid_mask,
    segment_ids,
    routes,
    gate_weights,
    norm1_gain,
    query_weight,
    key_weight,
    value_weight,
    output_weight,
    norm2_gain,
    shared_gate_weight,
    shared_up_weight,
    shared_down_weight,
    expert_gate_weight,
    expert_up_weight,
    expert_down_weight,
):
    length, groups = lax.axis_size("seq"), lax.axis_size("fsdp")
    seq_index, group_index = lax.axis_index("seq"), lax.axis_index("fsdp")
    devices = length * groups
    tok_rows, feat_width = tokens.shape[1], tokens.shape[2]
    seq_len = segment_ids.shape[1]
    score_scale = 1.0 / math.sqrt(HEAD)
    key_width = KV_HEADS * HEAD
    query_width = HEADS * HEAD
    shared_width = shared_gate_weight.shape[1]

    lanes = 128
    gains = jnp.pad(jnp.stack([norm1_gain, norm2_gain], axis=1), ((0, 0), (0, lanes - 2)))
    meta = jnp.concatenate([routes[0].T.astype(F32), gate_weights[0].T], axis=0)
    meta = jnp.pad(meta, ((0, 16 - 2 * TOP), (0, 0)))
    longest = seq_len // 2
    back = min(length - 1, -(-(longest - 1) // tok_rows))
    gathered = gather_dense(
        [
            jnp.concatenate([query_weight, key_weight, value_weight, gains], axis=1),
            output_weight,
            jnp.concatenate([shared_gate_weight, shared_up_weight], axis=1),
            shared_down_weight,
            meta,
        ],
        expert_gate_weight,
        tokens[0],
        back,
        2 * key_width,
    )
    qkv_full, output_full, gate_up_full, down_full, meta, expert_gate_full = gathered[:6]
    normed_one, query_rows, key_value_all = gathered[6:]

    def weight_grad(rows, grad_rows):
        grad = dot(rows, grad_rows, 0, 0).astype(BF16)
        return grad.reshape(devices, -1, grad.shape[1])

    qkv_width = query_width + 2 * key_width
    gain_plain = qkv_full[:, qkv_width : qkv_width + 2].T.astype(F32)
    qkv_full = qkv_full[:, :qkv_width]
    gain_one, gain_two = gain_plain[0], gain_plain[1]

    num_local = expert_gate_weight.shape[0]
    num_held = num_local // PAIR
    side = seq_index % PAIR

    def share(weight, k):
        return lax.dynamic_slice_in_dim(weight, (side ^ (k % PAIR)) * num_held, num_held, axis=0)

    def collect_start(weight, wait):
        sent = after(weight, *wait)
        return [exchange(share(sent, k), "seq", k) for k in range(1, length)]

    def collect_done(weight, came):
        part = weight.shape[1]
        full = jnp.zeros((num_held, length * part, weight.shape[2]), weight.dtype)
        for k, block in enumerate([share(weight, 0)] + came):
            full = lax.dynamic_update_slice(full, block, (0, (seq_index ^ k) * part, 0))
        return full

    x_float = tokens[0].astype(F32)
    if normed_one is None:
        normed_one = rms_norm(x_float, gain_one).astype(BF16)
        qkv_rows = dot(normed_one, qkv_full, 1, 0).astype(BF16)
        query_rows = qkv_rows[:, :query_width]
        key_value = [qkv_rows[:, query_width:]]
        for _ in range(back):
            key_value.insert(0, shift(key_value[0], "seq", 1))
        key_value_all = jnp.concatenate(key_value, axis=0)
    up_came = collect_start(expert_up_weight, [key_value_all])
    window = (back + 1) * tok_rows
    seg_padded = jnp.concatenate([jnp.full((back * tok_rows,), -1, jnp.int32), segment_ids[0]])
    seg_keys = lax.dynamic_slice_in_dim(seg_padded, seq_index * tok_rows, window)
    seg_here = seg_keys[back * tok_rows :]
    seg_rows, seg_line = seg_here[:, None], seg_keys[None, :]
    attended, log_total = attend(query_rows, key_value_all, seg_rows, seg_line, score_scale)
    mixed_rows = x_float + dot(attended, output_full, 1, 0)
    normed_two = rms_norm(mixed_rows, gain_two).astype(BF16)

    experts_all = num_local * groups
    capacity = tok_rows * TOP * 4 // (3 * experts_all)
    meta = lax.dynamic_slice_in_dim(
        meta.reshape(length, groups, 16, tok_rows), seq_index // PAIR * PAIR, PAIR, axis=0
    ).reshape(PAIR * groups, 16, tok_rows)
    route_all, gate_all = meta[:, :TOP], meta[:, TOP : 2 * TOP]
    held_ids = group_index * num_local + side * num_held + jnp.arange(num_held, dtype=jnp.int32)
    named = route_all[:, None] == held_ids.astype(F32)[None, :, None, None]
    has = jnp.any(named, axis=2)
    gate_of = jnp.sum(jnp.where(named, gate_all[:, None], 0.0), axis=2)
    token_order = jnp.arange(tok_rows, dtype=jnp.int32)
    earlier = (token_order[:, None] < token_order[None, :]).astype(BF16)
    before = lax.dot_general(
        has.astype(BF16), earlier, (((2,), (0,)), ((), ())), preferred_element_type=F32
    )
    slot_number = jnp.arange(capacity, dtype=F32)
    chosen = has[:, :, None] & (before[:, :, None] == slot_number[None, None, :, None])
    gate_slots = jnp.sum(jnp.where(chosen, gate_of[:, :, None], 0.0), axis=3)
    sources = PAIR * groups
    chosen_low = chosen.astype(BF16).reshape(sources, num_held * capacity, tok_rows)
    gate_canonical = jnp.moveaxis(gate_slots, 0, 1).reshape(num_held, sources * capacity, 1)
    down_came = collect_start(expert_down_weight, [normed_two])
    slot_rows = gather_rows(normed_two, chosen_low, num_held, 1, False)

    gate_up = dot(normed_two, gate_up_full, 1, 0)
    shared_gate, shared_up = gate_up[:, :shared_width], gate_up[:, shared_width:]
    shared_hidden = swiglu(shared_gate, shared_up).astype(BF16)
    shared_out = dot(shared_hidden, down_full, 1, 0)
    expert_gate_rows = batch_dot(slot_rows, expert_gate_full, 2, 1)
    up_came = [after(came, shared_out) for came in up_came]
    expert_up_full = collect_done(expert_up_weight, up_came)
    expert_up_rows = batch_dot(slot_rows, expert_up_full, 2, 1)
    expert_hidden = swiglu(expert_gate_rows, expert_up_rows).astype(BF16)
    expert_down_full = collect_done(
        expert_down_weight, [after(came, expert_hidden) for came in down_came]
    )
    expert_output = (gate_canonical * batch_dot(expert_hidden, expert_down_full, 2, 1)).astype(BF16)
    routed = scatter_rows(expert_output, chosen_low, num_held, 2, False)

    output = mixed_rows + shared_out + routed
    block_output = output.astype(BF16)
    valid_rows = valid_mask[0].astype(F32)[:, None]
    grad_out = valid_rows * (output - teacher[0].astype(F32))
    grad_low = grad_out.astype(BF16)

    grad_slots = gather_rows(grad_low, chosen_low, num_held, 3, False)
    grad_slots = (gate_canonical * grad_slots.astype(F32)).astype(BF16)

    def expert_grad(left, right, wait):
        grad = after(batch_dot(left, right, 1, 1).astype(BF16), *wait)
        rows = grad.shape[1] // length
        own = [None] * length
        for k in range(length):
            slab = lax.dynamic_slice_in_dim(grad, (seq_index ^ k) * rows, rows, axis=1)
            own[k] = exchange(slab, "seq", k) if k else slab
        return own

    def expert_sum(own, wait):
        own = [after(part, *wait) for part in own]
        same = sum(own[k].astype(F32) for k in range(0, length, PAIR))
        crossed = sum(own[k].astype(F32) for k in range(1, length, PAIR))
        first = (jnp.arange(PAIR) == side)[:, None, None, None]
        return jnp.where(first, same[None], crossed[None]).reshape(num_local, *same.shape[1:])

    expert_down_own = expert_grad(expert_hidden, grad_slots, [])
    grad_hidden = batch_dot(grad_slots, expert_down_full, 2, 2)
    grad_gate_rows, grad_up_rows = swiglu_backward(expert_gate_rows, expert_up_rows, grad_hidden)
    expert_gate_own = expert_grad(slot_rows, grad_gate_rows, [])
    grad_input = (
        batch_dot(grad_gate_rows, expert_gate_full, 2, 2) + batch_dot(grad_up_rows, expert_up_full, 2, 2)
    ).astype(BF16)
    grad_shidden = dot(grad_low, down_full, 1, 1)
    grad_sgate_rows, grad_sup_rows = swiglu_backward(shared_gate, shared_up, grad_shidden)
    grad_gate_up = jnp.concatenate([grad_sgate_rows, grad_sup_rows], axis=1)
    grad_shared = dot(grad_gate_up, gate_up_full, 1, 1)
    grad_routed = scatter_rows(grad_input, chosen_low, num_held, 4, True, grad_shared)
    grad_normed_two = grad_routed
    _, pull_two = jax.vjp(rms_norm, mixed_rows, gain_two)
    grad_mixed_norm, grad_gain_two = pull_two(grad_normed_two)
    grad_mixed = grad_out + grad_mixed_norm
    grad_mixed_low = grad_mixed.astype(BF16)

    grad_attended = dot(grad_mixed_low, output_full, 1, 1).astype(BF16)
    grad_query, grad_key_value = attend_back(
        query_rows, key_value_all, seg_rows, seg_line, log_total, grad_attended, score_scale
    )
    expert_up_own = expert_grad(slot_rows, grad_up_rows, [])
    gain_grads = jnp.pad(grad_gain_two.reshape(devices, 1, -1), ((0, 0), (0, 7), (0, 0)))
    gain_rows = gain_grads.shape[2]
    gain_grads = jnp.pad(gain_grads, ((0, 0), (0, 0), (0, lanes - gain_rows)))
    if gain_rows % 16 == 0:
        sums = sum_dense(
            [normed_two.T, attended.T, shared_hidden.T, normed_one.T],
            [grad_gate_up, grad_mixed_low, grad_low, grad_query],
            gain_grads,
            grad_key_value,
            ((shared_width, shared_width), (query_width, feat_width), (feat_width,), (key_width, key_width), (lanes,)),
            (((0, 0),), ((3, 3), (1, 1)), ((2, 2),), ((3, None),)),
            5,
        )
        gate_up_blocks, query_block, grad_output_block = sums[:2], sums[2], sums[3]
        qkv_blocks = [query_block, sums[5], sums[6]]
        grad_down_block, grad_gain_block = sums[4], sums[7]
        grad_qkv = jnp.concatenate([grad_query, sums[8]], axis=1)
    else:
        grad_key_value = jnp.concatenate([grad_key_value[0], grad_key_value[1]], axis=1)
        total = grad_key_value[:tok_rows]
        for step in range(1, back + 1):
            came = shift(total.astype(BF16), "seq", -1)
            total = came.astype(F32) + grad_key_value[step * tok_rows : (step + 1) * tok_rows]
        grad_qkv = jnp.concatenate([grad_query, total.astype(BF16)], axis=1)
        dense_grads = [
            weight_grad(normed_two, grad_gate_up),
            weight_grad(attended, grad_mixed_low),
            weight_grad(shared_hidden, grad_low),
            weight_grad(normed_one, grad_qkv),
            gain_grads,
        ]
        sums = scatter_dense(dense_grads, 5)
        gate_up_blocks, grad_output_block, grad_down_block, qkv_blocks, grad_gain_block = sums
        gate_up_blocks = jnp.split(gate_up_blocks, [shared_width], axis=1)
        qkv_blocks = jnp.split(qkv_blocks, [query_width, query_width + key_width], axis=1)
    grad_normed_one = dot(grad_qkv, qkv_full, 1, 1)
    _, pull_one = jax.vjp(lambda values: rms_norm(values, gain_one), x_float)
    grad_tokens = grad_mixed + pull_one(grad_normed_one)[0]
    grad_gain_one = sum(
        jnp.sum(weight.astype(F32) * grad, axis=1)
        for weight, grad in zip((query_weight, key_weight, value_weight), qkv_blocks)
    ) / norm1_gain.astype(F32)
    last = [grad_gain_block]
    grad_expert_down = expert_sum(expert_down_own, last)
    grad_expert_gate = expert_sum(expert_gate_own, last)
    grad_expert_up = expert_sum(expert_up_own, last)
    return (
        block_output[None],
        grad_tokens[None],
        grad_gain_one,
        *qkv_blocks,
        grad_output_block,
        grad_gain_block[0, :gain_rows],
        *gate_up_blocks,
        grad_down_block,
        grad_expert_gate,
        grad_expert_up,
        grad_expert_down,
    )


def solution(mesh):
    rows = P("fsdp", "seq", None)
    dense = P(("seq", "fsdp"), None)
    gain = P(("seq", "fsdp"))
    return jax.shard_map(
        block,
        mesh=mesh,
        in_specs=(
            rows, rows, P("fsdp", "seq"), P("fsdp", None), rows, rows,
            gain, dense, dense, dense, dense, gain, dense, dense, dense, rows, rows, rows,
        ),
        out_specs=(
            rows, rows, gain, dense, dense, dense, dense, gain, dense, dense, dense, rows, rows, rows,
        ),
        check_vma=False,
    )
```
